256 devices in a mesh: member: 2 (over core), tp: 128 (over x, z, y).
Axes of the slice: x: 4, y: 4, z: 8, core: 2. Of those that a mesh axis runs over, the one named last changes fastest.
Arguments:
- stream_in: bfloat16 [512, 4096], P(('member', 'tp')), may hold values from -6 to 6
- kv_cache: bfloat16 [512, 512, 2048], P(('member', 'tp')), may hold values from -400 to 400
- lengths: int32 [128], replicated, may hold values from 1 to 512
- targets: int32 [128], replicated, may hold values from 0 to 65535
- norm_gains: float32 [3, 4096], replicated, may hold values from 0.1 to 1.9
- w_qkv: bfloat16 [4096, 6144], P(None, 'tp'), may hold values from -0.09375 to 0.09375
- w_out: bfloat16 [4096, 4096], P('tp'), may hold values from -0.09375 to 0.09375
- w_gate_up: bfloat16 [2, 4096, 14336], P(None, None, 'tp'), may hold values from -0.09375 to 0.09375
- w_down: bfloat16 [14336, 4096], P('tp'), may hold values from -0.046875 to 0.046875
- lm_head: bfloat16 [4096, 65536], P(None, 'tp'), may hold values from -300 to 300
- fast_in: float32 [4, 2, 4096], P('member'), may hold values from 0.1 to 1.9
- fast_hidden: float32 [4, 3, 14336], P('member', None, 'tp'), may hold values from 0.1 to 1.9
- fast_out: float32 [4, 4096], P('member'), may hold values from 0.1 to 1.9
Outputs:
- mean_logits: bfloat16 [128, 65536], P(None, 'tp')
- token_logprob: float32 [128], replicated
The draws below stay inside these ranges and needn't reach their ends.
Inputs may be any that keep to these rules, and one draw needn't show every extreme that they name: lengths is the same for all members.
All inputs are finite; a program needn't handle non-finite values.
Results may differ from the reference program's by a relative error of at most 0.02.
Values may be sent and summed in bfloat16 or wider, within the bound.
A program may use at most 128 MiB of HBM per device.

```python
import math
import jax
import jax.numpy as jnp
import numpy as np
from jax import lax

D = 4096
HEADS = 32
KV = 8
HD = 128
FF = 14336
VOCAB = 65536
B = 128
CACHE = 512
MEMBERS = 4


def draw_kv_cache(key, part):
    row_total = MEMBERS * B
    array_shape = (row_total, CACHE, 2 * KV * HD)
    key_main = jax.random.fold_in(key, 11)
    raw_draw = jnp.clip(jax.random.normal(key_main, array_shape, jnp.float32), -6.0, 6.0)
    return raw_draw.astype(jnp.bfloat16)


def draw_lm_head(key, part):
    array_shape = (D, VOCAB)
    key_main = jax.random.fold_in(key, 61)
    spread_scale = 3.0 / math.sqrt(D)
    result = jnp.clip(jax.random.normal(key_main, array_shape, jnp.float32) * spread_scale, -6.0 * spread_scale, 6.0 * spread_scale)
    return result.astype(jnp.bfloat16)


def with_ends(values, stream_key, low, largest):
    longest = values.shape.index(max(values.shape))
    spots = []
    for shift in (0, 1):
        where = [jax.random.randint(jax.random.fold_in(stream_key, axis), (), 0, length) for axis, length in enumerate(values.shape)]
        where[longest] = (where[longest] + shift) % values.shape[longest]
        spots.append(tuple(where))
    return values.at[spots[0]].set(low).at[spots[1]].set(largest)


def shard_levels(own_key, shape, shards, least, high):
    def one(axis_at, blocks):
        steps = jax.random.uniform(jax.random.fold_in(jax.random.fold_in(own_key, 6), axis_at), (blocks,), jnp.float32, least / len(shards), high / len(shards))
        return jnp.repeat(jnp.exp(steps), shape[axis_at] // blocks).reshape((-1,) + (1,) * (len(shape) - axis_at - 1))

    factor_of = one(*shards[0])
    for cut in shards[1:]:
        factor_of = factor_of * one(*cut)
    return factor_of


def rank_bounds(amount, skew):
    portions = [(1 << 20) // math.isqrt(grade ** skew) + 1 for grade in range(1, amount + 1)]
    deviation = 1 + sum(portions) // (1 << 30)
    return np.cumsum(np.array([max(1, weight // deviation) for weight in portions]))


def skewed_ids(stream_key, shape, number_of, slope):
    grid = rank_bounds(number_of, slope)
    lot = jax.random.randint(jax.random.fold_in(stream_key, 1), shape, 0, int(grid[number_of - 1]))
    grade = jnp.searchsorted(jnp.asarray(grid, jnp.int32), lot, side="right")
    return jax.random.permutation(jax.random.fold_in(stream_key, 2), number_of)[grade].astype(jnp.int32)


def noise(rng, shape, scale, most, cuts=(), held_as=jnp.bfloat16):
    values = scale * jax.random.normal(rng, shape, jnp.float32)
    if cuts:
        values = values * shard_levels(rng, shape, cuts, -0.22, 0.18)
    return jnp.clip(values, -most, most).astype(held_as)


def setup_inputs(seed: int = 0) -> dict:
    keys = jax.random.split(jax.random.key(seed), 14)
    return {
        "stream_in": noise(keys[0], (MEMBERS * B, D), 1.0, 6.0, ((0, 256),)),
        "kv_cache": draw_kv_cache(jax.random.fold_in(keys[13], 71), 0),
        "lengths": with_ends(jax.random.randint(keys[2], (B,), 1, CACHE + 1), jax.random.fold_in(keys[2], 1), 1, CACHE).astype(jnp.int32),
        "targets": with_ends(skewed_ids(keys[3], (B,), VOCAB, 2), jax.random.fold_in(keys[3], 3), 0, VOCAB - 1).astype(jnp.int32),
        "norm_gains": jnp.clip(1.0 + 0.18 * jax.random.normal(keys[4], (3, D), jnp.float32), 0.1, 1.9),
        "w_qkv": noise(keys[5], (D, (HEADS + 2 * KV) * HD), D ** -0.5, 0.09375, ((1, 128),)),
        "w_out": noise(keys[6], (HEADS * HD, D), (HEADS * HD) ** -0.5, 0.09375, ((0, 128),)),
        "w_gate_up": noise(keys[7], (2, D, FF), D ** -0.5, 0.09375, ((2, 128),)),
        "w_down": noise(keys[8], (FF, D), FF ** -0.5, 0.046875, ((0, 128),)),
        "lm_head": draw_lm_head(jax.random.fold_in(keys[13], 71), 0),
        "fast_in": jnp.clip(1.0 + 0.18 * jax.random.normal(keys[10], (MEMBERS, 2, D), jnp.float32), 0.1, 1.9),
        "fast_hidden": jnp.clip(1.0 + 0.18 * jax.random.normal(keys[11], (MEMBERS, 3, FF), jnp.float32), 0.1, 1.9),
        "fast_out": jnp.clip(1.0 + 0.18 * jax.random.normal(keys[12], (MEMBERS, D), jnp.float32), 0.1, 1.9),
    }


ROPE_BASE = 500000.0

def rms_norm(values_in, gain):
    return values_in * lax.rsqrt(lax.optimization_barrier(jnp.mean(values_in * values_in, axis=-1, keepdims=True)) + 1e-05) * gain

def rotate(values_in, positions):
    half_dim = values_in.shape[-1] // 2
    frequency = ROPE_BASE ** (-jnp.arange(half_dim, dtype=jnp.float32) * 2.0 / values_in.shape[-1])
    angles = positions.astype(jnp.float32)[:, None, None] * frequency[None, None, :]
    lower_half = values_in[..., :half_dim]
    upper_half = values_in[..., half_dim:]
    return jnp.concatenate([lower_half * jnp.cos(angles) - upper_half * jnp.sin(angles), upper_half * jnp.cos(angles) + lower_half * jnp.sin(angles)], axis=-1)

def attend(projected, cache_rows, positions):
    row_count = projected.shape[0]
    head_cols = HEADS * HD
    kv_cols = KV * HD
    queries = rotate(projected[:, :head_cols].astype(jnp.float32).reshape(row_count, HEADS, HD), positions).astype(jnp.bfloat16)
    new_key = rotate(projected[:, head_cols:head_cols + kv_cols].astype(jnp.float32).reshape(row_count, KV, HD), positions).astype(jnp.bfloat16)
    new_value = projected[:, head_cols + kv_cols:].reshape(row_count, KV, HD)
    cache_keys = cache_rows[:, :, :kv_cols].reshape(row_count, CACHE, KV, HD)
    cache_values = cache_rows[:, :, kv_cols:].reshape(row_count, CACHE, KV, HD)
    grouped = queries.reshape(row_count, KV, HEADS // KV, HD).astype(jnp.float32)
    inv_root = HD ** (-0.5)
    cached = jnp.einsum('rkgd,rckd->rkgc', grouped, cache_keys.astype(jnp.float32)) * inv_root
    fresh = jnp.einsum('rkgd,rkd->rkg', grouped, new_key.astype(jnp.float32)) * inv_root
    in_cache = jnp.arange(CACHE)[None, :] < positions[:, None]
    cached = jnp.where(in_cache[:, None, None, :], cached, -1e+30)
    peak = jnp.maximum(lax.optimization_barrier(jnp.max(cached, axis=-1)), fresh)
    weights = jnp.exp(cached - peak[..., None])
    fresh_w = jnp.exp(fresh - peak)
    total_sum = lax.optimization_barrier(jnp.sum(weights, axis=-1)) + fresh_w
    probs = (weights / total_sum[..., None]).astype(jnp.bfloat16)
    fresh_p = (fresh_w / total_sum).astype(jnp.bfloat16)
    result = jnp.einsum('rkgc,rckd->rkgd', probs.astype(jnp.float32), cache_values.astype(jnp.float32))
    result = result + fresh_p.astype(jnp.float32)[..., None] * new_value.astype(jnp.float32)[:, :, None, :]
    return result.reshape(row_count, HEADS * HD).astype(jnp.bfloat16)

def reference(stream_in, kv_cache, lengths, targets, norm_gains, w_qkv, w_out, w_gate_up, w_down, lm_head, fast_in, fast_hidden, fast_out):
    row_count = stream_in.shape[0]
    positions = jnp.tile(lengths, MEMBERS).astype(jnp.int32)
    attn_in = rms_norm(stream_in.astype(jnp.float32), norm_gains[0]).astype(jnp.bfloat16)
    projected = jnp.dot(attn_in, w_qkv, preferred_element_type=jnp.float32).astype(jnp.bfloat16)
    blocks = lax.map(lambda block_item: attend(block_item[0], block_item[1], block_item[2]), (projected.reshape(row_count // 8, 8, -1), kv_cache.reshape(row_count // 8, 8, CACHE, 2 * KV * HD), positions.reshape(row_count // 8, 8)))
    attended = blocks.reshape(row_count, HEADS * HD)
    middle = (stream_in.astype(jnp.float32) + jnp.dot(attended, w_out, preferred_element_type=jnp.float32)).astype(jnp.bfloat16)
    ffn_in = rms_norm(middle.astype(jnp.float32), norm_gains[1]).astype(jnp.bfloat16)
    grouped = ffn_in.astype(jnp.float32).reshape(MEMBERS, B, D)
    gate_in = (grouped * fast_in[:, 0][:, None, :]).astype(jnp.bfloat16).reshape(row_count, D)
    up_in = (grouped * fast_in[:, 1][:, None, :]).astype(jnp.bfloat16).reshape(row_count, D)
    gate_act = jnp.dot(gate_in, w_gate_up[0], preferred_element_type=jnp.float32).reshape(MEMBERS, B, FF) * fast_hidden[:, 0][:, None, :]
    up_act = jnp.dot(up_in, w_gate_up[1], preferred_element_type=jnp.float32).reshape(MEMBERS, B, FF) * fast_hidden[:, 1][:, None, :]
    hidden = (jax.nn.silu(gate_act) * up_act * fast_hidden[:, 2][:, None, :]).astype(jnp.bfloat16).reshape(row_count, FF)
    down_sum = jnp.dot(hidden, w_down, preferred_element_type=jnp.float32).reshape(MEMBERS, B, D) * fast_out[:, None, :]
    layer_out = (middle.astype(jnp.float32).reshape(MEMBERS, B, D) + down_sum).astype(jnp.bfloat16).reshape(row_count, D)
    final_in = rms_norm(layer_out.astype(jnp.float32), norm_gains[2]).astype(jnp.bfloat16)
    logits = jnp.dot(final_in, lm_head, preferred_element_type=jnp.float32)
    mean_logit = lax.optimization_barrier(jnp.sum(logits.reshape(MEMBERS, B, VOCAB), axis=0)) / MEMBERS
    peak = lax.optimization_barrier(jnp.max(mean_logit, axis=-1))
    log_total = peak + jnp.log(lax.optimization_barrier(jnp.sum(jnp.exp(mean_logit - peak[:, None]), axis=-1)))
    target_logit = lax.optimization_barrier(jnp.sum(jnp.where(jnp.arange(VOCAB)[None, :] == targets[:, None], mean_logit, 0.0), axis=-1))
    return (mean_logit.astype(jnp.bfloat16), target_logit - log_total)
```

```python
import jax
import jax.numpy as jnp
import numpy as np
from jax import lax
from jax.experimental import pallas as pl
from jax.experimental.pallas import tpu as pltpu
from jax.sharding import Mesh
from jax.sharding import PartitionSpec as P

MESH = pl.DeviceIdType.MESH
F32 = jnp.float32
BF = jnp.bfloat16
NX, NZ, NY = 4, 8, 4
NP = NX * NY
D, HEADS, KV, HD, CACHE, FFD, VD = 4096, 32, 8, 128, 512, 112, 512
B = 128
QN = 384
ZORDER = (4, 3, 5, 2, 6, 1, 7)
NCH, CW = 4, 512
HALF = D // 2

VM = pltpu.VMEM
DMA = pltpu.SemaphoreType.DMA

SCRATCH = dict(
    st=VM((2, D), BF),
    kvv=VM((2, CACHE, 2 * KV * HD), BF),
    tg=VM((1, B), jnp.int32),
    gn=VM((3, D), F32),
    fi=VM((2, 2, D), F32),
    fh=VM((2, 3, FFD), F32),
    fo=VM((2, D), F32),
    fq=VM((1, 128), F32),
    wq=VM((NZ, 4, 128, 48), BF),
    wo=VM((NP, 32, 256), BF),
    wg=VM((2, NP, 256, FFD), BF),
    wd=VM((FFD, D), BF),
    lm=VM((HALF, VD), BF),
    sc=VM((64, 128), F32),
    s1s=VM((64, 128), F32),
    s1r=VM((64, 128), F32),
    raw=VM((NP, 16, 512), BF),
    p1=VM((3, 256, 128), F32),
    s3s=VM((NZ, 32, QN), BF),
    s3r=VM((NZ, 32, QN), BF),
    q1=VM((3, 32, 128), F32),
    s4s=VM((128, 128), F32),
    s4r=VM((128, 128), F32),
    hs=VM((96, 128), F32),
    osc=VM((64, 128), F32),
    s5s=VM((64, 128), F32),
    s5r=VM((64, 128), F32),
    att=VM((NP, 16, 512), BF),
    s7s=VM((NZ, 32, 256), BF),
    s7r=VM((NZ, 32, 256), BF),
    mid=VM((NP, 256, 256), BF),
    accg=VM((256, FFD), F32),
    accu=VM((256, FFD), F32),
    ssq=VM((256, 128), F32),
    hid=VM((256, FFD), BF),
    p3=VM((NX, NY, 16, D), BF),
    r1a=VM((NX, NY, 16, HALF), BF),
    r1b=VM((NY, NX, 16, HALF), BF),
    s2a=VM((NY, 16, HALF), BF),
    s2b=VM((NX, 16, HALF), BF),
    r2a=VM((NY, 16, HALF), BF),
    r2b=VM((NX, 16, HALF), BF),
    f3=VM((512, 128), F32),
    g3=VM((32, 128), F32),
    s13s=VM((NZ, 64, 128), BF),
    s13r=VM((NZ, 64, 128), BF),
    fs=VM((32, 128), F32),
    fr=VM((16, 128), F32),
    fb=VM((NP, NZ, 16, 128), BF),
    ff=VM((2048, 128), F32),
    lh=VM((B, HALF), BF),
    lp=VM((B, VD), F32),
    lr=VM((B, VD), F32),
    sz=VM((NZ, 8, 128), F32),
    sx=VM((NP, 8, 128), F32),
)
PHASES = dict(
    wq=NZ, wo=NP, s1=NZ, s2=NP, s3=NZ, s4=NP, s5=NZ, s6=NP, s7=NZ, s8=NZ,
    da=NP, fa=NP * 4, fb_=NP * 4, a1=NCH * 4, b1=NCH * 4, a2=NCH * 4, b2=NCH * 4,
    s13=NZ, fx=1, s14=NZ, s15=NP, lx=1, s16=NZ, s17=NP,
)
LOCAL = ("st", "kvv", "tg", "gn", "fi", "fh", "fo", "fq", "wq", "wo", "wg", "wd", "lm")
INPUTS = (
    "stream", "kv", "lengths", "targets", "gains", "wqkv", "wout", "wgu", "wdown", "lmh",
    "fin", "fhid", "fout", "freq",
)


def kernel(names, debug, *refs):
    r = dict(zip(names, refs))
    c, x, z, y = (lax.axis_index(a) for a in ("member", "tp_0", "tp_1", "tp_2"))
    t = x * 32 + z * 4 + y
    n = x * 4 + y
    sends = []

    def rem(v, k):
        return lax.rem(v, k)

    def at_z(zz):
        return (c, x, zz, y)

    def at_xy(xx, yy):
        return (c, xx, z, yy)

    partner = (1 - c, x, z, y)

    def copy(phase, src, dst, slot, dev, sslot=None):
        sslot = slot if sslot is None else sslot
        return pltpu.make_async_remote_copy(
            src_ref=src,
            dst_ref=dst,
            send_sem=r["ss_" + phase].at[sslot],
            recv_sem=r["rs_" + phase].at[slot],
            device_id=dev,
            device_id_type=MESH,
        )

    def send(phase, src, dst, slot, dev, sslot=None):
        k = copy(phase, src, dst, slot, dev, sslot)
        k.start()
        sends.append(k)

    def recv(phase, dst, slot, sslot=None):
        copy(phase, dst, dst, slot, partner, sslot).wait_recv()

    zpeers = [rem(z + d, NZ) for d in ZORDER]
    plane = [
        (rem(x + dx, NX), rem(y + dy, NY))
        for dx, dy in sorted(
            ((a, b) for a in range(NX) for b in range(NY) if a or b),
            key=lambda p: -(min(p[0], 4 - p[0]) + min(p[1], 4 - p[1])),
        )
    ]

    def z_send(phase, src_at, dst):
        for zz in zpeers:
            send(phase, src_at(zz), dst, z, at_z(zz), zz)

    def z_recv(phase, dst_at):
        for zz in zpeers:
            recv(phase, dst_at(zz), zz)

    def xy_send(phase, src_at, dst):
        for xx, yy in plane:
            send(phase, src_at(xx * 4 + yy), dst, n, at_xy(xx, yy), xx * 4 + yy)

    def xy_recv(phase, dst_at):
        for xx, yy in plane:
            recv(phase, dst_at(xx * 4 + yy), xx * 4 + yy)

    bar = pltpu.get_barrier_semaphore()
    peers = [at_z(zz) for zz in zpeers] + [at_xy(*p) for p in plane] + [partner]
    for dev in peers:
        pl.semaphore_signal(bar, inc=1, device_id=dev, device_id_type=MESH)

    local = {}

    def fetch(name, src, dst):
        k = pltpu.make_async_copy(src, dst, r["ls"].at[LOCAL.index(name)])
        k.start()
        local[name] = k

    fetch("st", r["stream"], r["st"])
    fetch("gn", r["gains"], r["gn"])
    fetch("fq", r["freq"], r["fq"])
    fetch("wq", r["wqkv"].at[:, z], r["wq"].at[z])
    fetch("wo", r["wout"].at[:, pl.ds(pl.multiple_of(n * 256, 256), 256)], r["wo"].at[n])
    fetch("kvv", r["kv"], r["kvv"])
    fetch("fi", r["fin"], r["fi"])
    fetch("fh", r["fhid"], r["fh"])
    fetch("fo", r["fout"], r["fo"])
    fetch("tg", r["targets"], r["tg"])
    fetch("wg", r["wgu"], r["wg"])
    fetch("wd", r["wdown"], r["wd"])
    fetch("lm", r["lmh"].at[pl.ds(pl.multiple_of(c * HALF, HALF), HALF)], r["lm"])

    def spread(scratch, dst):
        for zz in range(NZ):
            r[dst][zz * 8 : zz * 8 + 8] = r[scratch][pl.ds(zz, 8, stride=8), :]

    z8 = pl.ds(pl.multiple_of(z * 8, 8), 8)

    def z_then_plane(zphase, pphase, s, rr, buf):
        def piece(zz):
            return pl.ds(pl.multiple_of(zz * 8, 8), 8)

        z_send(zphase, lambda zz: r[s].at[piece(zz)], r[rr].at[z8])
        r[rr][z8, :] = r[s][z8, :]
        z_recv(zphase, lambda zz: r[rr].at[piece(zz)])
        for k in range(4):
            rows = [r[rr][pl.ds(j * 4 + k, 8, stride=8), :] for j in range(2)]
            r[buf][n, :, k * 128 : (k + 1) * 128] = jnp.concatenate(rows, axis=0).astype(BF)
        xy_send(pphase, lambda m: r[buf].at[n], r[buf].at[n])
        return lambda: xy_recv(pphase, lambda m: r[buf].at[m])

    local["st"].wait()
    x32 = r["st"][...].astype(F32)
    rs = lax.rsqrt(jnp.mean(x32 * x32, axis=-1, keepdims=True) + 1e-5)
    for b in range(32):
        for j in range(2):
            r["sc"][j * 32 + b : j * 32 + b + 1, :] = x32[j : j + 1, b * 128 : (b + 1) * 128]
    spread("sc", "s1s")
    r["s4s"][...] = jnp.zeros((128, 128), F32)
    row8 = lax.broadcasted_iota(jnp.int32, (8, 128), 0)
    lane8 = lax.broadcasted_iota(jnp.int32, (8, 128), 1)
    rs8 = jnp.where(row8 < 4, rs[0:1, 0:1], rs[1:2, 0:1])

    pl.semaphore_wait(bar, len(peers))

    finish = z_then_plane("s1", "s2", "s1s", "s1r", "raw")
    z_send("wq", lambda zz: r["wqkv"].at[:, zz], r["wq"].at[z])
    xy_send(
        "wo",
        lambda m: r["wout"].at[:, pl.ds(pl.multiple_of(m * 256, 256), 256)],
        r["wo"].at[n],
    )
    local["fq"].wait()
    local["gn"].wait()
    pos = [r["lengths"][rem(2 * t + j, B)] for j in range(2)]
    ang = jnp.where(row8 < 4, pos[0], pos[1]).astype(F32) * r["fq"][0:1, :]
    cos8 = jnp.cos(ang)
    sin8 = jnp.where(lane8 < 64, -jnp.sin(ang), jnp.sin(ang))
    for b in range(32):
        r["g3"][b : b + 1, :] = r["gn"][2:3, b * 128 : (b + 1) * 128]

    local["wq"].wait()
    z_recv("wq", lambda zz: r["wq"].at[zz])
    wcat = jnp.concatenate([r["wq"][s].reshape(512, 48) for s in range(NZ)], axis=1)
    gq = jnp.concatenate(
        [r["gn"][0:1, pl.ds(pl.multiple_of(k * 1024 + z * 128, 128), 128)] for k in range(4)], axis=1
    )
    finish()
    lhs = (r["raw"][...].reshape(256, 512).astype(F32) * gq).astype(BF)
    prod = jnp.dot(lhs, wcat, preferred_element_type=F32)
    for l in range(3):
        r["p1"][l] = prod[:, l * 128 : (l + 1) * 128]
    for zz in range(NZ):
        for l in range(3):
            r["s3s"][zz, :, l * 128 : (l + 1) * 128] = r["p1"].at[l][
                pl.ds(zz, 32, stride=8), :
            ].astype(BF)
    z_send("s3", lambda zz: r["s3s"].at[zz], r["s3r"].at[z])
    r["s3r"][z] = r["s3s"][z]
    z_recv("s3", lambda zz: r["s3r"].at[zz])
    acc = r["s3r"][0].astype(F32)
    for s in range(1, NZ):
        acc = acc + r["s3r"][s].astype(F32)
    for l in range(3):
        r["q1"][l] = acc[:, l * 128 : (l + 1) * 128]
    for l in range(3):
        for j in range(2):
            r["s4s"][pl.ds(l * 2 + j, 16, stride=8), :] = r["q1"].at[l][pl.ds(j, 16, stride=2), :]

    def tile(m):
        return pl.ds(pl.multiple_of(m * 8, 8), 8)

    xy_send("s4", lambda m: r["s4s"].at[tile(m)], r["s4r"].at[tile(n)])
    r["s4r"][tile(n), :] = r["s4s"][tile(n), :]
    xy_recv("s4", lambda m: r["s4r"].at[tile(m)])

    blocks = {
        (yy, l): jnp.concatenate(
            [r["s4r"][pl.ds(yy * 8 + l * 2 + j, 4, stride=32), :] for j in range(2)], axis=0
        )
        for yy in range(NY)
        for l in range(3)
    }
    for hh in range(12):
        val = jnp.zeros((8, 128), F32)
        lane = 0
        while lane < 128:
            col = hh * 128 + lane
            tt, i = divmod(col, 48)
            at = (tt // 4) * 48 + i
            l, src = divmod(at, 128)
            width = min(48 - i, 128 - src, 128 - lane)
            piece = blocks[(tt % 4, l)]
            shift = (lane - src) % 128
            if shift:
                piece = pltpu.roll(piece, shift, 1)
            val = jnp.where((lane8 >= lane) & (lane8 < lane + width), piece, val)
            lane += width
        val = (val * rs8).astype(BF).astype(F32)
        turned = (val * cos8 + pltpu.roll(val, 64, 1) * sin8).astype(BF).astype(F32)
        if hh >= 4:
            turned = jnp.where(row8 % 4 == 3, val, turned)
        r["hs"][pl.ds(hh, 8, stride=12), :] = turned

    local["kvv"].wait()
    inv_root = HD**-0.5
    group = lax.broadcasted_iota(jnp.int32, (32, 128), 0) // 4
    group8 = (
        lax.broadcasted_iota(jnp.int32, (32, 8), 0) // 4
        == lax.broadcasted_iota(jnp.int32, (32, 8), 1)
    )
    place = lax.broadcasted_iota(jnp.int32, (32, CACHE), 1)
    nt = (((1,), (1,)), ((), ()))
    for j in range(2):
        q = r["hs"][j * 48 : j * 48 + 32, :]
        kn = r["hs"][j * 48 + 32 : j * 48 + 40, :].astype(BF)
        vn = r["hs"][j * 48 + 40 : j * 48 + 48, :].astype(BF)
        qd = jnp.concatenate([jnp.where(group == k, q, 0.0) for k in range(KV)], axis=1).astype(BF)
        scores = (
            lax.dot_general(qd, r["kvv"][j, :, : KV * HD], nt, preferred_element_type=F32) * inv_root
        )
        fresh = lax.dot_general(q.astype(BF), kn, nt, preferred_element_type=F32)
        fresh = jnp.sum(jnp.where(group8, fresh, 0.0), axis=1, keepdims=True) * inv_root
        scores = jnp.where(place < pos[j], scores, -1e30)
        peak = jnp.maximum(jnp.max(scores, axis=1, keepdims=True), fresh)
        weights = jnp.exp(scores - peak)
        fresh_w = jnp.exp(fresh - peak)
        total = jnp.sum(weights, axis=1, keepdims=True) + fresh_w
        probs = (weights / total).astype(BF)
        fresh_p = jnp.where(group8, fresh_w / total, 0.0).astype(BF)
        wide = jnp.dot(probs, r["kvv"][j, :, KV * HD :], preferred_element_type=F32)
        out = jnp.dot(fresh_p, vn, preferred_element_type=F32)
        for k in range(KV):
            out = out + jnp.where(group == k, wide[:, k * 128 : (k + 1) * 128], 0.0)
        r["osc"][j * 32 : j * 32 + 32, :] = out.astype(BF).astype(F32)

    spread("osc", "s5s")
    finish = z_then_plane("s5", "s6", "s5s", "s5r", "att")
    local["wo"].wait()
    xy_recv("wo", lambda m: r["wo"].at[m])
    resid = r["raw"][:, :, pl.ds(pl.multiple_of(x * 128, 128), 128)].reshape(256, 128).astype(F32)
    lo = resid * jnp.where(z == 2 * y, 1.0, 0.0)
    hi = resid * jnp.where(z == 2 * y + 1, 1.0, 0.0)
    finish()
    prod = jnp.dot(
        r["att"][...].reshape(256, 512), r["wo"][...].reshape(512, 256), preferred_element_type=F32
    ) + jnp.concatenate([lo, hi], axis=1)
    for xl in range(2):
        for ys in range(NY):
            for j in range(2):
                at = [((m * 2 + xl) * 4 + ys) * 16 + j * 8 for m in range(2)]
                r["s7s"][xl * 4 + ys, j * 16 : j * 16 + 16, :] = jnp.concatenate(
                    [prod[a : a + 8] for a in at], axis=0
                ).astype(BF)
    z_send("s7", lambda zz: r["s7s"].at[zz], r["s7r"].at[z])
    r["s7r"][z] = r["s7s"][z]
    z_recv("s7", lambda zz: r["s7r"].at[zz])
    acc = r["s7r"][0].astype(F32)
    for s in range(1, NZ):
        acc = acc + r["s7r"][s].astype(F32)

    def z32(zz):
        return pl.ds(pl.multiple_of(zz * 32, 32), 32)

    r["mid"][n, z32(z), :] = acc.astype(BF)
    z_send("s8", lambda zz: r["mid"].at[n, z32(z)], r["mid"].at[n, z32(z)])
    r["accg"][...] = jnp.zeros((256, FFD), F32)
    r["accu"][...] = jnp.zeros((256, FFD), F32)
    r["ssq"][...] = jnp.zeros((256, 128), F32)
    for name in ("fi", "fh", "fo", "wg", "wd"):
        local[name].wait()
    z_recv("s8", lambda zz: r["mid"].at[n, z32(zz)])

    near = (1, 3, 2)
    for d in (2, 1, 3):
        xx, yy = rem(x + d, NX), rem(y + d, NY)
        send("da", r["mid"].at[n], r["mid"].at[n], n, at_xy(xx, y), xx * 4 + y)
        send("da", r["mid"].at[n], r["mid"].at[n], n, at_xy(x, yy), x * 4 + yy)

    def ffn_chunk(m):
        v = r["mid"][m].astype(F32)
        r["ssq"][...] += v[:, :128] * v[:, :128] + v[:, 128:] * v[:, 128:]
        cols = pl.ds(pl.multiple_of(m * 256, 256), 256)
        g = r["gn"][1:2, cols]
        v4 = v.reshape(16, 2, 8, 256)
        for k, name in enumerate(("accg", "accu")):
            f = jnp.concatenate(
                [
                    (r["fi"][i, k : k + 1, cols] * g).reshape(1, 1, 1, 256)
                    for i in range(2)
                ],
                axis=1,
            )
            act = (v4 * f).reshape(256, 256).astype(BF)
            r[name][...] += jnp.dot(act, r["wg"][k, m], preferred_element_type=F32)

    ffn_chunk(n)
    top, low = pl.ds(0, 128), pl.ds(128, 128)
    for d in near:
        xx = rem(x + d, NX)
        m = xx * 4 + y
        recv("da", r["mid"].at[m], m)
        for e in (2, 1, 3):
            yy = rem(y + e, NY)
            send("fa", r["mid"].at[m, top], r["mid"].at[m, top], m, at_xy(x, yy), m * 4 + e)
        yy = rem(y + d, NY)
        m = x * 4 + yy
        recv("da", r["mid"].at[m], m)
        for e in (2, 1, 3):
            xx = rem(x + e, NX)
            send("fb_", r["mid"].at[m, low], r["mid"].at[m, low], m, at_xy(xx, y), m * 4 + e)

    def line_step(i, carry):
        ffn_chunk(rem(x + 1 + i, NX) * 4 + y)
        ffn_chunk(x * 4 + rem(y + 1 + i, NY))
        return carry

    lax.fori_loop(0, 3, line_step, 0)

    def diag_step(i, carry):
        m = rem(x + 1 + i // 3, NX) * 4 + rem(y + 1 + i % 3, NY)
        recv("fa", r["mid"].at[m, top], m)
        recv("fb_", r["mid"].at[m, low], m)
        ffn_chunk(m)
        return carry

    lax.fori_loop(0, 9, diag_step, 0)
    scale = lax.rsqrt(jnp.sum(r["ssq"][...], axis=1, keepdims=True) * (1.0 / D) + 1e-5)

    def by_member(k):
        return jnp.concatenate(
            [r["fh"][i, k : k + 1, :].reshape(1, 1, 1, FFD) for i in range(2)], axis=1
        )

    gate = (r["accg"][...] * scale).reshape(16, 2, 8, FFD) * by_member(0)
    up = (r["accu"][...] * scale).reshape(16, 2, 8, FFD) * by_member(1)
    hidden = gate / (1.0 + jnp.exp(-gate)) * up * by_member(2)
    r["hid"][...] = hidden.reshape(256, FFD).astype(BF)

    def chunk(ch):
        return pl.ds(pl.multiple_of(ch * CW, CW), CW)

    def high(ch):
        return pl.ds(pl.multiple_of(HALF + ch * CW, CW), CW)

    def a1(ch, xx):
        return copy(
            "a1", r["p3"].at[xx, :, :, chunk(ch)], r["r1a"].at[x, :, :, chunk(ch)],
            ch * 4 + x, at_xy(xx, y), ch * 4 + xx,
        )

    def b1(ch, yy):
        return copy(
            "b1", r["p3"].at[:, yy, :, high(ch)], r["r1b"].at[y, :, :, chunk(ch)],
            ch * 4 + y, at_xy(x, yy), ch * 4 + yy,
        )

    def down_step(ch, carry):
        for cols in (chunk(ch), high(ch)):
            v = jnp.dot(r["hid"][...], r["wd"][:, cols], preferred_element_type=F32)
            r["p3"][:, :, :, cols] = v.astype(BF).reshape(NX, NY, 16, CW)
        for d in (2, 1, 3):
            a1(ch, rem(x + d, NX)).start()
            b1(ch, rem(y + d, NY)).start()
        return carry

    lax.fori_loop(0, NCH, down_step, 0)

    def a2(ch, yy):
        return copy(
            "a2", r["s2a"].at[yy, :, chunk(ch)], r["r2a"].at[y, :, chunk(ch)],
            ch * 4 + y, at_xy(x, yy), ch * 4 + yy,
        )

    def b2(ch, xx):
        return copy(
            "b2", r["s2b"].at[xx, :, chunk(ch)], r["r2b"].at[x, :, chunk(ch)],
            ch * 4 + x, at_xy(xx, y), ch * 4 + xx,
        )

    def second_step(ch, carry):
        for d in near:
            xx = rem(x + d, NX)
            recv("a1", r["r1a"].at[xx, :, :, chunk(ch)], ch * 4 + xx)
        v = r["p3"][x, :, :, chunk(ch)].astype(F32)
        for d in near:
            v = v + r["r1a"][rem(x + d, NX), :, :, chunk(ch)].astype(F32)
        r["s2a"][:, :, chunk(ch)] = v.astype(BF)
        for d in (2, 1, 3):
            a2(ch, rem(y + d, NY)).start()
        for d in near:
            yy = rem(y + d, NY)
            recv("b1", r["r1b"].at[yy, :, :, chunk(ch)], ch * 4 + yy)
        v = r["p3"][:, y, :, high(ch)].astype(F32)
        for d in near:
            v = v + r["r1b"][rem(y + d, NY), :, :, chunk(ch)].astype(F32)
        r["s2b"][:, :, chunk(ch)] = v.astype(BF)
        for d in (2, 1, 3):
            b2(ch, rem(x + d, NX)).start()
        return carry

    lax.fori_loop(0, NCH, second_step, 0)
    for ch in range(NCH):
        for d in near:
            yy = rem(y + d, NY)
            recv("a2", r["r2a"].at[yy, :, chunk(ch)], ch * 4 + yy)
            xx = rem(x + d, NX)
            recv("b2", r["r2b"].at[xx, :, chunk(ch)], ch * 4 + xx)

    row16 = lax.broadcasted_iota(jnp.int32, (16, 128), 0)
    own_row = rem(row16, 8) == z
    tile16 = pl.ds(pl.multiple_of(n * 16, 16), 16)
    for b in range(32):
        own, got, me, count = (
            ("s2a", "r2a", y, NY) if b < 16 else ("s2b", "r2b", x, NX)
        )
        cols = slice((b % 16) * 128, (b % 16 + 1) * 128)
        v = r[own][me, :, cols].astype(F32)
        for d in near:
            v = v + r[got][rem(me + d, count), :, cols].astype(F32)
        at = slice(b * 128, (b + 1) * 128)
        v = v * jnp.where(row16 < 8, r["fo"][0:1, at], r["fo"][1:2, at])
        m = r["mid"][b // 2, tile16, (b % 2) * 128 : (b % 2 + 1) * 128].astype(F32)
        r["f3"][b * 16 : (b + 1) * 16, :] = v + jnp.where(own_row, m, 0.0)

    for zz in range(NZ):
        for m in range(2):
            r["s13s"][zz, m * 32 : (m + 1) * 32, :] = r["f3"][
                pl.ds(m * 8 + zz, 32, stride=16), :
            ].astype(BF)
    z_send("s13", lambda zz: r["s13s"].at[zz], r["s13r"].at[z])
    owned = [r["f3"][pl.ds(m * 8 + z, 32, stride=16), :] for m in range(2)]
    z_recv("s13", lambda zz: r["s13r"].at[zz])
    both = jnp.zeros((32, 128), F32)
    for m in range(2):
        v = owned[m]
        for zz in zpeers:
            v = v + r["s13r"][zz, m * 32 : (m + 1) * 32, :].astype(F32)
        v = v.astype(BF).astype(F32)
        mean = jnp.sum(jnp.sum(v * v, axis=1, keepdims=True), axis=0, keepdims=True) * (1.0 / D)
        both = both + (v * lax.rsqrt(mean + 1e-5) * r["g3"][...]).astype(BF).astype(F32)
    r["fs"][...] = both

    def half(k):
        return pl.ds(pl.multiple_of(k * 16, 16), 16)

    send("fx", r["fs"].at[half(1 - c)], r["fr"], 0, partner)
    recv("fx", r["fr"], 0)
    r["fb"][n, z] = ((r["fs"][half(c), :] + r["fr"][...]) * 0.25).astype(BF)
    z_send("s14", lambda zz: r["fb"].at[n, z], r["fb"].at[n, z])
    local["lm"].wait()
    local["tg"].wait()
    wanted = jnp.broadcast_to(r["tg"][...].astype(F32), (B, B)).T[:, 0:1]
    z_recv("s14", lambda zz: r["fb"].at[n, zz])
    xy_send("s15", lambda m: r["fb"].at[n], r["fb"].at[n])
    xy_recv("s15", lambda m: r["fb"].at[m])
    r["ff"][...] = r["fb"][...].reshape(2048, 128).astype(F32)
    for b in range(16):
        rows = [
            r["ff"][pl.ds(xl * 1024 + zz * 16 + b, 8, stride=128), :]
            for xl in range(2)
            for zz in range(NZ)
        ]
        r["lh"][:, b * 128 : (b + 1) * 128] = jnp.concatenate(rows, axis=0).astype(BF)
    r["lp"][...] = jnp.dot(r["lh"][...], r["lm"][...], preferred_element_type=F32)
    send("lx", r["lp"], r["lr"], 0, partner)
    recv("lx", r["lr"], 0)
    mean_f = r["lp"][...] + r["lr"][...]
    r["logits_o"][...] = mean_f.astype(BF)

    ids = (lax.broadcasted_iota(jnp.int32, (B, VD), 1) + t * VD).astype(F32)
    found = jnp.sum(jnp.where(ids == wanted, mean_f, 0.0), axis=1, keepdims=True)
    peak = jnp.max(mean_f, axis=1, keepdims=True)
    total = jnp.sum(jnp.exp(mean_f - peak), axis=1, keepdims=True)
    lane = lax.broadcasted_iota(jnp.int32, (B, B), 1)
    stat = jnp.where(lane == 0, peak, jnp.where(lane == 1, total, jnp.where(lane == 2, found, 0.0)))
    r["sz"][z] = stat.T[:8]

    def combine(ref, count):
        peaks = [ref[k, 0:1, :] for k in range(count)]
        top_ = peaks[0]
        for k in range(1, count):
            top_ = jnp.maximum(top_, peaks[k])
        tot = ref[0, 1:2, :] * jnp.exp(peaks[0] - top_)
        hit = ref[0, 2:3, :]
        for k in range(1, count):
            tot = tot + ref[k, 1:2, :] * jnp.exp(peaks[k] - top_)
            hit = hit + ref[k, 2:3, :]
        return top_, tot, hit

    z_send("s16", lambda zz: r["sz"].at[z], r["sz"].at[z])
    z_recv("s16", lambda zz: r["sz"].at[zz])
    a, b_, h = combine(r["sz"], NZ)
    r["sx"][n] = jnp.concatenate([a, b_, h, jnp.zeros((5, 128), F32)], axis=0)
    xy_send("s17", lambda m: r["sx"].at[n], r["sx"].at[n])
    xy_recv("s17", lambda m: r["sx"].at[m])
    a, b_, h = combine(r["sx"], NP)
    r["lp_o"][...] = h - (a + jnp.log(b_))

    for k in sends:
        k.wait_send()

    def drain(ch, carry):
        for d in near:
            a1(ch, rem(x + d, NX)).wait_send()
            b1(ch, rem(y + d, NY)).wait_send()
            a2(ch, rem(y + d, NY)).wait_send()
            b2(ch, rem(x + d, NX)).wait_send()
        return carry

    lax.fori_loop(0, NCH, drain, 0)
    for name in debug:
        r["dbg_" + name][...] = r[name][...]


def body(
    stream_in, kv_cache, lengths, targets, norm_gains, w_qkv, w_out, w_gate_up, w_down, lm_head,
    fast_in, fast_hidden, fast_out, debug=(),
):
    freq = np.float32(500000.0) ** (-np.arange(64, dtype=np.float32) * 2.0 / 128)
    freq = jnp.asarray(np.concatenate([freq, freq])[None, :], F32)
    args = dict(
        stream=stream_in, kv=kv_cache, lengths=lengths, targets=targets.reshape(1, B),
        gains=norm_gains, wqkv=w_qkv.reshape(4, NZ, 128, 48), wout=w_out,
        wgu=w_gate_up.reshape(2, NP, 256, FFD), wdown=w_down, lmh=lm_head,
        fin=fast_in, fhid=fast_hidden, fout=fast_out, freq=freq,
    )
    outs = ["logits_o", "lp_o"] + ["dbg_" + k for k in debug]
    shapes = [jax.ShapeDtypeStruct((B, VD), BF), jax.ShapeDtypeStruct((1, B), F32)] + [
        jax.ShapeDtypeStruct(SCRATCH[k].shape, SCRATCH[k].dtype) for k in debug
    ]
    sems = {}
    for k, count in PHASES.items():
        sems["ss_" + k] = DMA((count,))
        sems["rs_" + k] = DMA((count,))
    sems["ls"] = DMA((len(LOCAL),))
    names = list(INPUTS) + outs + list(SCRATCH) + list(sems)
    import functools

    got = pl.pallas_call(
        functools.partial(kernel, names, debug),
        out_shape=shapes,
        in_specs=[
            pl.BlockSpec(memory_space=pltpu.SMEM if k == "lengths" else pl.ANY) for k in INPUTS
        ],
        out_specs=[pl.BlockSpec(memory_space=VM)] * len(outs),
        scratch_shapes=list(SCRATCH.values()) + list(sems.values()),
        compiler_params=pltpu.CompilerParams(
            collective_id=0, has_side_effects=True, vmem_limit_bytes=60 * 1024 * 1024
        ),
        name="step",
    )(*(args[k] for k in INPUTS))
    return (got[0], got[1].reshape(B), *got[2:])


MEMBER_TP = ("member", "tp_0", "tp_1", "tp_2")
TP = ("tp_0", "tp_1", "tp_2")
IN_SPECS = (
    P(MEMBER_TP, None), P(MEMBER_TP, None, None), P(), P(), P(), P(None, TP), P(TP, None),
    P(None, None, TP), P(TP, None), P(None, TP), P("member", None, None), P("member", None, TP),
    P("member", None),
)


def solution(mesh):
    split = Mesh(
        mesh.devices.reshape(mesh.shape["member"], NX, NZ, NY), ("member", "tp_0", "tp_1", "tp_2")
    )
    return jax.shard_map(
        body, mesh=split, in_specs=IN_SPECS, out_specs=(P(None, TP), P()), check_vma=False
    )
```

```python
import jax
import jax.numpy as jnp
import numpy as np
from jax import lax
from jax.experimental import pallas as pl
from jax.experimental.pallas import tpu as pltpu
from jax.sharding import Mesh
from jax.sharding import PartitionSpec as P

MESH = pl.DeviceIdType.MESH
F32 = jnp.float32
BF = jnp.bfloat16
NX, NZ, NY = 4, 8, 4
NP = NX * NY
D, HEADS, KV, HD, CACHE, FFD, VD = 4096, 32, 8, 128, 512, 112, 512
B = 128
QN = 384
ZORDER = (4, 3, 5, 2, 6, 1, 7)
NCH, CW = 4, 512
HALF = D // 2
NT = (((1,), (1,)), ((), ()))

VM = pltpu.VMEM
DMA = pltpu.SemaphoreType.DMA

SCRATCH = dict(
    st=VM((2, D), BF),
    kvv=VM((2, CACHE, 2 * KV * HD), BF),
    tg=VM((1, B), jnp.int32),
    gn=VM((3, D), F32),
    fi=VM((2, 2, D), F32),
    fh=VM((3, 2, FFD), F32),
    fo=VM((2, D), F32),
    fq=VM((1, 128), F32),
    wq=VM((NZ, 48, 512), BF),
    wo=VM((NP, 32, 256), BF),
    wg=VM((2, FFD, D), BF),
    wd=VM((FFD, D), BF),
    lm=VM((HALF, VD), BF),
    sc=VM((64, 128), F32),
    s1s=VM((64, 128), F32),
    s1r=VM((64, 128), F32),
    raw=VM((NP, 16, 512), BF),
    p1=VM((3, 256, 128), F32),
    s3s=VM((NZ, 32, QN), BF),
    s3r=VM((NZ, 32, QN), BF),
    q1=VM((3, 32, 128), F32),
    s4s=VM((128, 128), F32),
    s4r=VM((128, 128), F32),
    hs=VM((96, 128), F32),
    osc=VM((64, 128), F32),
    s5s=VM((64, 128), F32),
    s5r=VM((64, 128), F32),
    att=VM((NP, 16, 512), BF),
    s7s=VM((NZ, 32, 256), BF),
    s7r=VM((NZ, 32, 256), BF),
    mid=VM((NP, 256, 256), BF),
    accg=VM((256, FFD), F32),
    accu=VM((256, FFD), F32),
    ssq=VM((256, 128), F32),
    hid=VM((256, FFD), BF),
    p3=VM((NX, NY, 16, D), BF),
    r1a=VM((NX, NY, 16, HALF), BF),
    r1b=VM((NY, NX, 16, HALF), BF),
    s2a=VM((NY, 16, HALF), BF),
    s2b=VM((NX, 16, HALF), BF),
    r2a=VM((NY, 16, HALF), BF),
    r2b=VM((NX, 16, HALF), BF),
    f3=VM((512, 128), F32),
    g3=VM((32, 128), F32),
    s13s=VM((NZ, 64, 128), BF),
    s13r=VM((NZ, 64, 128), BF),
    fs=VM((32, 128), F32),
    fr=VM((16, 128), F32),
    fb=VM((NP, NZ, 16, 128), BF),
    ff=VM((2048, 128), F32),
    lh=VM((B, HALF), BF),
    lp=VM((B, VD), F32),
    lr=VM((B, VD), F32),
    sz=VM((NZ, 8, 128), F32),
    sx=VM((NP, 8, 128), F32),
)
PHASES = dict(
    wq=NZ * 4, wo=NP, s1=NZ, s2=NP, s3=NZ, s4=NP, s5=NZ, s6=NP, s7=NZ, s8=NZ,
    da=NP, fa=NP * 4, fb_=NP * 4, a1=NCH * 4, b1=NCH * 4, a2=NCH * 4, b2=NCH * 4,
    s13=NZ, fx=1, s14=NZ, s15=NP, lx=1, s16=NZ, s17=NP,
)
LOCAL = (
    "st", "kvv", "tg", "gn", "fi", "fh", "fo", "fq", "wq0", "wq1", "wq2", "wq3", "wo", "wg", "wd", "lm",
)
INPUTS = (
    "stream", "kv", "lengths", "targets", "gains", "wqkv", "wout", "wgu", "wdown", "lmh",
    "fin", "fhid", "fout", "freq",
)


def kernel(names, debug, *refs):
    r = dict(zip(names, refs))
    c, x, z, y = (lax.axis_index(a) for a in ("member", "tp_0", "tp_1", "tp_2"))
    t = x * 32 + z * 4 + y
    n = x * 4 + y
    sends = []
    scope = []

    def mark(name):
        while scope:
            scope.pop().__exit__(None, None, None)
        if name:
            scope.append(jax.named_scope(name))
            scope[-1].__enter__()

    mark("start")
    def rem(v, k):
        return lax.rem(v, k)

    def at_z(zz):
        return (c, x, zz, y)

    def at_xy(xx, yy):
        return (c, xx, z, yy)

    partner = (1 - c, x, z, y)

    def copy(phase, src, dst, slot, dev, sslot=None):
        sslot = slot if sslot is None else sslot
        return pltpu.make_async_remote_copy(
            src_ref=src,
            dst_ref=dst,
            send_sem=r["ss_" + phase].at[sslot],
            recv_sem=r["rs_" + phase].at[slot],
            device_id=dev,
            device_id_type=MESH,
        )

    def send(phase, src, dst, slot, dev, sslot=None):
        k = copy(phase, src, dst, slot, dev, sslot)
        k.start()
        sends.append(k)

    def recv(phase, dst, slot, sslot=None):
        copy(phase, dst, dst, slot, partner, sslot).wait_recv()

    zpeers = [rem(z + d, NZ) for d in ZORDER]
    plane = [
        (rem(x + dx, NX), rem(y + dy, NY))
        for dx, dy in sorted(
            ((a, b) for a in range(NX) for b in range(NY) if a or b),
            key=lambda p: -(min(p[0], 4 - p[0]) + min(p[1], 4 - p[1])),
        )
    ]

    def z_send(phase, src_at, dst):
        for zz in zpeers:
            send(phase, src_at(zz), dst, z, at_z(zz), zz)

    def z_recv(phase, dst_at):
        for zz in zpeers:
            recv(phase, dst_at(zz), zz)

    def xy_send(phase, src_at, dst):
        for xx, yy in plane:
            send(phase, src_at(xx * 4 + yy), dst, n, at_xy(xx, yy), xx * 4 + yy)

    def xy_recv(phase, dst_at):
        for xx, yy in plane:
            recv(phase, dst_at(xx * 4 + yy), xx * 4 + yy)

    bar = pltpu.get_barrier_semaphore()
    peers = [at_z(zz) for zz in zpeers] + [at_xy(*p) for p in plane] + [partner]
    for dev in peers:
        pl.semaphore_signal(bar, inc=1, device_id=dev, device_id_type=MESH)

    def qcols(zz, k):
        return r["wqkv"].at[:, pl.ds(pl.multiple_of(k * 1024 + zz * 128, 128), 128)]

    local = {}

    def fetch(name, src, dst):
        k = pltpu.make_async_copy(src, dst, r["ls"].at[LOCAL.index(name)])
        k.start()
        local[name] = k

    fetch("st", r["stream"], r["st"])
    fetch("gn", r["gains"], r["gn"])
    fetch("fq", r["freq"], r["fq"])
    for k in range(4):
        fetch("wq%d" % k, qcols(z, k), r["wq"].at[z, :, k * 128 : (k + 1) * 128])
    fetch("wo", r["wout"].at[:, pl.ds(pl.multiple_of(n * 256, 256), 256)], r["wo"].at[n])
    fetch("kvv", r["kv"], r["kvv"])
    fetch("fi", r["fin"], r["fi"])
    fetch("fh", r["fhid"], r["fh"])
    fetch("fo", r["fout"], r["fo"])
    fetch("tg", r["targets"], r["tg"])
    fetch("wg", r["wgu"], r["wg"])
    fetch("wd", r["wdown"], r["wd"])
    fetch("lm", r["lmh"].at[pl.ds(pl.multiple_of(c * HALF, HALF), HALF)], r["lm"])

    def spread(scratch, dst):
        for zz in range(NZ):
            r[dst][zz * 8 : zz * 8 + 8] = r[scratch][pl.ds(zz, 8, stride=8), :]

    z8 = pl.ds(pl.multiple_of(z * 8, 8), 8)

    def z_then_plane(zphase, pphase, s, rr, buf):
        def piece(zz):
            return pl.ds(pl.multiple_of(zz * 8, 8), 8)

        z_send(zphase, lambda zz: r[s].at[piece(zz)], r[rr].at[z8])
        r[rr][z8, :] = r[s][z8, :]
        z_recv(zphase, lambda zz: r[rr].at[piece(zz)])
        for k in range(4):
            rows = [r[rr][pl.ds(j * 4 + k, 8, stride=8), :] for j in range(2)]
            r[buf][n, :, k * 128 : (k + 1) * 128] = jnp.concatenate(rows, axis=0).astype(BF)
        xy_send(pphase, lambda m: r[buf].at[n], r[buf].at[n])
        return lambda: xy_recv(pphase, lambda m: r[buf].at[m])

    local["st"].wait()
    x32 = r["st"][...].astype(F32)
    rs = lax.rsqrt(jnp.mean(x32 * x32, axis=-1, keepdims=True) + 1e-5)
    for b in range(32):
        for j in range(2):
            r["sc"][j * 32 + b : j * 32 + b + 1, :] = x32[j : j + 1, b * 128 : (b + 1) * 128]
    spread("sc", "s1s")
    r["s4s"][...] = jnp.zeros((128, 128), F32)
    row8 = lax.broadcasted_iota(jnp.int32, (8, 128), 0)
    lane8 = lax.broadcasted_iota(jnp.int32, (8, 128), 1)
    rs8 = jnp.where(row8 < 4, rs[0:1, 0:1], rs[1:2, 0:1])

    mark("barrier")
    pl.semaphore_wait(bar, len(peers))
    mark("s1")

    finish = z_then_plane("s1", "s2", "s1s", "s1r", "raw")
    for zz in zpeers:
        for k in range(4):
            send(
                "wq", qcols(zz, k), r["wq"].at[z, :, k * 128 : (k + 1) * 128],
                z * 4 + k, at_z(zz), zz * 4 + k,
            )
    xy_send(
        "wo",
        lambda m: r["wout"].at[:, pl.ds(pl.multiple_of(m * 256, 256), 256)],
        r["wo"].at[n],
    )
    local["fq"].wait()
    local["gn"].wait()
    pos = [r["lengths"][rem(2 * t + j, B)] for j in range(2)]
    ang = jnp.where(row8 < 4, pos[0], pos[1]).astype(F32) * r["fq"][0:1, :]
    cos8 = jnp.cos(ang)
    sin8 = jnp.where(lane8 < 64, -jnp.sin(ang), jnp.sin(ang))
    for b in range(32):
        r["g3"][b : b + 1, :] = r["gn"][2:3, b * 128 : (b + 1) * 128]

    mark("wqwait")
    for k in range(4):
        local["wq%d" % k].wait()
    for zz in zpeers:
        for k in range(4):
            recv("wq", r["wq"].at[zz, :, k * 128 : (k + 1) * 128], zz * 4 + k)
    gq = jnp.concatenate(
        [r["gn"][0:1, pl.ds(pl.multiple_of(k * 1024 + z * 128, 128), 128)] for k in range(4)], axis=1
    )
    mark("s2wait")
    finish()
    mark("qkv")
    lhs = (r["raw"][...].reshape(256, 512).astype(F32) * gq).astype(BF)
    prod = lax.dot_general(lhs, r["wq"][...].reshape(QN, 512), NT, preferred_element_type=F32)
    for l in range(3):
        r["p1"][l] = prod[:, l * 128 : (l + 1) * 128]
    for zz in range(NZ):
        for l in range(3):
            r["s3s"][zz, :, l * 128 : (l + 1) * 128] = r["p1"].at[l][
                pl.ds(zz, 32, stride=8), :
            ].astype(BF)
    mark("s3")
    z_send("s3", lambda zz: r["s3s"].at[zz], r["s3r"].at[z])
    r["s3r"][z] = r["s3s"][z]
    z_recv("s3", lambda zz: r["s3r"].at[zz])
    acc = r["s3r"][0].astype(F32)
    for s in range(1, NZ):
        acc = acc + r["s3r"][s].astype(F32)
    for l in range(3):
        r["q1"][l] = acc[:, l * 128 : (l + 1) * 128]
    for l in range(3):
        for j in range(2):
            r["s4s"][pl.ds(l * 2 + j, 16, stride=8), :] = r["q1"].at[l][pl.ds(j, 16, stride=2), :]

    def tile(m):
        return pl.ds(pl.multiple_of(m * 8, 8), 8)

    mark("s4")
    xy_send("s4", lambda m: r["s4s"].at[tile(m)], r["s4r"].at[tile(n)])
    r["s4r"][tile(n), :] = r["s4s"][tile(n), :]
    xy_recv("s4", lambda m: r["s4r"].at[tile(m)])

    mark("heads")
    blocks = {
        (yy, l): jnp.concatenate(
            [r["s4r"][pl.ds(yy * 8 + l * 2 + j, 4, stride=32), :] for j in range(2)], axis=0
        )
        for yy in range(NY)
        for l in range(3)
    }
    for hh in range(12):
        val = jnp.zeros((8, 128), F32)
        lane = 0
        while lane < 128:
            col = hh * 128 + lane
            tt, i = divmod(col, 48)
            at = (tt // 4) * 48 + i
            l, src = divmod(at, 128)
            width = min(48 - i, 128 - src, 128 - lane)
            piece = blocks[(tt % 4, l)]
            shift = (lane - src) % 128
            if shift:
                piece = pltpu.roll(piece, shift, 1)
            val = jnp.where((lane8 >= lane) & (lane8 < lane + width), piece, val)
            lane += width
        val = (val * rs8).astype(BF).astype(F32)
        turned = (val * cos8 + pltpu.roll(val, 64, 1) * sin8).astype(BF).astype(F32)
        if hh >= 4:
            turned = jnp.where(row8 % 4 == 3, val, turned)
        r["hs"][pl.ds(hh, 8, stride=12), :] = turned

    mark("attn")
    local["kvv"].wait()
    inv_root = HD**-0.5
    group = lax.broadcasted_iota(jnp.int32, (32, 128), 0) // 4
    group8 = (
        lax.broadcasted_iota(jnp.int32, (32, 8), 0) // 4
        == lax.broadcasted_iota(jnp.int32, (32, 8), 1)
    )
    place = lax.broadcasted_iota(jnp.int32, (32, CACHE), 1)
    for j in range(2):
        q = r["hs"][j * 48 : j * 48 + 32, :]
        kn = r["hs"][j * 48 + 32 : j * 48 + 40, :].astype(BF)
        vn = r["hs"][j * 48 + 40 : j * 48 + 48, :].astype(BF)
        qd = jnp.concatenate([jnp.where(group == k, q, 0.0) for k in range(KV)], axis=1).astype(BF)
        scores = (
            lax.dot_general(qd, r["kvv"][j, :, : KV * HD], NT, preferred_element_type=F32) * inv_root
        )
        fresh = lax.dot_general(q.astype(BF), kn, NT, preferred_element_type=F32)
        fresh = jnp.sum(jnp.where(group8, fresh, 0.0), axis=1, keepdims=True) * inv_root
        scores = jnp.where(place < pos[j], scores, -1e30)
        peak = jnp.maximum(jnp.max(scores, axis=1, keepdims=True), fresh)
        weights = jnp.exp(scores - peak)
        fresh_w = jnp.exp(fresh - peak)
        total = jnp.sum(weights, axis=1, keepdims=True) + fresh_w
        probs = (weights / total).astype(BF)
        fresh_p = jnp.where(group8, fresh_w / total, 0.0).astype(BF)
        wide = jnp.dot(probs, r["kvv"][j, :, KV * HD :], preferred_element_type=F32)
        out = jnp.dot(fresh_p, vn, preferred_element_type=F32)
        for k in range(KV):
            out = out + jnp.where(group == k, wide[:, k * 128 : (k + 1) * 128], 0.0)
        r["osc"][j * 32 : j * 32 + 32, :] = out.astype(BF).astype(F32)

    mark("s5")
    spread("osc", "s5s")
    finish = z_then_plane("s5", "s6", "s5s", "s5r", "att")
    local["wo"].wait()
    xy_recv("wo", lambda m: r["wo"].at[m])
    resid = r["raw"][:, :, pl.ds(pl.multiple_of(x * 128, 128), 128)].reshape(256, 128).astype(F32)
    lo = resid * jnp.where(z == 2 * y, 1.0, 0.0)
    hi = resid * jnp.where(z == 2 * y + 1, 1.0, 0.0)
    mark("s6wait")
    finish()
    mark("oproj")
    prod = jnp.dot(
        r["att"][...].reshape(256, 512), r["wo"][...].reshape(512, 256), preferred_element_type=F32
    ) + jnp.concatenate([lo, hi], axis=1)
    for xl in range(2):
        for ys in range(NY):
            for j in range(2):
                at = [((m * 2 + xl) * 4 + ys) * 16 + j * 8 for m in range(2)]
                r["s7s"][xl * 4 + ys, j * 16 : j * 16 + 16, :] = jnp.concatenate(
                    [prod[a : a + 8] for a in at], axis=0
                ).astype(BF)
    mark("s7")
    z_send("s7", lambda zz: r["s7s"].at[zz], r["s7r"].at[z])
    r["s7r"][z] = r["s7s"][z]
    z_recv("s7", lambda zz: r["s7r"].at[zz])
    acc = r["s7r"][0].astype(F32)
    for s in range(1, NZ):
        acc = acc + r["s7r"][s].astype(F32)

    def z32(zz):
        return pl.ds(pl.multiple_of(zz * 32, 32), 32)

    r["mid"][n, z32(z), :] = acc.astype(BF)
    mark("s8")
    z_send("s8", lambda zz: r["mid"].at[n, z32(z)], r["mid"].at[n, z32(z)])
    r["accg"][...] = jnp.zeros((256, FFD), F32)
    r["accu"][...] = jnp.zeros((256, FFD), F32)
    r["ssq"][...] = jnp.zeros((256, 128), F32)
    for name in ("fi", "fh", "fo", "wg", "wd"):
        local[name].wait()
    z_recv("s8", lambda zz: r["mid"].at[n, z32(zz)])

    mark("gather1")
    near = (1, 3, 2)
    for d in (2, 1, 3):
        xx, yy = rem(x + d, NX), rem(y + d, NY)
        send("da", r["mid"].at[n], r["mid"].at[n], n, at_xy(xx, y), xx * 4 + y)
        send("da", r["mid"].at[n], r["mid"].at[n], n, at_xy(x, yy), x * 4 + yy)

    def ffn_chunk(m):
        v = r["mid"][m].astype(F32)
        r["ssq"][...] += v[:, :128] * v[:, :128] + v[:, 128:] * v[:, 128:]
        cols = pl.ds(pl.multiple_of(m * 256, 256), 256)
        g = r["gn"][1:2, cols]
        v4 = v.reshape(16, 2, 8, 256)
        for k, name in enumerate(("accg", "accu")):
            f = jnp.concatenate(
                [
                    (r["fi"][i, k : k + 1, cols] * g).reshape(1, 1, 1, 256)
                    for i in range(2)
                ],
                axis=1,
            )
            act = (v4 * f).reshape(256, 256).astype(BF)
            r[name][...] += lax.dot_general(
                act, r["wg"][k, :, cols], NT, preferred_element_type=F32
            )

    ffn_chunk(n)
    top, low = pl.ds(0, 128), pl.ds(128, 128)
    for d in near:
        xx = rem(x + d, NX)
        m = xx * 4 + y
        recv("da", r["mid"].at[m], m)
        for e in (2, 1, 3):
            yy = rem(y + e, NY)
            send("fa", r["mid"].at[m, top], r["mid"].at[m, top], m, at_xy(x, yy), m * 4 + e)
        yy = rem(y + d, NY)
        m = x * 4 + yy
        recv("da", r["mid"].at[m], m)
        for e in (2, 1, 3):
            xx = rem(x + e, NX)
            send("fb_", r["mid"].at[m, low], r["mid"].at[m, low], m, at_xy(xx, y), m * 4 + e)

    mark("lines")

    def line_step(i, carry):
        ffn_chunk(rem(x + 1 + i, NX) * 4 + y)
        ffn_chunk(x * 4 + rem(y + 1 + i, NY))
        return carry

    lax.fori_loop(0, 3, line_step, 0)

    mark("diag")

    def diag_step(i, carry):
        m = rem(x + 1 + i // 3, NX) * 4 + rem(y + 1 + i % 3, NY)
        recv("fa", r["mid"].at[m, top], m)
        recv("fb_", r["mid"].at[m, low], m)
        ffn_chunk(m)
        return carry

    lax.fori_loop(0, 9, diag_step, 0)
    mark("act")
    scale = lax.rsqrt(jnp.sum(r["ssq"][...], axis=1, keepdims=True) * (1.0 / D) + 1e-5)

    def by_member(k):
        return jnp.concatenate(
            [r["fh"][k, i : i + 1, :].reshape(1, 1, 1, FFD) for i in range(2)], axis=1
        )

    gate = (r["accg"][...] * scale).reshape(16, 2, 8, FFD) * by_member(0)
    up = (r["accu"][...] * scale).reshape(16, 2, 8, FFD) * by_member(1)
    hidden = gate / (1.0 + jnp.exp(-gate)) * up * by_member(2)
    r["hid"][...] = hidden.reshape(256, FFD).astype(BF)

    def chunk(ch):
        return pl.ds(pl.multiple_of(ch * CW, CW), CW)

    def high(ch):
        return pl.ds(pl.multiple_of(HALF + ch * CW, CW), CW)

    def a1(ch, xx):
        return copy(
            "a1", r["p3"].at[xx, :, :, chunk(ch)], r["r1a"].at[x, :, :, chunk(ch)],
            ch * 4 + x, at_xy(xx, y), ch * 4 + xx,
        )

    def b1(ch, yy):
        return copy(
            "b1", r["p3"].at[:, yy, :, high(ch)], r["r1b"].at[y, :, :, chunk(ch)],
            ch * 4 + y, at_xy(x, yy), ch * 4 + yy,
        )

    mark("down")

    def down_step(ch, carry):
        for cols in (chunk(ch), high(ch)):
            v = jnp.dot(r["hid"][...], r["wd"][:, cols], preferred_element_type=F32)
            r["p3"][:, :, :, cols] = v.astype(BF).reshape(NX, NY, 16, CW)
        for d in (2, 1, 3):
            a1(ch, rem(x + d, NX)).start()
            b1(ch, rem(y + d, NY)).start()
        return carry

    lax.fori_loop(0, NCH, down_step, 0)

    def a2(ch, yy):
        return copy(
            "a2", r["s2a"].at[yy, :, chunk(ch)], r["r2a"].at[y, :, chunk(ch)],
            ch * 4 + y, at_xy(x, yy), ch * 4 + yy,
        )

    def b2(ch, xx):
        return copy(
            "b2", r["s2b"].at[xx, :, chunk(ch)], r["r2b"].at[x, :, chunk(ch)],
            ch * 4 + x, at_xy(xx, y), ch * 4 + xx,
        )

    mark("rs1")

    def second_step(ch, carry):
        for d in near:
            xx = rem(x + d, NX)
            recv("a1", r["r1a"].at[xx, :, :, chunk(ch)], ch * 4 + xx)
        v = r["p3"][x, :, :, chunk(ch)].astype(F32)
        for d in near:
            v = v + r["r1a"][rem(x + d, NX), :, :, chunk(ch)].astype(F32)
        r["s2a"][:, :, chunk(ch)] = v.astype(BF)
        for d in (2, 1, 3):
            a2(ch, rem(y + d, NY)).start()
        for d in near:
            yy = rem(y + d, NY)
            recv("b1", r["r1b"].at[yy, :, :, chunk(ch)], ch * 4 + yy)
        v = r["p3"][:, y, :, high(ch)].astype(F32)
        for d in near:
            v = v + r["r1b"][rem(y + d, NY), :, :, chunk(ch)].astype(F32)
        r["s2b"][:, :, chunk(ch)] = v.astype(BF)
        for d in (2, 1, 3):
            b2(ch, rem(x + d, NX)).start()
        return carry

    lax.fori_loop(0, NCH, second_step, 0)
    mark("rs2wait")
    for ch in range(NCH):
        for d in near:
            yy = rem(y + d, NY)
            recv("a2", r["r2a"].at[yy, :, chunk(ch)], ch * 4 + yy)
            xx = rem(x + d, NX)
            recv("b2", r["r2b"].at[xx, :, chunk(ch)], ch * 4 + xx)

    mark("rs2sum")
    row16 = lax.broadcasted_iota(jnp.int32, (16, 128), 0)
    own_row = rem(row16, 8) == z
    tile16 = pl.ds(pl.multiple_of(n * 16, 16), 16)
    for b in range(32):
        own, got, me, count = (
            ("s2a", "r2a", y, NY) if b < 16 else ("s2b", "r2b", x, NX)
        )
        cols = slice((b % 16) * 128, (b % 16 + 1) * 128)
        v = r[own][me, :, cols].astype(F32)
        for d in near:
            v = v + r[got][rem(me + d, count), :, cols].astype(F32)
        at = slice(b * 128, (b + 1) * 128)
        v = v * jnp.where(row16 < 8, r["fo"][0:1, at], r["fo"][1:2, at])
        m = r["mid"][b // 2, tile16, (b % 2) * 128 : (b % 2 + 1) * 128].astype(F32)
        r["f3"][b * 16 : (b + 1) * 16, :] = v + jnp.where(own_row, m, 0.0)

    mark("s13")
    for zz in range(NZ):
        for m in range(2):
            r["s13s"][zz, m * 32 : (m + 1) * 32, :] = r["f3"][
                pl.ds(m * 8 + zz, 32, stride=16), :
            ].astype(BF)
    z_send("s13", lambda zz: r["s13s"].at[zz], r["s13r"].at[z])
    owned = [r["f3"][pl.ds(m * 8 + z, 32, stride=16), :] for m in range(2)]
    z_recv("s13", lambda zz: r["s13r"].at[zz])
    mark("finalnorm")
    both = jnp.zeros((32, 128), F32)
    for m in range(2):
        v = owned[m]
        for zz in zpeers:
            v = v + r["s13r"][zz, m * 32 : (m + 1) * 32, :].astype(F32)
        v = v.astype(BF).astype(F32)
        mean = jnp.sum(jnp.sum(v * v, axis=1, keepdims=True), axis=0, keepdims=True) * (1.0 / D)
        both = both + (v * lax.rsqrt(mean + 1e-5) * r["g3"][...]).astype(BF).astype(F32)
    r["fs"][...] = both

    def half(k):
        return pl.ds(pl.multiple_of(k * 16, 16), 16)

    mark("fx")
    send("fx", r["fs"].at[half(1 - c)], r["fr"], 0, partner)
    recv("fx", r["fr"], 0)
    r["fb"][n, z] = ((r["fs"][half(c), :] + r["fr"][...]) * 0.25).astype(BF)
    mark("s14")
    z_send("s14", lambda zz: r["fb"].at[n, z], r["fb"].at[n, z])
    local["lm"].wait()
    local["tg"].wait()
    wanted = jnp.broadcast_to(r["tg"][...].astype(F32), (B, B)).T[:, 0:1]
    z_recv("s14", lambda zz: r["fb"].at[n, zz])
    mark("s15")
    xy_send("s15", lambda m: r["fb"].at[n], r["fb"].at[n])
    xy_recv("s15", lambda m: r["fb"].at[m])
    mark("lhs")
    r["ff"][...] = r["fb"][...].reshape(2048, 128).astype(F32)
    for b in range(16):
        rows = [
            r["ff"][pl.ds(xl * 1024 + zz * 16 + b, 8, stride=128), :]
            for xl in range(2)
            for zz in range(NZ)
        ]
        r["lh"][:, b * 128 : (b + 1) * 128] = jnp.concatenate(rows, axis=0).astype(BF)
    mark("lmdot")
    r["lp"][...] = jnp.dot(r["lh"][...], r["lm"][...], preferred_element_type=F32)
    mark("lx")
    send("lx", r["lp"], r["lr"], 0, partner)
    recv("lx", r["lr"], 0)
    mean_f = r["lp"][...] + r["lr"][...]
    r["logits_o"][...] = mean_f.astype(BF)

    mark("stats")
    ids = (lax.broadcasted_iota(jnp.int32, (B, VD), 1) + t * VD).astype(F32)
    found = jnp.sum(jnp.where(ids == wanted, mean_f, 0.0), axis=1, keepdims=True)
    peak = jnp.max(mean_f, axis=1, keepdims=True)
    total = jnp.sum(jnp.exp(mean_f - peak), axis=1, keepdims=True)
    lane = lax.broadcasted_iota(jnp.int32, (B, B), 1)
    stat = jnp.where(lane == 0, peak, jnp.where(lane == 1, total, jnp.where(lane == 2, found, 0.0)))
    r["sz"][z] = stat.T[:8]

    def combine(ref, count):
        peaks = [ref[k, 0:1, :] for k in range(count)]
        top_ = peaks[0]
        for k in range(1, count):
            top_ = jnp.maximum(top_, peaks[k])
        tot = ref[0, 1:2, :] * jnp.exp(peaks[0] - top_)
        hit = ref[0, 2:3, :]
        for k in range(1, count):
            tot = tot + ref[k, 1:2, :] * jnp.exp(peaks[k] - top_)
            hit = hit + ref[k, 2:3, :]
        return top_, tot, hit

    mark("s16")
    z_send("s16", lambda zz: r["sz"].at[z], r["sz"].at[z])
    z_recv("s16", lambda zz: r["sz"].at[zz])
    a, b_, h = combine(r["sz"], NZ)
    r["sx"][n] = jnp.concatenate([a, b_, h, jnp.zeros((5, 128), F32)], axis=0)
    mark("s17")
    xy_send("s17", lambda m: r["sx"].at[n], r["sx"].at[n])
    xy_recv("s17", lambda m: r["sx"].at[m])
    a, b_, h = combine(r["sx"], NP)
    r["lp_o"][...] = h - (a + jnp.log(b_))

    mark("drain")
    for k in sends:
        k.wait_send()

    def drain(ch, carry):
        for d in near:
            a1(ch, rem(x + d, NX)).wait_send()
            b1(ch, rem(y + d, NY)).wait_send()
            a2(ch, rem(y + d, NY)).wait_send()
            b2(ch, rem(x + d, NX)).wait_send()
        return carry

    lax.fori_loop(0, NCH, drain, 0)
    mark(None)
    for name in debug:
        r["dbg_" + name][...] = r[name][...]


def body(
    stream_in, kv_cache, lengths, targets, norm_gains, w_qkv, w_out, w_gate_up, w_down, lm_head,
    fast_in, fast_hidden, fast_out, debug=(),
):
    freq = np.float32(500000.0) ** (-np.arange(64, dtype=np.float32) * 2.0 / 128)
    freq = jnp.asarray(np.concatenate([freq, freq])[None, :], F32)
    args = dict(
        stream=stream_in, kv=kv_cache, lengths=lengths, targets=targets.reshape(1, B),
        gains=norm_gains, wqkv=w_qkv.T, wout=w_out,
        wgu=w_gate_up.swapaxes(1, 2), wdown=w_down, lmh=lm_head,
        fin=fast_in, fhid=fast_hidden.swapaxes(0, 1), fout=fast_out, freq=freq,
    )
    outs = ["logits_o", "lp_o"] + ["dbg_" + k for k in debug]
    shapes = [jax.ShapeDtypeStruct((B, VD), BF), jax.ShapeDtypeStruct((1, B), F32)] + [
        jax.ShapeDtypeStruct(SCRATCH[k].shape, SCRATCH[k].dtype) for k in debug
    ]
    sems = {}
    for k, count in PHASES.items():
        sems["ss_" + k] = DMA((count,))
        sems["rs_" + k] = DMA((count,))
    sems["ls"] = DMA((len(LOCAL),))
    names = list(INPUTS) + outs + list(SCRATCH) + list(sems)
    import functools

    got = pl.pallas_call(
        functools.partial(kernel, names, debug),
        out_shape=shapes,
        in_specs=[
            pl.BlockSpec(memory_space=pltpu.SMEM if k == "lengths" else pl.ANY) for k in INPUTS
        ],
        out_specs=[pl.BlockSpec(memory_space=VM)] * len(outs),
        scratch_shapes=list(SCRATCH.values()) + list(sems.values()),
        compiler_params=pltpu.CompilerParams(
            collective_id=0, has_side_effects=True, vmem_limit_bytes=60 * 1024 * 1024
        ),
        name="step",
    )(*(args[k] for k in INPUTS))
    return (got[0], got[1].reshape(B), *got[2:])


MEMBER_TP = ("member", "tp_0", "tp_1", "tp_2")
TP = ("tp_0", "tp_1", "tp_2")
IN_SPECS = (
    P(MEMBER_TP, None), P(MEMBER_TP, None, None), P(), P(), P(), P(None, TP), P(TP, None),
    P(None, None, TP), P(TP, None), P(None, TP), P("member", None, None), P("member", None, TP),
    P("member", None),
)


def solution(mesh):
    split = Mesh(
        mesh.devices.reshape(mesh.shape["member"], NX, NZ, NY), ("member", "tp_0", "tp_1", "tp_2")
    )
    return jax.shard_map(
        body, mesh=split, in_specs=IN_SPECS, out_specs=(P(None, TP), P()), check_vma=False
    )
```

```python
import functools
from types import SimpleNamespace

import jax
import jax.numpy as jnp
import numpy as np
from jax import lax
from jax.experimental import pallas as pl
from jax.experimental.pallas import tpu as pltpu
from jax.sharding import Mesh
from jax.sharding import PartitionSpec as P

MESH = pl.DeviceIdType.MESH
F32 = jnp.float32
BF = jnp.bfloat16
NX, NZ, NY = 4, 8, 4
NP = NX * NY
D, HEADS, KV, HD, CACHE, FFD, VD = 4096, 32, 8, 128, 512, 112, 512
B = 128
QN = 384
ZORDER = (4, 3, 5, 2, 6, 1, 7)
NCH, CW = 4, 512
HALF = D // 2
NT = (((1,), (1,)), ((), ()))

VM = pltpu.VMEM
DMA = pltpu.SemaphoreType.DMA

SCRATCH = dict(
    st=VM((2, D), BF),
    kvv=VM((2, CACHE, 2 * KV * HD), BF),
    tg=VM((1, B), jnp.int32),
    gn=VM((3, D), F32),
    fi=VM((2, 2, D), F32),
    fh=VM((3, 2, FFD), F32),
    fo=VM((2, D), F32),
    fq=VM((1, 128), F32),
    wq=VM((NZ, 48, 512), BF),
    wo=VM((NP, 32, 256), BF),
    wg=VM((2, FFD, D), BF),
    wd=VM((FFD, D), BF),
    lm=VM((HALF, VD), BF),
    sc=VM((64, 128), F32),
    s1s=VM((64, 128), F32),
    s1r=VM((64, 128), F32),
    raw=VM((NP, 16, 512), BF),
    p1=VM((3, 256, 128), F32),
    s3s=VM((NZ, 32, QN), BF),
    s3r=VM((NZ, 32, QN), BF),
    q1=VM((3, 32, 128), F32),
    s4s=VM((128, 128), F32),
    s4r=VM((128, 128), F32),
    hs=VM((96, 128), F32),
    osc=VM((64, 128), F32),
    s5s=VM((64, 128), F32),
    s5r=VM((64, 128), F32),
    att=VM((NP, 16, 512), BF),
    s7s=VM((NZ, 32, 256), BF),
    s7r=VM((NZ, 32, 256), BF),
    mid=VM((NP, 256, 256), BF),
    accg=VM((256, FFD), F32),
    accu=VM((256, FFD), F32),
    ssq=VM((256, 128), F32),
    hid=VM((256, FFD), BF),
    p3=VM((NX, NY, 16, D), BF),
    r1a=VM((NX, NY, 16, HALF), BF),
    r1b=VM((NY, NX, 16, HALF), BF),
    s2a=VM((NY, 16, HALF), BF),
    s2b=VM((NX, 16, HALF), BF),
    r2a=VM((NY, 16, HALF), BF),
    r2b=VM((NX, 16, HALF), BF),
    f3=VM((512, 128), F32),
    g3=VM((32, 128), F32),
    s13s=VM((NZ, 64, 128), BF),
    s13r=VM((NZ, 64, 128), BF),
    fs=VM((32, 128), F32),
    fr=VM((16, 128), F32),
    fb=VM((NP, NZ, 16, 128), BF),
    ff=VM((2048, 128), F32),
    lh=VM((B, HALF), BF),
    lp=VM((B, VD), F32),
    lr=VM((B, VD), F32),
    sz=VM((NZ, 8, 128), F32),
    sx=VM((NP, 8, 128), F32),
)
PHASES = dict(
    wq=1, wqf=1, wo=1, s1=1, s2=1, s3=1, s4=1, s5=1, s6=1, s7=1, s8=1, da=6, dg=9,
    a1=NCH, b1=NCH, a2=1, b2=1, s13=1, fx=1, s14=1, s15=1, lx=1, s16=1, s17=1,
)
LS = dict(ls=DMA((16,)))
OUTS = dict(
    logits_o=jax.ShapeDtypeStruct((B, VD), BF), lp_o=jax.ShapeDtypeStruct((1, B), F32)
)


def kernel(inputs, *refs):
    names = [*inputs, *OUTS, *SCRATCH, *LS]
    r = SimpleNamespace(**dict(zip(names, refs)))
    sems = iter(refs[len(names) :])
    p = SimpleNamespace(**{k: (next(sems), next(sems)) for k in PHASES})
    c, x, z, y = (lax.axis_index(a) for a in MEMBER_TP)
    t = x * 32 + z * 4 + y
    n = x * 4 + y
    drains = []
    def rem(v, k):
        return lax.rem(v, k)

    def at_z(zz):
        return (c, x, zz, y)

    def at_xy(xx, yy):
        return (c, xx, z, yy)

    partner = (1 - c, x, z, y)

    def copy(phase, src, dst, dev, slot=0):
        return pltpu.make_async_remote_copy(
            src_ref=src,
            dst_ref=dst,
            send_sem=phase[0].at[0],
            recv_sem=phase[1].at[slot],
            device_id=dev,
            device_id_type=MESH,
        )

    def send(phase, src, dst, dev, slot=0):
        copy(phase, src, dst, dev, slot).start()

    def wait_bytes(sem, ref):
        pltpu.make_async_copy(ref, ref, sem).wait()

    def recv(phase, ref, slot=0):
        wait_bytes(phase[1].at[slot], ref)

    def sent(phase, ref):
        drains.append((phase[0].at[0], ref))

    zpeers = [rem(z + d, NZ) for d in ZORDER]
    plane = [
        (rem(x + dx, NX), rem(y + dy, NY))
        for dx, dy in sorted(
            ((a, b) for a in range(NX) for b in range(NY) if a or b),
            key=lambda p: -(min(p[0], 4 - p[0]) + min(p[1], 4 - p[1])),
        )
    ]

    def z_send(phase, src_at, dst):
        for zz in zpeers:
            send(phase, src_at(zz), dst, at_z(zz))

    def xy_send(phase, src_at, dst):
        for xx, yy in plane:
            send(phase, src_at(xx * 4 + yy), dst, at_xy(xx, yy))

    def done(phase, ref):
        recv(phase, ref)
        sent(phase, ref)

    bar = pltpu.get_barrier_semaphore()
    peers = [at_z(zz) for zz in zpeers] + [at_xy(*p) for p in plane] + [partner]
    for dev in peers:
        pl.semaphore_signal(bar, inc=1, device_id=dev, device_id_type=MESH)

    def qcols(zz, k):
        return r.wqkv.at[:, pl.ds(pl.multiple_of(k * 1024 + zz * 128, 128), 128)]

    def half_cols(k):
        return pl.ds(pl.multiple_of((2 * c + k) * 128, 128), 128)

    local = SimpleNamespace()
    begun = []

    def fetch(src, dst):
        k = pltpu.make_async_copy(src, dst, r.ls.at[len(begun)])
        k.start()
        begun.append(k)
        return k

    local.st = fetch(r.stream, r.st)
    local.gn = fetch(r.gains, r.gn)
    local.fq = fetch(r.freq, r.fq)
    local_wq = [fetch(qcols(z, 2 * c + k), r.wq.at[z, :, half_cols(k)]) for k in range(2)]
    local.wo = fetch(r.wout.at[:, pl.ds(pl.multiple_of(n * 256, 256), 256)], r.wo.at[n])
    local.kvv = fetch(r.kv, r.kvv)
    local.fi = fetch(r.fin, r.fi)
    local.fh = fetch(r.fhid, r.fh)
    local.fo = fetch(r.fout, r.fo)
    local.tg = fetch(r.targets, r.tg)
    local.wg = fetch(r.wgu, r.wg)
    local.wd = fetch(r.wdown, r.wd)
    local.lm = fetch(r.lmh.at[pl.ds(pl.multiple_of(c * HALF, HALF), HALF)], r.lm)

    def spread(scratch, dst):
        for zz in range(NZ):
            dst[zz * 8 : zz * 8 + 8] = scratch[pl.ds(zz, 8, stride=8), :]

    z8 = pl.ds(pl.multiple_of(z * 8, 8), 8)

    def z_then_plane(zphase, pphase, s, rr, buf, start=True):
        def piece(zz):
            return pl.ds(pl.multiple_of(zz * 8, 8), 8)

        if start:
            z_send(zphase, lambda zz: s.at[piece(zz)], rr.at[z8])
        rr[z8, :] = s[z8, :]
        done(zphase, rr.at[0:56])
        for k in range(4):
            rows = [rr[pl.ds(j * 4 + k, 8, stride=8), :] for j in range(2)]
            buf[n, :, k * 128 : (k + 1) * 128] = jnp.concatenate(rows, axis=0).astype(BF)
        xy_send(pphase, lambda m: buf.at[n], buf.at[n])
        return lambda: done(pphase, buf.at[0:15])

    local.st.wait()
    x32 = r.st[...].astype(F32)
    rs = lax.rsqrt(jnp.mean(x32 * x32, axis=-1, keepdims=True) + 1e-5)
    for b in range(32):
        for j in range(2):
            r.sc[j * 32 + b : j * 32 + b + 1, :] = x32[j : j + 1, b * 128 : (b + 1) * 128]
    spread(r.sc, r.s1s)
    r.s4s[...] = jnp.zeros((128, 128), F32)
    row8 = lax.broadcasted_iota(jnp.int32, (8, 128), 0)
    lane8 = lax.broadcasted_iota(jnp.int32, (8, 128), 1)
    rs8 = jnp.where(row8 < 4, rs[0:1, 0:1], rs[1:2, 0:1])

    pl.semaphore_wait(bar, len(peers))

    for zz in zpeers:
        send(p.s1, r.s1s.at[pl.ds(pl.multiple_of(zz * 8, 8), 8)], r.s1r.at[z8], at_z(zz))
    for zz in zpeers:
        for k in range(2):
            send(p.wq, qcols(zz, 2 * c + k), r.wq.at[z, :, half_cols(k)], at_z(zz))
    finish = z_then_plane(p.s1, p.s2, r.s1s, r.s1r, r.raw, False)
    xy_send(
        p.wo,
        lambda m: r.wout.at[:, pl.ds(pl.multiple_of(m * 256, 256), 256)],
        r.wo.at[n],
    )
    local.fq.wait()
    local.gn.wait()
    pos = [r.lengths[rem(2 * t + j, B)] for j in range(2)]
    ang = jnp.where(row8 < 4, pos[0], pos[1]).astype(F32) * r.fq[0:1, :]
    cos8 = jnp.cos(ang)
    sin8 = jnp.where(lane8 < 64, -jnp.sin(ang), jnp.sin(ang))
    for b in range(32):
        r.g3[b : b + 1, :] = r.gn[2:3, b * 128 : (b + 1) * 128]

    for k in range(2):
        local_wq[k].wait()
    done(p.wq, r.wq.at[0:7, :, 0:256])
    mine = r.wq.at[:, :, pl.ds(pl.multiple_of(c * 256, 256), 256)]
    send(p.wqf, mine, mine, partner)
    done(p.wqf, mine)
    gq = jnp.concatenate(
        [r.gn[0:1, pl.ds(pl.multiple_of(k * 1024 + z * 128, 128), 128)] for k in range(4)], axis=1
    )
    finish()
    lhs = (r.raw[...].reshape(256, 512).astype(F32) * gq).astype(BF)
    prod = lax.dot_general(lhs, r.wq[...].reshape(QN, 512), NT, preferred_element_type=F32)
    for l in range(3):
        r.p1[l] = prod[:, l * 128 : (l + 1) * 128]
    for zz in range(NZ):
        for l in range(3):
            r.s3s[zz, :, l * 128 : (l + 1) * 128] = r.p1.at[l][
                pl.ds(zz, 32, stride=8), :
            ].astype(BF)
    z_send(p.s3, lambda zz: r.s3s.at[zz], r.s3r.at[z])
    r.s3r[z] = r.s3s[z]
    done(p.s3, r.s3r.at[0:7])
    acc = r.s3r[0].astype(F32)
    for s in range(1, NZ):
        acc = acc + r.s3r[s].astype(F32)
    for l in range(3):
        r.q1[l] = acc[:, l * 128 : (l + 1) * 128]
    for l in range(3):
        for j in range(2):
            r.s4s[pl.ds(l * 2 + j, 16, stride=8), :] = r.q1.at[l][pl.ds(j, 16, stride=2), :]

    def tile(m):
        return pl.ds(pl.multiple_of(m * 8, 8), 8)

    xy_send(p.s4, lambda m: r.s4s.at[tile(m)], r.s4r.at[tile(n)])
    r.s4r[tile(n), :] = r.s4s[tile(n), :]
    done(p.s4, r.s4r.at[0:120])

    blocks = {
        (yy, l): jnp.concatenate(
            [r.s4r[pl.ds(yy * 8 + l * 2 + j, 4, stride=32), :] for j in range(2)], axis=0
        )
        for yy in range(NY)
        for l in range(3)
    }
    for hh in range(12):
        val = jnp.zeros((8, 128), F32)
        lane = 0
        while lane < 128:
            col = hh * 128 + lane
            tt, i = divmod(col, 48)
            at = (tt // 4) * 48 + i
            l, src = divmod(at, 128)
            width = min(48 - i, 128 - src, 128 - lane)
            piece = blocks[(tt % 4, l)]
            shift = (lane - src) % 128
            if shift:
                piece = pltpu.roll(piece, shift, 1)
            val = jnp.where((lane8 >= lane) & (lane8 < lane + width), piece, val)
            lane += width
        val = (val * rs8).astype(BF).astype(F32)
        turned = (val * cos8 + pltpu.roll(val, 64, 1) * sin8).astype(BF).astype(F32)
        if hh >= 4:
            turned = jnp.where(row8 % 4 == 3, val, turned)
        r.hs[pl.ds(hh, 8, stride=12), :] = turned

    local.kvv.wait()
    inv_root = HD**-0.5
    group = lax.broadcasted_iota(jnp.int32, (32, 128), 0) // 4
    group8 = (
        lax.broadcasted_iota(jnp.int32, (32, 8), 0) // 4
        == lax.broadcasted_iota(jnp.int32, (32, 8), 1)
    )
    place = lax.broadcasted_iota(jnp.int32, (32, CACHE), 1)
    for j in range(2):
        q = r.hs[j * 48 : j * 48 + 32, :]
        kn = r.hs[j * 48 + 32 : j * 48 + 40, :].astype(BF)
        vn = r.hs[j * 48 + 40 : j * 48 + 48, :].astype(BF)
        qd = jnp.concatenate([jnp.where(group == k, q, 0.0) for k in range(KV)], axis=1).astype(BF)
        scores = (
            lax.dot_general(qd, r.kvv[j, :, : KV * HD], NT, preferred_element_type=F32) * inv_root
        )
        fresh = lax.dot_general(q.astype(BF), kn, NT, preferred_element_type=F32)
        fresh = jnp.sum(jnp.where(group8, fresh, 0.0), axis=1, keepdims=True) * inv_root
        scores = jnp.where(place < pos[j], scores, -1e30)
        peak = jnp.maximum(jnp.max(scores, axis=1, keepdims=True), fresh)
        weights = jnp.exp(scores - peak)
        fresh_w = jnp.exp(fresh - peak)
        total = jnp.sum(weights, axis=1, keepdims=True) + fresh_w
        probs = (weights / total).astype(BF)
        fresh_p = jnp.where(group8, fresh_w / total, 0.0).astype(BF)
        wide = jnp.dot(probs, r.kvv[j, :, KV * HD :], preferred_element_type=F32)
        out = jnp.dot(fresh_p, vn, preferred_element_type=F32)
        for k in range(KV):
            out = out + jnp.where(group == k, wide[:, k * 128 : (k + 1) * 128], 0.0)
        r.osc[j * 32 : j * 32 + 32, :] = out.astype(BF).astype(F32)

    spread(r.osc, r.s5s)
    finish = z_then_plane(p.s5, p.s6, r.s5s, r.s5r, r.att)
    local.wo.wait()
    done(p.wo, r.wo.at[0:15])
    resid = r.raw[:, :, pl.ds(pl.multiple_of(x * 128, 128), 128)].reshape(256, 128).astype(F32)
    lo = resid * jnp.where(z == 2 * y, 1.0, 0.0)
    hi = resid * jnp.where(z == 2 * y + 1, 1.0, 0.0)
    finish()
    prod = jnp.dot(
        r.att[...].reshape(256, 512), r.wo[...].reshape(512, 256), preferred_element_type=F32
    ) + jnp.concatenate([lo, hi], axis=1)
    for xl in range(2):
        for ys in range(NY):
            for j in range(2):
                at = [((m * 2 + xl) * 4 + ys) * 16 + j * 8 for m in range(2)]
                r.s7s[xl * 4 + ys, j * 16 : j * 16 + 16, :] = jnp.concatenate(
                    [prod[a : a + 8] for a in at], axis=0
                ).astype(BF)
    z_send(p.s7, lambda zz: r.s7s.at[zz], r.s7r.at[z])
    r.s7r[z] = r.s7s[z]
    done(p.s7, r.s7r.at[0:7])
    acc = r.s7r[0].astype(F32)
    for s in range(1, NZ):
        acc = acc + r.s7r[s].astype(F32)

    def z32(zz):
        return pl.ds(pl.multiple_of(zz * 32, 32), 32)

    r.mid[n, z32(z), :] = acc.astype(BF)
    z_send(p.s8, lambda zz: r.mid.at[n, z32(z)], r.mid.at[n, z32(z)])
    r.accg[...] = jnp.zeros((256, FFD), F32)
    r.accu[...] = jnp.zeros((256, FFD), F32)
    r.ssq[...] = jnp.zeros((256, 128), F32)
    for k in (local.fi, local.fh, local.fo, local.wg, local.wd):
        k.wait()
    done(p.s8, r.mid.at[n, 0:224])

    near = (1, 3, 2)
    for d in (2, 1, 3):
        xx, yy = rem(x + d, NX), rem(y + d, NY)
        send(p.da, r.mid.at[n], r.mid.at[n], at_xy(xx, y), 3 - d)
        send(p.da, r.mid.at[n], r.mid.at[n], at_xy(x, yy), 6 - d)
    sent(p.da, r.mid.at[0:6])

    def ffn_chunk(m):
        v = r.mid[m].astype(F32)
        r.ssq[...] += v[:, :128] * v[:, :128] + v[:, 128:] * v[:, 128:]
        cols = pl.ds(pl.multiple_of(m * 256, 256), 256)
        g = r.gn[1:2, cols]
        v4 = v.reshape(16, 2, 8, 256)
        for k, total in enumerate((r.accg, r.accu)):
            f = jnp.concatenate(
                [
                    (r.fi[i, k : k + 1, cols] * g).reshape(1, 1, 1, 256)
                    for i in range(2)
                ],
                axis=1,
            )
            act = (v4 * f).reshape(256, 256).astype(BF)
            total[...] += lax.dot_general(
                act, r.wg[k, :, cols], NT, preferred_element_type=F32
            )

    ffn_chunk(n)
    top, low = pl.ds(0, 128), pl.ds(128, 128)
    for d in near:
        m = rem(x + d, NX) * 4 + y
        recv(p.da, r.mid.at[m], d - 1)
        for e in (2, 1, 3):
            yy = rem(y + e, NY)
            send(p.dg, r.mid.at[m, top], r.mid.at[m, top], at_xy(x, yy), (d - 1) * 3 + 3 - e)
        m = x * 4 + rem(y + d, NY)
        recv(p.da, r.mid.at[m], d + 2)
        for e in (2, 1, 3):
            xx = rem(x + e, NX)
            send(p.dg, r.mid.at[m, low], r.mid.at[m, low], at_xy(xx, y), (3 - e) * 3 + d - 1)
    sent(p.dg, r.mid.at[0:9])

    def line_step(i, carry):
        ffn_chunk(rem(x + 1 + i, NX) * 4 + y)
        ffn_chunk(x * 4 + rem(y + 1 + i, NY))
        return carry

    lax.fori_loop(0, 3, line_step, 0)

    def diag_step(i, carry):
        m = rem(x + 1 + i // 3, NX) * 4 + rem(y + 1 + i % 3, NY)
        recv(p.dg, r.mid.at[m], i)
        ffn_chunk(m)
        return carry

    lax.fori_loop(0, 9, diag_step, 0)
    scale = lax.rsqrt(jnp.sum(r.ssq[...], axis=1, keepdims=True) * (1.0 / D) + 1e-5)

    def by_member(k):
        return jnp.concatenate(
            [r.fh[k, i : i + 1, :].reshape(1, 1, 1, FFD) for i in range(2)], axis=1
        )

    gate = (r.accg[...] * scale).reshape(16, 2, 8, FFD) * by_member(0)
    up = (r.accu[...] * scale).reshape(16, 2, 8, FFD) * by_member(1)
    hidden = gate / (1.0 + jnp.exp(-gate)) * up * by_member(2)
    r.hid[...] = hidden.reshape(256, FFD).astype(BF)

    def chunk(ch):
        return pl.ds(pl.multiple_of(ch * CW, CW), CW)

    def high(ch):
        return pl.ds(pl.multiple_of(HALF + ch * CW, CW), CW)

    def a1(ch, xx):
        at = r.p3.at[xx, :, :, chunk(ch)]
        send(p.a1, at, r.r1a.at[x, :, :, chunk(ch)], at_xy(xx, y), ch)

    def b1(ch, yy):
        at = r.p3.at[:, yy, :, high(ch)]
        send(p.b1, at, r.r1b.at[y, :, :, chunk(ch)], at_xy(x, yy), ch)

    def down_step(ch, carry):
        for cols in (chunk(ch), high(ch)):
            v = jnp.dot(r.hid[...], r.wd[:, cols], preferred_element_type=F32)
            r.p3[:, :, :, cols] = v.astype(BF).reshape(NX, NY, 16, CW)
        for d in (2, 1, 3):
            a1(ch, rem(x + d, NX))
            b1(ch, rem(y + d, NY))
        return carry

    lax.fori_loop(0, NCH, down_step, 0)

    def a2(ch, yy):
        send(p.a2, r.s2a.at[yy, :, chunk(ch)], r.r2a.at[y, :, chunk(ch)], at_xy(x, yy))

    def b2(ch, xx):
        send(p.b2, r.s2b.at[xx, :, chunk(ch)], r.r2b.at[x, :, chunk(ch)], at_xy(xx, y))

    def second_step(ch, carry):
        recv(p.a1, r.r1a.at[0:3, :, :, chunk(ch)], ch)
        v = r.p3[x, :, :, chunk(ch)].astype(F32)
        for d in near:
            v = v + r.r1a[rem(x + d, NX), :, :, chunk(ch)].astype(F32)
        r.s2a[:, :, chunk(ch)] = v.astype(BF)
        for d in (2, 1, 3):
            a2(ch, rem(y + d, NY))
        recv(p.b1, r.r1b.at[0:3, :, :, chunk(ch)], ch)
        v = r.p3[:, y, :, high(ch)].astype(F32)
        for d in near:
            v = v + r.r1b[rem(y + d, NY), :, :, chunk(ch)].astype(F32)
        r.s2b[:, :, chunk(ch)] = v.astype(BF)
        for d in (2, 1, 3):
            b2(ch, rem(x + d, NX))
        return carry

    lax.fori_loop(0, NCH, second_step, 0)
    sent(p.a1, r.r1a.at[0:3])
    sent(p.b1, r.r1b.at[0:3])
    done(p.a2, r.r2a.at[0:3])
    done(p.b2, r.r2b.at[0:3])

    row16 = lax.broadcasted_iota(jnp.int32, (16, 128), 0)
    own_row = rem(row16, 8) == z
    tile16 = pl.ds(pl.multiple_of(n * 16, 16), 16)
    for b in range(32):
        own, got, me, count = (
            (r.s2a, r.r2a, y, NY) if b < 16 else (r.s2b, r.r2b, x, NX)
        )
        cols = slice((b % 16) * 128, (b % 16 + 1) * 128)
        v = own[me, :, cols].astype(F32)
        for d in near:
            v = v + got[rem(me + d, count), :, cols].astype(F32)
        at = slice(b * 128, (b + 1) * 128)
        v = v * jnp.where(row16 < 8, r.fo[0:1, at], r.fo[1:2, at])
        m = r.mid[b // 2, tile16, (b % 2) * 128 : (b % 2 + 1) * 128].astype(F32)
        r.f3[b * 16 : (b + 1) * 16, :] = v + jnp.where(own_row, m, 0.0)

    for zz in range(NZ):
        for m in range(2):
            r.s13s[zz, m * 32 : (m + 1) * 32, :] = r.f3[
                pl.ds(m * 8 + zz, 32, stride=16), :
            ].astype(BF)
    z_send(p.s13, lambda zz: r.s13s.at[zz], r.s13r.at[z])
    owned = [r.f3[pl.ds(m * 8 + z, 32, stride=16), :] for m in range(2)]
    done(p.s13, r.s13r.at[0:7])
    both = jnp.zeros((32, 128), F32)
    for m in range(2):
        v = owned[m]
        for zz in zpeers:
            v = v + r.s13r[zz, m * 32 : (m + 1) * 32, :].astype(F32)
        v = v.astype(BF).astype(F32)
        mean = jnp.sum(jnp.sum(v * v, axis=1, keepdims=True), axis=0, keepdims=True) * (1.0 / D)
        both = both + (v * lax.rsqrt(mean + 1e-5) * r.g3[...]).astype(BF).astype(F32)
    r.fs[...] = both

    def half(k):
        return pl.ds(pl.multiple_of(k * 16, 16), 16)

    send(p.fx, r.fs.at[half(1 - c)], r.fr, partner)
    done(p.fx, r.fr)
    r.fb[n, z] = ((r.fs[half(c), :] + r.fr[...]) * 0.25).astype(BF)
    z_send(p.s14, lambda zz: r.fb.at[n, z], r.fb.at[n, z])
    local.lm.wait()
    local.tg.wait()
    wanted = jnp.broadcast_to(r.tg[...].astype(F32), (B, B)).T[:, 0:1]
    done(p.s14, r.fb.at[n, 0:7])
    xy_send(p.s15, lambda m: r.fb.at[n], r.fb.at[n])
    done(p.s15, r.fb.at[0:15])
    r.ff[...] = r.fb[...].reshape(2048, 128).astype(F32)
    for b in range(16):
        rows = [
            r.ff[pl.ds(xl * 1024 + zz * 16 + b, 8, stride=128), :]
            for xl in range(2)
            for zz in range(NZ)
        ]
        r.lh[:, b * 128 : (b + 1) * 128] = jnp.concatenate(rows, axis=0).astype(BF)
    r.lp[...] = jnp.dot(r.lh[...], r.lm[...], preferred_element_type=F32)
    send(p.lx, r.lp, r.lr, partner)
    done(p.lx, r.lr)
    mean_f = r.lp[...] + r.lr[...]
    r.logits_o[...] = mean_f.astype(BF)

    ids = (lax.broadcasted_iota(jnp.int32, (B, VD), 1) + t * VD).astype(F32)
    found = jnp.sum(jnp.where(ids == wanted, mean_f, 0.0), axis=1, keepdims=True)
    peak = jnp.max(mean_f, axis=1, keepdims=True)
    total = jnp.sum(jnp.exp(mean_f - peak), axis=1, keepdims=True)
    lane = lax.broadcasted_iota(jnp.int32, (B, B), 1)
    stat = jnp.where(lane == 0, peak, jnp.where(lane == 1, total, jnp.where(lane == 2, found, 0.0)))
    r.sz[z] = stat.T[:8]

    def combine(ref, count):
        peaks = [ref[k, 0:1, :] for k in range(count)]
        top_ = peaks[0]
        for k in range(1, count):
            top_ = jnp.maximum(top_, peaks[k])
        tot = ref[0, 1:2, :] * jnp.exp(peaks[0] - top_)
        hit = ref[0, 2:3, :]
        for k in range(1, count):
            tot = tot + ref[k, 1:2, :] * jnp.exp(peaks[k] - top_)
            hit = hit + ref[k, 2:3, :]
        return top_, tot, hit

    z_send(p.s16, lambda zz: r.sz.at[z], r.sz.at[z])
    done(p.s16, r.sz.at[0:7])
    a, b_, h = combine(r.sz, NZ)
    r.sx[n] = jnp.concatenate([a, b_, h, jnp.zeros((5, 128), F32)], axis=0)
    xy_send(p.s17, lambda m: r.sx.at[n], r.sx.at[n])
    done(p.s17, r.sx.at[0:15])
    a, b_, h = combine(r.sx, NP)
    r.lp_o[...] = h - (a + jnp.log(b_))

    for sem, ref in drains:
        wait_bytes(sem, ref)


def body(
    stream_in, kv_cache, lengths, targets, norm_gains, w_qkv, w_out, w_gate_up, w_down, lm_head,
    fast_in, fast_hidden, fast_out,
):
    freq = np.float32(500000.0) ** (-np.arange(64, dtype=np.float32) * 2.0 / 128)
    freq = jnp.asarray(np.concatenate([freq, freq])[None, :], F32)
    args = dict(
        stream=stream_in, kv=kv_cache, lengths=lengths, targets=targets.reshape(1, B),
        gains=norm_gains, wqkv=w_qkv.T, wout=w_out,
        wgu=w_gate_up.swapaxes(1, 2), wdown=w_down, lmh=lm_head,
        fin=fast_in, fhid=fast_hidden.swapaxes(0, 1), fout=fast_out, freq=freq,
    )
    got = pl.pallas_call(
        functools.partial(kernel, list(args)),
        out_shape=list(OUTS.values()),
        in_specs=[
            pl.BlockSpec(memory_space=pltpu.SMEM if v is lengths else pl.ANY)
            for v in args.values()
        ],
        out_specs=[pl.BlockSpec(memory_space=VM)] * len(OUTS),
        scratch_shapes=[
            *SCRATCH.values(),
            *LS.values(),
            *(DMA((count,)) for n in PHASES.values() for count in (1, n)),
        ],
        compiler_params=pltpu.CompilerParams(
            collective_id=0, has_side_effects=True, vmem_limit_bytes=60 * 1024 * 1024
        ),
        name="step",
    )(*args.values())
    return (got[0], got[1].reshape(B))


MEMBER_TP = ("member", "tp_0", "tp_1", "tp_2")
TP = ("tp_0", "tp_1", "tp_2")
IN_SPECS = (
    P(MEMBER_TP, None), P(MEMBER_TP, None, None), P(), P(), P(), P(None, TP), P(TP, None),
    P(None, None, TP), P(TP, None), P(None, TP), P("member", None, None), P("member", None, TP),
    P("member", None),
)


def solution(mesh):
    split = Mesh(
        mesh.devices.reshape(mesh.shape["member"], NX, NZ, NY), MEMBER_TP
    )
    return jax.shard_map(
        body, mesh=split, in_specs=IN_SPECS, out_specs=(P(None, TP), P()), check_vma=False
    )
```

```python
import functools
from types import SimpleNamespace

import jax
import jax.numpy as jnp
import numpy as np
from jax import lax
from jax.experimental import pallas as pl
from jax.experimental.pallas import tpu as pltpu
from jax.sharding import Mesh
from jax.sharding import PartitionSpec as P

MESH = pl.DeviceIdType.MESH
F32 = jnp.float32
BF = jnp.bfloat16
NX, NZ, NY = 4, 8, 4
NP = NX * NY
D, HEADS, KV, HD, CACHE, FFD, VD = 4096, 32, 8, 128, 512, 112, 512
B = 128
QN = 384
ZORDER = (4, 3, 5, 2, 6, 1, 7)
NCH, CW = 4, 512
HALF = D // 2
NT = (((1,), (1,)), ((), ()))

VM = pltpu.VMEM
DMA = pltpu.SemaphoreType.DMA

SCRATCH = dict(
    st=VM((2, D), BF),
    kvv=VM((2, CACHE, 2 * KV * HD), BF),
    tg=VM((1, B), jnp.int32),
    gn=VM((3, D), F32),
    fi=VM((2, 2, D), F32),
    fh=VM((3, 2, FFD), F32),
    fo=VM((2, D), F32),
    fq=VM((1, 128), F32),
    wq=VM((NZ, 48, 512), BF),
    wo=VM((NP, 32, 256), BF),
    wg=VM((2, 256, D), BF),
    wd=VM((256, D), BF),
    fhx=VM((2, 3, 2, FFD), F32),
    fhp=VM((3, 2, 256), F32),
    lm=VM((HALF, VD), BF),
    sc=VM((64, 128), F32),
    s1s=VM((64, 128), F32),
    s1r=VM((64, 128), F32),
    raw=VM((NP, 16, 512), BF),
    p1=VM((3, 256, 128), F32),
    s3s=VM((NZ, 32, QN), BF),
    s3r=VM((NZ, 32, QN), BF),
    q1=VM((3, 32, 128), F32),
    s4s=VM((128, 128), F32),
    s4r=VM((128, 128), F32),
    hs=VM((96, 128), F32),
    osc=VM((64, 128), F32),
    s5s=VM((64, 128), F32),
    s5r=VM((64, 128), F32),
    att=VM((NP, 16, 512), BF),
    s7s=VM((NZ, 32, 256), BF),
    s7r=VM((NZ, 32, 256), BF),
    mc=VM((2, 128, 256), BF),
    xb=VM((NY, 64, 256), BF),
    mid=VM((NP, 128, 256), BF),
    accg=VM((128, 256), F32),
    accu=VM((128, 256), F32),
    ssq=VM((128, 128), F32),
    hid=VM((128, 256), BF),
    p3=VM((2, NY, 16, D), BF),
    r1a=VM((NY, 16, HALF), BF),
    r1b=VM((NY, 2, 16, HALF), BF),
    s2a=VM((NY, 16, HALF), BF),
    s2b=VM((2, 16, HALF), BF),
    r2a=VM((NY, 16, HALF), BF),
    r2b=VM((16, HALF), BF),
    f3=VM((512, 128), F32),
    g3=VM((32, 128), F32),
    s13s=VM((NZ, 64, 128), BF),
    s13r=VM((NZ, 64, 128), BF),
    fs=VM((32, 128), F32),
    fr=VM((16, 128), F32),
    fb=VM((NP, NZ, 16, 128), BF),
    ff=VM((2048, 128), F32),
    lh=VM((B, HALF), BF),
    lp=VM((B, VD), F32),
    lr=VM((B, VD), F32),
    sz=VM((NZ, 8, 128), F32),
    sx=VM((NP, 8, 128), F32),
)
PHASES = dict(
    wq=1, wqf=1, wo=1, s1=1, s2=1, s3=1, s4=1, s5=1, s6=1, s7=1, s8=1, da=6, db=3, dg=9,
    xg=2, xd=2, fg=2, fd=2, xh=2,
    a1=NCH, b1=NCH, a2=1, b2=1, s13=1, fx=1, s14=1, s15=1, lx=1, s16=1, s17=1,
)
LS = dict(ls=DMA((16,)))
OUTS = dict(
    logits_o=jax.ShapeDtypeStruct((B, VD), BF), lp_o=jax.ShapeDtypeStruct((1, B), F32)
)


def kernel(inputs, *refs):
    names = [*inputs, *OUTS, *SCRATCH, *LS]
    r = SimpleNamespace(**dict(zip(names, refs)))
    sems = iter(refs[len(names) :])
    p = SimpleNamespace(**{k: (next(sems), next(sems)) for k in PHASES})
    c, x, z, y = (lax.axis_index(a) for a in MEMBER_TP)
    t = x * 32 + z * 4 + y
    n = x * 4 + y
    xl, par = x // 2, lax.rem(x, 2)
    own = xl * 8 + y * 2 + par
    drains = []
    def rem(v, k):
        return lax.rem(v, k)

    def at_z(zz):
        return (c, x, zz, y)

    def at_xy(xx, yy):
        return (c, xx, z, yy)

    partner = (1 - c, x, z, y)

    def copy(phase, src, dst, dev, slot=0):
        return pltpu.make_async_remote_copy(
            src_ref=src,
            dst_ref=dst,
            send_sem=phase[0].at[0],
            recv_sem=phase[1].at[slot],
            device_id=dev,
            device_id_type=MESH,
        )

    def send(phase, src, dst, dev, slot=0):
        copy(phase, src, dst, dev, slot).start()

    def wait_bytes(sem, ref):
        pltpu.make_async_copy(ref, ref, sem).wait()

    def recv(phase, ref, slot=0):
        wait_bytes(phase[1].at[slot], ref)

    def sent(phase, ref):
        drains.append((phase[0].at[0], ref))

    zpeers = [rem(z + d, NZ) for d in ZORDER]
    plane = [
        (rem(x + dx, NX), rem(y + dy, NY))
        for dx, dy in sorted(
            ((a, b) for a in range(NX) for b in range(NY) if a or b),
            key=lambda p: -(min(p[0], 4 - p[0]) + min(p[1], 4 - p[1])),
        )
    ]

    def z_send(phase, src_at, dst):
        for zz in zpeers:
            send(phase, src_at(zz), dst, at_z(zz))

    def xy_send(phase, src_at, dst):
        for xx, yy in plane:
            send(phase, src_at(xx * 4 + yy), dst, at_xy(xx, yy))

    def done(phase, ref):
        recv(phase, ref)
        sent(phase, ref)

    bar = pltpu.get_barrier_semaphore()
    peers = [at_z(zz) for zz in zpeers] + [at_xy(*p) for p in plane] + [partner]
    for dev in peers:
        pl.semaphore_signal(bar, inc=1, device_id=dev, device_id_type=MESH)

    def qcols(zz, k):
        return r.wqkv.at[:, pl.ds(pl.multiple_of(k * 1024 + zz * 128, 128), 128)]

    def half_cols(k):
        return pl.ds(pl.multiple_of((2 * c + k) * 128, 128), 128)

    local = SimpleNamespace()
    begun = []

    def fetch(src, dst):
        k = pltpu.make_async_copy(src, dst, r.ls.at[len(begun)])
        k.start()
        begun.append(k)
        return k

    local.st = fetch(r.stream, r.st)
    local.gn = fetch(r.gains, r.gn)
    local.fq = fetch(r.freq, r.fq)
    local_wq = [fetch(qcols(z, 2 * c + k), r.wq.at[z, :, half_cols(k)]) for k in range(2)]
    local.wo = fetch(r.wout.at[:, pl.ds(pl.multiple_of(n * 256, 256), 256)], r.wo.at[n])
    local.kvv = fetch(r.kv, r.kvv)
    local.fi = fetch(r.fin, r.fi)
    local.fh = fetch(r.fhid, r.fh)
    local.fo = fetch(r.fout, r.fo)
    local.tg = fetch(r.targets, r.tg)
    local.wg = fetch(r.wgu, r.wg.at[:, 0:FFD])
    local.wd = fetch(r.wdown, r.wd.at[0:FFD])
    local.lm = fetch(r.lmh.at[pl.ds(pl.multiple_of(c * HALF, HALF), HALF)], r.lm)

    right, left = at_xy(rem(x + 1, NX), y), at_xy(rem(x + 3, NX), y)

    def weight_piece(i):
        cols = pl.ds(pl.multiple_of(c * HALF + i * 256, 256), 256)
        for dev, a, b in ((right, 0, 64), (left, 64, FFD)):
            g = r.wg.at[:, 128 + a : 128 + b, cols]
            send(p.xg, r.wgu.at[:, a:b, cols], g, dev, i // 4)
            send(p.xd, r.wdown.at[a:b, cols], r.wd.at[128 + a : 128 + b, cols], dev, i // 4)

    def pass_weights(g):
        cols = pl.ds(pl.multiple_of(c * HALF + g * 1024, 1024), 1024)
        for came, went, at in (
            (p.xg, p.fg, r.wg.at[:, 128 : 128 + FFD, cols]),
            (p.xd, p.fd, r.wd.at[128 : 128 + FFD, cols]),
        ):
            recv(came, at, g)
            send(went, at, at, partner, g)

    def spread(scratch, dst):
        for zz in range(NZ):
            dst[zz * 8 : zz * 8 + 8] = scratch[pl.ds(zz, 8, stride=8), :]

    z8 = pl.ds(pl.multiple_of(z * 8, 8), 8)

    def z_then_plane(zphase, pphase, s, rr, buf, start=True, beside=lambda: None):
        def piece(zz):
            return pl.ds(pl.multiple_of(zz * 8, 8), 8)

        if start:
            z_send(zphase, lambda zz: s.at[piece(zz)], rr.at[z8])
        beside()
        rr[z8, :] = s[z8, :]
        done(zphase, rr.at[0:56])
        for k in range(4):
            rows = [rr[pl.ds(j * 4 + k, 8, stride=8), :] for j in range(2)]
            buf[n, :, k * 128 : (k + 1) * 128] = jnp.concatenate(rows, axis=0).astype(BF)
        xy_send(pphase, lambda m: buf.at[n], buf.at[n])
        return lambda: done(pphase, buf.at[0:15])

    local.st.wait()
    x32 = r.st[...].astype(F32)
    rs = lax.rsqrt(jnp.mean(x32 * x32, axis=-1, keepdims=True) + 1e-5)
    for b in range(32):
        for j in range(2):
            r.sc[j * 32 + b : j * 32 + b + 1, :] = x32[j : j + 1, b * 128 : (b + 1) * 128]
    spread(r.sc, r.s1s)
    r.s4s[...] = jnp.zeros((128, 128), F32)
    row8 = lax.broadcasted_iota(jnp.int32, (8, 128), 0)
    lane8 = lax.broadcasted_iota(jnp.int32, (8, 128), 1)
    rs8 = jnp.where(row8 < 4, rs[0:1, 0:1], rs[1:2, 0:1])

    pl.semaphore_wait(bar, len(peers))

    for zz in zpeers:
        send(p.s1, r.s1s.at[pl.ds(pl.multiple_of(zz * 8, 8), 8)], r.s1r.at[z8], at_z(zz))
    for zz in zpeers:
        for k in range(2):
            send(p.wq, qcols(zz, 2 * c + k), r.wq.at[z, :, half_cols(k)], at_z(zz))
    weight_piece(0)
    weight_piece(1)
    send(p.xh, r.fhid, r.fhx.at[0], right, 0)
    send(p.xh, r.fhid, r.fhx.at[1], left, 1)
    finish = z_then_plane(p.s1, p.s2, r.s1s, r.s1r, r.raw, False)
    xy_send(
        p.wo,
        lambda m: r.wout.at[:, pl.ds(pl.multiple_of(m * 256, 256), 256)],
        r.wo.at[n],
    )
    local.fq.wait()
    local.gn.wait()
    pos = [r.lengths[rem(2 * t + j, B)] for j in range(2)]
    ang = jnp.where(row8 < 4, pos[0], pos[1]).astype(F32) * r.fq[0:1, :]
    cos8 = jnp.cos(ang)
    sin8 = jnp.where(lane8 < 64, -jnp.sin(ang), jnp.sin(ang))
    for b in range(32):
        r.g3[b : b + 1, :] = r.gn[2:3, b * 128 : (b + 1) * 128]

    for k in range(2):
        local_wq[k].wait()
    done(p.wq, r.wq.at[0:7, :, 0:256])
    mine = r.wq.at[:, :, pl.ds(pl.multiple_of(c * 256, 256), 256)]
    send(p.wqf, mine, mine, partner)
    done(p.wqf, mine)
    gq = jnp.concatenate(
        [r.gn[0:1, pl.ds(pl.multiple_of(k * 1024 + z * 128, 128), 128)] for k in range(4)], axis=1
    )
    finish()
    lhs = (r.raw[...].reshape(256, 512).astype(F32) * gq).astype(BF)
    prod = lax.dot_general(lhs, r.wq[...].reshape(QN, 512), NT, preferred_element_type=F32)
    for l in range(3):
        r.p1[l] = prod[:, l * 128 : (l + 1) * 128]
    for zz in range(NZ):
        for l in range(3):
            r.s3s[zz, :, l * 128 : (l + 1) * 128] = r.p1.at[l][
                pl.ds(zz, 32, stride=8), :
            ].astype(BF)
    z_send(p.s3, lambda zz: r.s3s.at[zz], r.s3r.at[z])
    weight_piece(2)
    weight_piece(3)
    r.s3r[z] = r.s3s[z]
    done(p.s3, r.s3r.at[0:7])
    acc = r.s3r[0].astype(F32)
    for s in range(1, NZ):
        acc = acc + r.s3r[s].astype(F32)
    for l in range(3):
        r.q1[l] = acc[:, l * 128 : (l + 1) * 128]
    for l in range(3):
        for j in range(2):
            r.s4s[pl.ds(l * 2 + j, 16, stride=8), :] = r.q1.at[l][pl.ds(j, 16, stride=2), :]

    def tile(m):
        return pl.ds(pl.multiple_of(m * 8, 8), 8)

    xy_send(p.s4, lambda m: r.s4s.at[tile(m)], r.s4r.at[tile(n)])
    r.s4r[tile(n), :] = r.s4s[tile(n), :]
    done(p.s4, r.s4r.at[0:120])

    blocks = {
        (yy, l): jnp.concatenate(
            [r.s4r[pl.ds(yy * 8 + l * 2 + j, 4, stride=32), :] for j in range(2)], axis=0
        )
        for yy in range(NY)
        for l in range(3)
    }
    for hh in range(12):
        val = jnp.zeros((8, 128), F32)
        lane = 0
        while lane < 128:
            col = hh * 128 + lane
            tt, i = divmod(col, 48)
            at = (tt // 4) * 48 + i
            l, src = divmod(at, 128)
            width = min(48 - i, 128 - src, 128 - lane)
            piece = blocks[(tt % 4, l)]
            shift = (lane - src) % 128
            if shift:
                piece = pltpu.roll(piece, shift, 1)
            val = jnp.where((lane8 >= lane) & (lane8 < lane + width), piece, val)
            lane += width
        val = (val * rs8).astype(BF).astype(F32)
        turned = (val * cos8 + pltpu.roll(val, 64, 1) * sin8).astype(BF).astype(F32)
        if hh >= 4:
            turned = jnp.where(row8 % 4 == 3, val, turned)
        r.hs[pl.ds(hh, 8, stride=12), :] = turned

    local.kvv.wait()
    inv_root = HD**-0.5
    group = lax.broadcasted_iota(jnp.int32, (32, 128), 0) // 4
    group8 = (
        lax.broadcasted_iota(jnp.int32, (32, 8), 0) // 4
        == lax.broadcasted_iota(jnp.int32, (32, 8), 1)
    )
    place = lax.broadcasted_iota(jnp.int32, (32, CACHE), 1)
    for j in range(2):
        q = r.hs[j * 48 : j * 48 + 32, :]
        kn = r.hs[j * 48 + 32 : j * 48 + 40, :].astype(BF)
        vn = r.hs[j * 48 + 40 : j * 48 + 48, :].astype(BF)
        qd = jnp.concatenate([jnp.where(group == k, q, 0.0) for k in range(KV)], axis=1).astype(BF)
        scores = (
            lax.dot_general(qd, r.kvv[j, :, : KV * HD], NT, preferred_element_type=F32) * inv_root
        )
        fresh = lax.dot_general(q.astype(BF), kn, NT, preferred_element_type=F32)
        fresh = jnp.sum(jnp.where(group8, fresh, 0.0), axis=1, keepdims=True) * inv_root
        scores = jnp.where(place < pos[j], scores, -1e30)
        peak = jnp.maximum(jnp.max(scores, axis=1, keepdims=True), fresh)
        weights = jnp.exp(scores - peak)
        fresh_w = jnp.exp(fresh - peak)
        total = jnp.sum(weights, axis=1, keepdims=True) + fresh_w
        probs = (weights / total).astype(BF)
        fresh_p = jnp.where(group8, fresh_w / total, 0.0).astype(BF)
        wide = jnp.dot(probs, r.kvv[j, :, KV * HD :], preferred_element_type=F32)
        out = jnp.dot(fresh_p, vn, preferred_element_type=F32)
        for k in range(KV):
            out = out + jnp.where(group == k, wide[:, k * 128 : (k + 1) * 128], 0.0)
        r.osc[j * 32 : j * 32 + 32, :] = out.astype(BF).astype(F32)

    spread(r.osc, r.s5s)

    def beside():
        weight_piece(4)
        weight_piece(5)

    finish = z_then_plane(p.s5, p.s6, r.s5s, r.s5r, r.att, beside=beside)
    pass_weights(0)
    local.wo.wait()
    done(p.wo, r.wo.at[0:15])
    resid = r.raw[:, :, pl.ds(pl.multiple_of(x * 128, 128), 128)].reshape(256, 128).astype(F32)
    lo = resid * jnp.where(z == 2 * y, 1.0, 0.0)
    hi = resid * jnp.where(z == 2 * y + 1, 1.0, 0.0)
    finish()
    prod = jnp.dot(
        r.att[...].reshape(256, 512), r.wo[...].reshape(512, 256), preferred_element_type=F32
    ) + jnp.concatenate([lo, hi], axis=1)
    for h in range(2):
        for ys in range(NY):
            for j in range(2):
                at = [((m * 2 + h) * 4 + ys) * 16 + j * 8 for m in range(2)]
                r.s7s[h * 4 + ys, j * 16 : j * 16 + 16, :] = jnp.concatenate(
                    [prod[a : a + 8] for a in at], axis=0
                ).astype(BF)
    z_send(p.s7, lambda zz: r.s7s.at[zz], r.s7r.at[z])
    weight_piece(6)
    weight_piece(7)
    r.s7r[z] = r.s7s[z]
    done(p.s7, r.s7r.at[0:7])
    acc = r.s7r[0].astype(F32)
    for s in range(1, NZ):
        acc = acc + r.s7r[s].astype(F32)

    z16 = pl.ds(pl.multiple_of(z * 16, 16), 16)
    for j in range(2):
        r.mc[j, z16, :] = acc[j * 16 : j * 16 + 16].astype(BF)
    z_send(p.s8, lambda zz: r.mc.at[:, z16], r.mc.at[:, z16])
    r.accg[...] = jnp.zeros((128, 256), F32)
    r.accu[...] = jnp.zeros((128, 256), F32)
    r.ssq[...] = jnp.zeros((128, 128), F32)
    for a in (FFD, 128 + FFD):
        r.wg[:, a : a + 16, :] = jnp.zeros((2, 16, D), BF)
        r.wd[a : a + 16, :] = jnp.zeros((16, D), BF)
    recv(p.xh, r.fhx.at[0], 0)
    recv(p.xh, r.fhx.at[1], 1)
    sent(p.xh, r.fhx)
    local.fh.wait()
    r.fhp[...] = jnp.zeros((3, 2, 256), F32)
    r.fhp[:, :, 0:FFD] = r.fh[...]
    lane_h = lax.broadcasted_iota(jnp.int32, (3, 2, FFD), 2)
    r.fhp[:, :, 128 : 128 + FFD] = jnp.where(lane_h < 64, r.fhx[0], r.fhx[1])
    pass_weights(1)
    mine_g = r.wg.at[:, 128 : 128 + FFD, 0:HALF]
    mine_d = r.wd.at[128 : 128 + FFD, 0:HALF]
    for k in (p.xg, p.fg):
        sent(k, mine_g)
    for k in (p.xd, p.fd):
        sent(k, mine_d)
    for k in (local.fi, local.fo, local.wg, local.wd):
        k.wait()
    done(p.s8, r.mc.at[:, 0:112])

    near = (1, 3, 2)
    top, low = pl.ds(0, 64), pl.ds(64, 64)
    for d in (2, 1, 3):
        xx, yy = rem(x + d, NX), rem(y + d, NY)
        send(p.da, r.mc.at[rem(xx, 2)], r.mid.at[n], at_xy(xx, y), 3 - d)
        send(p.da, r.mc.at[par], r.mid.at[n], at_xy(x, yy), 6 - d)
        send(p.db, r.mc.at[1 - par, low], r.xb.at[y], at_xy(x, yy), 3 - d)
    sent(p.da, r.mid.at[0:6])
    sent(p.db, r.xb.at[0:3])
    r.mid[n] = r.mc[par]
    for g in range(2):
        cols = pl.ds(pl.multiple_of((1 - c) * HALF + g * 1024, 1024), 1024)
        recv(p.fg, r.wg.at[:, 128 : 128 + FFD, cols], g)
        recv(p.fd, r.wd.at[128 : 128 + FFD, cols], g)

    def ffn_chunk(m):
        v = r.mid[m].astype(F32)
        r.ssq[...] += v[:, :128] * v[:, :128] + v[:, 128:] * v[:, 128:]
        cols = pl.ds(pl.multiple_of(m * 256, 256), 256)
        g = r.gn[1:2, cols]
        v4 = v.reshape(8, 2, 8, 256)
        for k, total in enumerate((r.accg, r.accu)):
            f = jnp.concatenate(
                [
                    (r.fi[i, k : k + 1, cols] * g).reshape(1, 1, 1, 256)
                    for i in range(2)
                ],
                axis=1,
            )
            act = (v4 * f).reshape(128, 256).astype(BF)
            total[...] += lax.dot_general(
                act, r.wg[k, :, cols], NT, preferred_element_type=F32
            )

    ffn_chunk(n)
    for d in near:
        m = rem(x + d, NX) * 4 + y
        recv(p.da, r.mid.at[m], d - 1)
        for e in (2, 1, 3):
            yy = rem(y + e, NY)
            send(p.dg, r.mid.at[m, top], r.mid.at[m, top], at_xy(x, yy), (d - 1) * 3 + 3 - e)
        yy = rem(y + d, NY)
        m = x * 4 + yy
        recv(p.da, r.mid.at[m], d + 2)
        recv(p.db, r.xb.at[yy], d - 1)
        for e in (2, 1, 3):
            xx = rem(x + e, NX)
            at = r.mid.at[m, low] if e == 2 else r.xb.at[yy]
            send(p.dg, at, r.mid.at[m, low], at_xy(xx, y), (3 - e) * 3 + d - 1)
    sent(p.dg, r.mid.at[0:9])

    def line_step(i, carry):
        ffn_chunk(rem(x + 1 + i, NX) * 4 + y)
        ffn_chunk(x * 4 + rem(y + 1 + i, NY))
        return carry

    lax.fori_loop(0, 3, line_step, 0)

    def diag_step(i, carry):
        m = rem(x + 1 + i // 3, NX) * 4 + rem(y + 1 + i % 3, NY)
        recv(p.dg, r.mid.at[m], i)
        ffn_chunk(m)
        return carry

    lax.fori_loop(0, 9, diag_step, 0)
    scale = lax.rsqrt(jnp.sum(r.ssq[...], axis=1, keepdims=True) * (1.0 / D) + 1e-5)

    def by_member(k):
        return jnp.concatenate(
            [r.fhp[k, i : i + 1, :].reshape(1, 1, 1, 256) for i in range(2)], axis=1
        )

    gate = (r.accg[...] * scale).reshape(8, 2, 8, 256) * by_member(0)
    up = (r.accu[...] * scale).reshape(8, 2, 8, 256) * by_member(1)
    hidden = gate / (1.0 + jnp.exp(-gate)) * up * by_member(2)
    r.hid[...] = hidden.reshape(128, 256).astype(BF)

    def chunk(ch):
        return pl.ds(pl.multiple_of(ch * CW, CW), CW)

    def high(ch):
        return pl.ds(pl.multiple_of(HALF + ch * CW, CW), CW)

    other = 1 - xl
    opposite = at_xy(rem(x + 2, NX), y)

    def a1(ch):
        send(p.a1, r.p3.at[other, :, :, chunk(ch)], r.r1a.at[:, :, chunk(ch)], opposite, ch)

    def b1(ch, yy):
        at = r.p3.at[:, yy, :, high(ch)]
        send(p.b1, at, r.r1b.at[y, :, :, chunk(ch)], at_xy(x, yy), ch)

    def down_step(ch, carry):
        for cols in (chunk(ch), high(ch)):
            v = jnp.dot(r.hid[...], r.wd[:, cols], preferred_element_type=F32)
            r.p3[:, :, :, cols] = v.astype(BF).reshape(2, NY, 16, CW)
        a1(ch)
        for d in (2, 1, 3):
            b1(ch, rem(y + d, NY))
        return carry

    lax.fori_loop(0, NCH, down_step, 0)

    def a2(ch, yy):
        send(p.a2, r.s2a.at[yy, :, chunk(ch)], r.r2a.at[y, :, chunk(ch)], at_xy(x, yy))

    def b2(ch):
        send(p.b2, r.s2b.at[other, :, chunk(ch)], r.r2b.at[:, chunk(ch)], opposite)

    def second_step(ch, carry):
        recv(p.a1, r.r1a.at[:, :, chunk(ch)], ch)
        v = r.p3[xl, :, :, chunk(ch)].astype(F32) + r.r1a[:, :, chunk(ch)].astype(F32)
        r.s2a[:, :, chunk(ch)] = v.astype(BF)
        for d in (2, 1, 3):
            a2(ch, rem(y + d, NY))
        recv(p.b1, r.r1b.at[0:3, :, :, chunk(ch)], ch)
        v = r.p3[:, y, :, high(ch)].astype(F32)
        for d in near:
            v = v + r.r1b[rem(y + d, NY), :, :, chunk(ch)].astype(F32)
        r.s2b[:, :, chunk(ch)] = v.astype(BF)
        b2(ch)
        return carry

    lax.fori_loop(0, NCH, second_step, 0)
    sent(p.a1, r.r1a)
    sent(p.b1, r.r1b.at[0:3])
    done(p.a2, r.r2a.at[0:3])
    done(p.b2, r.r2b)

    row16 = lax.broadcasted_iota(jnp.int32, (16, 128), 0)
    own_row = rem(row16, 8) == z
    tile16 = pl.ds(pl.multiple_of((xl * 4 + y) * 16, 16), 16)
    for b in range(32):
        cols = slice((b % 16) * 128, (b % 16 + 1) * 128)
        if b < 16:
            v = r.s2a[y, :, cols].astype(F32)
            for d in near:
                v = v + r.r2a[rem(y + d, NY), :, cols].astype(F32)
        else:
            v = r.s2b[xl, :, cols].astype(F32) + r.r2b[:, cols].astype(F32)
        at = slice(b * 128, (b + 1) * 128)
        v = v * jnp.where(row16 < 8, r.fo[0:1, at], r.fo[1:2, at])
        m = r.mid[b // 2, tile16, (b % 2) * 128 : (b % 2 + 1) * 128].astype(F32)
        r.f3[b * 16 : (b + 1) * 16, :] = v + jnp.where(own_row, m, 0.0)

    for zz in range(NZ):
        for m in range(2):
            r.s13s[zz, m * 32 : (m + 1) * 32, :] = r.f3[
                pl.ds(m * 8 + zz, 32, stride=16), :
            ].astype(BF)
    z_send(p.s13, lambda zz: r.s13s.at[zz], r.s13r.at[z])
    owned = [r.f3[pl.ds(m * 8 + z, 32, stride=16), :] for m in range(2)]
    done(p.s13, r.s13r.at[0:7])
    both = jnp.zeros((32, 128), F32)
    for m in range(2):
        v = owned[m]
        for zz in zpeers:
            v = v + r.s13r[zz, m * 32 : (m + 1) * 32, :].astype(F32)
        v = v.astype(BF).astype(F32)
        mean = jnp.sum(jnp.sum(v * v, axis=1, keepdims=True), axis=0, keepdims=True) * (1.0 / D)
        both = both + (v * lax.rsqrt(mean + 1e-5) * r.g3[...]).astype(BF).astype(F32)
    r.fs[...] = both

    def half(k):
        return pl.ds(pl.multiple_of(k * 16, 16), 16)

    send(p.fx, r.fs.at[half(1 - c)], r.fr, partner)
    done(p.fx, r.fr)
    r.fb[own, z] = ((r.fs[half(c), :] + r.fr[...]) * 0.25).astype(BF)
    z_send(p.s14, lambda zz: r.fb.at[own, z], r.fb.at[own, z])
    local.lm.wait()
    local.tg.wait()
    wanted = jnp.broadcast_to(r.tg[...].astype(F32), (B, B)).T[:, 0:1]
    done(p.s14, r.fb.at[own, 0:7])
    xy_send(p.s15, lambda m: r.fb.at[own], r.fb.at[own])
    done(p.s15, r.fb.at[0:15])
    r.ff[...] = r.fb[...].reshape(2048, 128).astype(F32)
    for b in range(16):
        rows = [
            r.ff[pl.ds(h * 1024 + zz * 16 + b, 8, stride=128), :]
            for h in range(2)
            for zz in range(NZ)
        ]
        r.lh[:, b * 128 : (b + 1) * 128] = jnp.concatenate(rows, axis=0).astype(BF)
    r.lp[...] = jnp.dot(r.lh[...], r.lm[...], preferred_element_type=F32)
    send(p.lx, r.lp, r.lr, partner)
    done(p.lx, r.lr)
    mean_f = r.lp[...] + r.lr[...]
    r.logits_o[...] = mean_f.astype(BF)

    ids = (lax.broadcasted_iota(jnp.int32, (B, VD), 1) + t * VD).astype(F32)
    found = jnp.sum(jnp.where(ids == wanted, mean_f, 0.0), axis=1, keepdims=True)
    peak = jnp.max(mean_f, axis=1, keepdims=True)
    total = jnp.sum(jnp.exp(mean_f - peak), axis=1, keepdims=True)
    lane = lax.broadcasted_iota(jnp.int32, (B, B), 1)
    stat = jnp.where(lane == 0, peak, jnp.where(lane == 1, total, jnp.where(lane == 2, found, 0.0)))
    r.sz[z] = stat.T[:8]

    def combine(ref, count):
        peaks = [ref[k, 0:1, :] for k in range(count)]
        top_ = peaks[0]
        for k in range(1, count):
            top_ = jnp.maximum(top_, peaks[k])
        tot = ref[0, 1:2, :] * jnp.exp(peaks[0] - top_)
        hit = ref[0, 2:3, :]
        for k in range(1, count):
            tot = tot + ref[k, 1:2, :] * jnp.exp(peaks[k] - top_)
            hit = hit + ref[k, 2:3, :]
        return top_, tot, hit

    z_send(p.s16, lambda zz: r.sz.at[z], r.sz.at[z])
    done(p.s16, r.sz.at[0:7])
    a, b_, h = combine(r.sz, NZ)
    r.sx[n] = jnp.concatenate([a, b_, h, jnp.zeros((5, 128), F32)], axis=0)
    xy_send(p.s17, lambda m: r.sx.at[n], r.sx.at[n])
    done(p.s17, r.sx.at[0:15])
    a, b_, h = combine(r.sx, NP)
    r.lp_o[...] = h - (a + jnp.log(b_))

    for sem, ref in drains:
        wait_bytes(sem, ref)


def body(
    stream_in, kv_cache, lengths, targets, norm_gains, w_qkv, w_out, w_gate_up, w_down, lm_head,
    fast_in, fast_hidden, fast_out,
):
    freq = np.float32(500000.0) ** (-np.arange(64, dtype=np.float32) * 2.0 / 128)
    freq = jnp.asarray(np.concatenate([freq, freq])[None, :], F32)
    args = dict(
        stream=stream_in, kv=kv_cache, lengths=lengths, targets=targets.reshape(1, B),
        gains=norm_gains, wqkv=w_qkv.T, wout=w_out,
        wgu=w_gate_up.swapaxes(1, 2), wdown=w_down, lmh=lm_head,
        fin=fast_in, fhid=fast_hidden.swapaxes(0, 1), fout=fast_out, freq=freq,
    )
    got = pl.pallas_call(
        functools.partial(kernel, list(args)),
        out_shape=list(OUTS.values()),
        in_specs=[
            pl.BlockSpec(memory_space=pltpu.SMEM if v is lengths else pl.ANY)
            for v in args.values()
        ],
        out_specs=[pl.BlockSpec(memory_space=VM)] * len(OUTS),
        scratch_shapes=[
            *SCRATCH.values(),
            *LS.values(),
            *(DMA((count,)) for n in PHASES.values() for count in (1, n)),
        ],
        compiler_params=pltpu.CompilerParams(
            collective_id=0, has_side_effects=True, vmem_limit_bytes=60 * 1024 * 1024
        ),
        name="step",
    )(*args.values())
    return (got[0], got[1].reshape(B))


MEMBER_TP = ("member", "tp_0", "tp_1", "tp_2")
TP = ("tp_0", "tp_1", "tp_2")
IN_SPECS = (
    P(MEMBER_TP, None), P(MEMBER_TP, None, None), P(), P(), P(), P(None, TP), P(TP, None),
    P(None, None, TP), P(TP, None), P(None, TP), P("member", None, None), P("member", None, TP),
    P("member", None),
)


def solution(mesh):
    split = Mesh(
        mesh.devices.reshape(mesh.shape["member"], NX, NZ, NY), MEMBER_TP
    )
    return jax.shard_map(
        body, mesh=split, in_specs=IN_SPECS, out_specs=(P(None, TP), P()), check_vma=False
    )
```

```python
import functools
from types import SimpleNamespace

import jax
import jax.numpy as jnp
import numpy as np
from jax import lax
from jax.experimental import pallas as pl
from jax.experimental.pallas import tpu as pltpu
from jax.sharding import Mesh
from jax.sharding import PartitionSpec as P

MESH = pl.DeviceIdType.MESH
F32 = jnp.float32
BF = jnp.bfloat16
NX, NZ, NY = 4, 8, 4
NP = NX * NY
D, HEADS, KV, HD, CACHE, FFD, VD = 4096, 32, 8, 128, 512, 112, 512
B = 128
QN = 384
ZORDER = (4, 3, 5, 2, 6, 1, 7)
NCH, CW = 4, 512
HALF = D // 2
NT = (((1,), (1,)), ((), ()))

VM = pltpu.VMEM
DMA = pltpu.SemaphoreType.DMA

SCRATCH = dict(
    st=VM((2, D), BF),
    kvv=VM((2, CACHE, 2 * KV * HD), BF),
    tg=VM((1, B), jnp.int32),
    gn=VM((3, D), F32),
    fi=VM((2, 2, D), F32),
    fh=VM((3, 2, FFD), F32),
    fo=VM((2, D), F32),
    fq=VM((1, 128), F32),
    wq=VM((NZ, 48, 512), BF),
    wo=VM((NP, 32, 256), BF),
    wg=VM((2, 256, D), BF),
    wd=VM((256, D), BF),
    fhx=VM((2, 3, 2, FFD), F32),
    fhy=VM((2, 3, 2, FFD), F32),
    fhp=VM((3, 2, 256), F32),
    lm=VM((HALF, VD), BF),
    sc=VM((64, 128), F32),
    s1s=VM((64, 128), F32),
    s1r=VM((64, 128), F32),
    raw=VM((NP, 16, 512), BF),
    p1=VM((3, 256, 128), F32),
    s3s=VM((NZ, 32, QN), BF),
    s3r=VM((NZ, 32, QN), BF),
    q1=VM((3, 32, 128), F32),
    s4s=VM((128, 128), F32),
    s4r=VM((128, 128), F32),
    hs=VM((96, 128), F32),
    osc=VM((64, 128), F32),
    s5s=VM((64, 128), F32),
    s5r=VM((64, 128), F32),
    att=VM((NP, 16, 512), BF),
    s7s=VM((NZ, 32, 256), BF),
    s7r=VM((NZ, 32, 256), BF),
    mc=VM((2, 128, 256), BF),
    xb=VM((NY, 64, 256), BF),
    mid=VM((NP, 128, 256), BF),
    accg=VM((128, 256), F32),
    accu=VM((128, 256), F32),
    ssq=VM((128, 128), F32),
    hid=VM((128, 256), BF),
    p3=VM((2, NY, 16, D), BF),
    r1a=VM((NY, 16, HALF), BF),
    r1b=VM((NY, 2, 16, HALF), BF),
    s2a=VM((NY, 16, HALF), BF),
    s2b=VM((2, 16, HALF), BF),
    r2a=VM((NY, 16, HALF), BF),
    r2b=VM((16, HALF), BF),
    f3=VM((512, 128), F32),
    g3=VM((32, 128), F32),
    s13s=VM((NZ, 64, 128), BF),
    s13r=VM((NZ, 64, 128), BF),
    fs=VM((32, 128), F32),
    fr=VM((16, 128), F32),
    fb=VM((NP, NZ, 16, 128), BF),
    ff=VM((2048, 128), F32),
    lh=VM((B, HALF), BF),
    lp=VM((B, VD), F32),
    lr=VM((B, VD), F32),
    sz=VM((NZ, 8, 128), F32),
    sx=VM((NP, 8, 128), F32),
)
PHASES = dict(
    wq=1, wqf=1, wo=1, s1=1, s2=1, s3=1, s4=1, s5=1, s6=1, s7=1, s8=1, da=6, db=3, dg=9,
    xg=2, xd=2, fg=2, fd=2, xh=2, fi=1, fh=1, fo=1, fy=1,
    a1=NCH, b1=NCH, a2=1, b2=1, s13=1, fx=1, s14=1, s15=1, lx=1, s16=1, s17=1,
)
LS = dict(ls=DMA((16,)))
OUTS = dict(
    logits_o=jax.ShapeDtypeStruct((B, VD), BF), lp_o=jax.ShapeDtypeStruct((1, B), F32)
)


def kernel(inputs, *refs):
    names = [*inputs, *OUTS, *SCRATCH, *LS]
    r = SimpleNamespace(**dict(zip(names, refs)))
    sems = iter(refs[len(names) :])
    p = SimpleNamespace(**{k: (next(sems), next(sems)) for k in PHASES})
    c, x, z, y = (lax.axis_index(a) for a in MEMBER_TP)
    t = x * 32 + z * 4 + y
    n = x * 4 + y
    xl, par = x // 2, lax.rem(x, 2)
    own = xl * 8 + y * 2 + par
    drains = []
    def rem(v, k):
        return lax.rem(v, k)

    def at_z(zz):
        return (c, x, zz, y)

    def at_xy(xx, yy):
        return (c, xx, z, yy)

    partner = (1 - c, x, z, y)

    def across_z(zz):
        return (1 - c, x, zz, y)

    def copy(phase, src, dst, dev, slot=0):
        return pltpu.make_async_remote_copy(
            src_ref=src,
            dst_ref=dst,
            send_sem=phase[0].at[0],
            recv_sem=phase[1].at[slot],
            device_id=dev,
            device_id_type=MESH,
        )

    def send(phase, src, dst, dev, slot=0):
        copy(phase, src, dst, dev, slot).start()

    def wait_bytes(sem, ref):
        pltpu.make_async_copy(ref, ref, sem).wait()

    def recv(phase, ref, slot=0):
        wait_bytes(phase[1].at[slot], ref)

    def sent(phase, ref):
        drains.append((phase[0].at[0], ref))

    zpeers = [rem(z + d, NZ) for d in ZORDER]
    plane = [
        (rem(x + dx, NX), rem(y + dy, NY))
        for dx, dy in sorted(
            ((a, b) for a in range(NX) for b in range(NY) if a or b),
            key=lambda p: -(min(p[0], 4 - p[0]) + min(p[1], 4 - p[1])),
        )
    ]

    def z_send(phase, src_at, dst):
        for zz in zpeers:
            send(phase, src_at(zz), dst, at_z(zz))

    def xy_send(phase, src_at, dst):
        for xx, yy in plane:
            send(phase, src_at(xx * 4 + yy), dst, at_xy(xx, yy))

    def done(phase, ref):
        recv(phase, ref)
        sent(phase, ref)

    bar = pltpu.get_barrier_semaphore()
    peers = [at_z(zz) for zz in zpeers] + [at_xy(*k) for k in plane] + [partner]
    peers += [across_z(zz) for zz in zpeers]
    for dev in peers:
        pl.semaphore_signal(bar, inc=1, device_id=dev, device_id_type=MESH)

    def qcols(zz, k):
        return r.wqkv.at[:, pl.ds(pl.multiple_of(k * 1024 + zz * 128, 128), 128)]

    def half_cols(k):
        return pl.ds(pl.multiple_of((2 * c + k) * 128, 128), 128)

    local = SimpleNamespace()
    begun = []

    def fetch(src, dst):
        k = pltpu.make_async_copy(src, dst, r.ls.at[len(begun)])
        k.start()
        begun.append(k)
        return k

    local.st = fetch(r.stream, r.st)
    local.gn = fetch(r.gains, r.gn)
    local.fq = fetch(r.freq, r.fq)
    local_wq = [fetch(qcols(z, 2 * c + k), r.wq.at[z, :, half_cols(k)]) for k in range(2)]
    local.wo = fetch(r.wout.at[:, pl.ds(pl.multiple_of(n * 256, 256), 256)], r.wo.at[n])
    local.kvv = fetch(r.kv, r.kvv)
    local.tg = fetch(r.targets, r.tg)
    local.wg = fetch(r.wgu, r.wg.at[:, 0:FFD])
    local.wd = fetch(r.wdown, r.wd.at[0:FFD])
    local.lm = fetch(r.lmh.at[pl.ds(pl.multiple_of(c * HALF, HALF), HALF)], r.lm)

    right, left = at_xy(rem(x + 1, NX), y), at_xy(rem(x + 3, NX), y)

    def weight_piece(i):
        cols = pl.ds(pl.multiple_of(c * HALF + i * 256, 256), 256)
        for dev, a, b in ((right, 0, 64), (left, 64, FFD)):
            g = r.wg.at[:, 128 + a : 128 + b, cols]
            send(p.xg, r.wgu.at[:, a:b, cols], g, dev, i // 4)
            send(p.xd, r.wdown.at[a:b, cols], r.wd.at[128 + a : 128 + b, cols], dev, i // 4)

    def pass_weights(g):
        cols = pl.ds(pl.multiple_of(c * HALF + g * 1024, 1024), 1024)
        for came, went, at in (
            (p.xg, p.fg, r.wg.at[:, 128 : 128 + FFD, cols]),
            (p.xd, p.fd, r.wd.at[128 : 128 + FFD, cols]),
        ):
            recv(came, at, g)
            send(went, at, at, partner, g)

    def spread(scratch, dst):
        for zz in range(NZ):
            dst[zz * 8 : zz * 8 + 8] = scratch[pl.ds(zz, 8, stride=8), :]

    z8 = pl.ds(pl.multiple_of(z * 8, 8), 8)

    def z_then_plane(zphase, pphase, s, rr, buf, start=True, beside=lambda: None):
        def piece(zz):
            return pl.ds(pl.multiple_of(zz * 8, 8), 8)

        if start:
            z_send(zphase, lambda zz: s.at[piece(zz)], rr.at[z8])
        beside()
        rr[z8, :] = s[z8, :]
        done(zphase, rr.at[0:56])
        for k in range(4):
            rows = [rr[pl.ds(j * 4 + k, 8, stride=8), :] for j in range(2)]
            buf[n, :, k * 128 : (k + 1) * 128] = jnp.concatenate(rows, axis=0).astype(BF)
        xy_send(pphase, lambda m: buf.at[n], buf.at[n])
        return lambda: done(pphase, buf.at[0:15])

    local.st.wait()
    x32 = r.st[...].astype(F32)
    rs = lax.rsqrt(jnp.mean(x32 * x32, axis=-1, keepdims=True) + 1e-5)
    for b in range(32):
        for j in range(2):
            r.sc[j * 32 + b : j * 32 + b + 1, :] = x32[j : j + 1, b * 128 : (b + 1) * 128]
    spread(r.sc, r.s1s)
    r.s4s[...] = jnp.zeros((128, 128), F32)
    row8 = lax.broadcasted_iota(jnp.int32, (8, 128), 0)
    lane8 = lax.broadcasted_iota(jnp.int32, (8, 128), 1)
    rs8 = jnp.where(row8 < 4, rs[0:1, 0:1], rs[1:2, 0:1])

    pl.semaphore_wait(bar, len(peers))

    for zz in zpeers:
        send(p.s1, r.s1s.at[pl.ds(pl.multiple_of(zz * 8, 8), 8)], r.s1r.at[z8], at_z(zz))
    for zz in zpeers:
        for k in range(2):
            send(p.wq, qcols(zz, 2 * c + k), r.wq.at[z, :, half_cols(k)], at_z(zz))
    weight_piece(0)
    weight_piece(1)
    send(p.fi, r.fin, r.fi, partner)
    send(p.fh, r.fhid, r.fh, partner)
    send(p.fo, r.fout, r.fo, partner)
    send(p.xh, r.fhid, r.fhx.at[0], right, 0)
    send(p.xh, r.fhid, r.fhx.at[1], left, 1)
    finish = z_then_plane(p.s1, p.s2, r.s1s, r.s1r, r.raw, False)
    xy_send(
        p.wo,
        lambda m: r.wout.at[:, pl.ds(pl.multiple_of(m * 256, 256), 256)],
        r.wo.at[n],
    )
    local.fq.wait()
    local.gn.wait()
    pos = [r.lengths[rem(2 * t + j, B)] for j in range(2)]
    ang = jnp.where(row8 < 4, pos[0], pos[1]).astype(F32) * r.fq[0:1, :]
    cos8 = jnp.cos(ang)
    sin8 = jnp.where(lane8 < 64, -jnp.sin(ang), jnp.sin(ang))
    for b in range(32):
        r.g3[b : b + 1, :] = r.gn[2:3, b * 128 : (b + 1) * 128]

    for k in range(2):
        local_wq[k].wait()
    done(p.wq, r.wq.at[0:7, :, 0:256])
    mine = r.wq.at[:, :, pl.ds(pl.multiple_of(c * 256, 256), 256)]
    send(p.wqf, mine, mine, partner)
    done(p.wqf, mine)
    gq = jnp.concatenate(
        [r.gn[0:1, pl.ds(pl.multiple_of(k * 1024 + z * 128, 128), 128)] for k in range(4)], axis=1
    )
    finish()
    lhs = (r.raw[...].reshape(256, 512).astype(F32) * gq).astype(BF)
    prod = lax.dot_general(lhs, r.wq[...].reshape(QN, 512), NT, preferred_element_type=F32)
    for l in range(3):
        r.p1[l] = prod[:, l * 128 : (l + 1) * 128]
    for zz in range(NZ):
        for l in range(3):
            r.s3s[zz, :, l * 128 : (l + 1) * 128] = r.p1.at[l][
                pl.ds(zz, 32, stride=8), :
            ].astype(BF)
    z_send(p.s3, lambda zz: r.s3s.at[zz], r.s3r.at[z])
    weight_piece(2)
    weight_piece(3)
    r.s3r[z] = r.s3s[z]
    done(p.s3, r.s3r.at[0:7])
    acc = r.s3r[0].astype(F32)
    for s in range(1, NZ):
        acc = acc + r.s3r[s].astype(F32)
    for l in range(3):
        r.q1[l] = acc[:, l * 128 : (l + 1) * 128]
    for l in range(3):
        for j in range(2):
            r.s4s[pl.ds(l * 2 + j, 16, stride=8), :] = r.q1.at[l][pl.ds(j, 16, stride=2), :]

    def tile(m):
        return pl.ds(pl.multiple_of(m * 8, 8), 8)

    xy_send(p.s4, lambda m: r.s4s.at[tile(m)], r.s4r.at[tile(n)])
    r.s4r[tile(n), :] = r.s4s[tile(n), :]
    done(p.s4, r.s4r.at[0:120])

    blocks = {
        (yy, l): jnp.concatenate(
            [r.s4r[pl.ds(yy * 8 + l * 2 + j, 4, stride=32), :] for j in range(2)], axis=0
        )
        for yy in range(NY)
        for l in range(3)
    }
    for hh in range(12):
        val = jnp.zeros((8, 128), F32)
        lane = 0
        while lane < 128:
            col = hh * 128 + lane
            tt, i = divmod(col, 48)
            at = (tt // 4) * 48 + i
            l, src = divmod(at, 128)
            width = min(48 - i, 128 - src, 128 - lane)
            piece = blocks[(tt % 4, l)]
            shift = (lane - src) % 128
            if shift:
                piece = pltpu.roll(piece, shift, 1)
            val = jnp.where((lane8 >= lane) & (lane8 < lane + width), piece, val)
            lane += width
        val = (val * rs8).astype(BF).astype(F32)
        turned = (val * cos8 + pltpu.roll(val, 64, 1) * sin8).astype(BF).astype(F32)
        if hh >= 4:
            turned = jnp.where(row8 % 4 == 3, val, turned)
        r.hs[pl.ds(hh, 8, stride=12), :] = turned

    local.kvv.wait()
    inv_root = HD**-0.5
    group = lax.broadcasted_iota(jnp.int32, (32, 128), 0) // 4
    group8 = (
        lax.broadcasted_iota(jnp.int32, (32, 8), 0) // 4
        == lax.broadcasted_iota(jnp.int32, (32, 8), 1)
    )
    place = lax.broadcasted_iota(jnp.int32, (32, CACHE), 1)
    for j in range(2):
        q = r.hs[j * 48 : j * 48 + 32, :]
        kn = r.hs[j * 48 + 32 : j * 48 + 40, :].astype(BF)
        vn = r.hs[j * 48 + 40 : j * 48 + 48, :].astype(BF)
        qd = jnp.concatenate([jnp.where(group == k, q, 0.0) for k in range(KV)], axis=1).astype(BF)
        scores = (
            lax.dot_general(qd, r.kvv[j, :, : KV * HD], NT, preferred_element_type=F32) * inv_root
        )
        fresh = lax.dot_general(q.astype(BF), kn, NT, preferred_element_type=F32)
        fresh = jnp.sum(jnp.where(group8, fresh, 0.0), axis=1, keepdims=True) * inv_root
        scores = jnp.where(place < pos[j], scores, -1e30)
        peak = jnp.maximum(jnp.max(scores, axis=1, keepdims=True), fresh)
        weights = jnp.exp(scores - peak)
        fresh_w = jnp.exp(fresh - peak)
        total = jnp.sum(weights, axis=1, keepdims=True) + fresh_w
        probs = (weights / total).astype(BF)
        fresh_p = jnp.where(group8, fresh_w / total, 0.0).astype(BF)
        wide = jnp.dot(probs, r.kvv[j, :, KV * HD :], preferred_element_type=F32)
        out = jnp.dot(fresh_p, vn, preferred_element_type=F32)
        for k in range(KV):
            out = out + jnp.where(group == k, wide[:, k * 128 : (k + 1) * 128], 0.0)
        r.osc[j * 32 : j * 32 + 32, :] = out.astype(BF).astype(F32)

    spread(r.osc, r.s5s)

    def beside():
        weight_piece(4)
        weight_piece(5)

    finish = z_then_plane(p.s5, p.s6, r.s5s, r.s5r, r.att, beside=beside)
    pass_weights(0)
    local.wo.wait()
    done(p.wo, r.wo.at[0:15])
    resid = r.raw[:, :, pl.ds(pl.multiple_of(x * 128, 128), 128)].reshape(256, 128).astype(F32)
    lo = resid * jnp.where(z == 2 * y, 1.0, 0.0)
    hi = resid * jnp.where(z == 2 * y + 1, 1.0, 0.0)
    finish()
    prod = jnp.dot(
        r.att[...].reshape(256, 512), r.wo[...].reshape(512, 256), preferred_element_type=F32
    ) + jnp.concatenate([lo, hi], axis=1)
    for h in range(2):
        for ys in range(NY):
            for j in range(2):
                at = [((m * 2 + h) * 4 + ys) * 16 + j * 8 for m in range(2)]
                r.s7s[h * 4 + ys, j * 16 : j * 16 + 16, :] = jnp.concatenate(
                    [prod[a : a + 8] for a in at], axis=0
                ).astype(BF)
    for zz in zpeers:
        send(p.s7, r.s7s.at[zz], r.s7r.at[z], across_z(zz))
    send(p.s7, r.s7s.at[z], r.s7r.at[z], partner)
    weight_piece(6)
    weight_piece(7)
    recv(p.xh, r.fhx.at[0], 0)
    recv(p.xh, r.fhx.at[1], 1)
    sent(p.xh, r.fhx)
    send(p.fy, r.fhx, r.fhy, partner)
    done(p.s7, r.s7r)
    acc = r.s7r[0].astype(F32)
    for s in range(1, NZ):
        acc = acc + r.s7r[s].astype(F32)

    z16 = pl.ds(pl.multiple_of(z * 16, 16), 16)
    for j in range(2):
        r.mc[j, z16, :] = acc[j * 16 : j * 16 + 16].astype(BF)
    z_send(p.s8, lambda zz: r.mc.at[:, z16], r.mc.at[:, z16])
    r.accg[...] = jnp.zeros((128, 256), F32)
    r.accu[...] = jnp.zeros((128, 256), F32)
    r.ssq[...] = jnp.zeros((128, 128), F32)
    for a in (FFD, 128 + FFD):
        r.wg[:, a : a + 16, :] = jnp.zeros((2, 16, D), BF)
        r.wd[a : a + 16, :] = jnp.zeros((16, D), BF)
    done(p.fi, r.fi)
    done(p.fh, r.fh)
    done(p.fo, r.fo)
    done(p.fy, r.fhy)
    r.fhp[...] = jnp.zeros((3, 2, 256), F32)
    r.fhp[:, :, 0:FFD] = r.fh[...]
    lane_h = lax.broadcasted_iota(jnp.int32, (3, 2, FFD), 2)
    r.fhp[:, :, 128 : 128 + FFD] = jnp.where(lane_h < 64, r.fhy[0], r.fhy[1])
    pass_weights(1)
    mine_g = r.wg.at[:, 128 : 128 + FFD, 0:HALF]
    mine_d = r.wd.at[128 : 128 + FFD, 0:HALF]
    for k in (p.xg, p.fg):
        sent(k, mine_g)
    for k in (p.xd, p.fd):
        sent(k, mine_d)
    for k in (local.wg, local.wd):
        k.wait()
    done(p.s8, r.mc.at[:, 0:112])

    near = (1, 3, 2)
    top, low = pl.ds(0, 64), pl.ds(64, 64)
    for d in (2, 1, 3):
        xx, yy = rem(x + d, NX), rem(y + d, NY)
        send(p.da, r.mc.at[rem(xx, 2)], r.mid.at[n], at_xy(xx, y), 3 - d)
        send(p.da, r.mc.at[par], r.mid.at[n], at_xy(x, yy), 6 - d)
        send(p.db, r.mc.at[1 - par, low], r.xb.at[y], at_xy(x, yy), 3 - d)
    sent(p.da, r.mid.at[0:6])
    sent(p.db, r.xb.at[0:3])
    r.mid[n] = r.mc[par]
    for g in range(2):
        cols = pl.ds(pl.multiple_of((1 - c) * HALF + g * 1024, 1024), 1024)
        recv(p.fg, r.wg.at[:, 128 : 128 + FFD, cols], g)
        recv(p.fd, r.wd.at[128 : 128 + FFD, cols], g)

    def ffn_chunk(m):
        v = r.mid[m].astype(F32)
        r.ssq[...] += v[:, :128] * v[:, :128] + v[:, 128:] * v[:, 128:]
        cols = pl.ds(pl.multiple_of(m * 256, 256), 256)
        g = r.gn[1:2, cols]
        v4 = v.reshape(8, 2, 8, 256)
        for k, total in enumerate((r.accg, r.accu)):
            f = jnp.concatenate(
                [
                    (r.fi[i, k : k + 1, cols] * g).reshape(1, 1, 1, 256)
                    for i in range(2)
                ],
                axis=1,
            )
            act = (v4 * f).reshape(128, 256).astype(BF)
            total[...] += lax.dot_general(
                act, r.wg[k, :, cols], NT, preferred_element_type=F32
            )

    ffn_chunk(n)
    for d in near:
        m = rem(x + d, NX) * 4 + y
        recv(p.da, r.mid.at[m], d - 1)
        for e in (2, 1, 3):
            yy = rem(y + e, NY)
            send(p.dg, r.mid.at[m, top], r.mid.at[m, top], at_xy(x, yy), (d - 1) * 3 + 3 - e)
        yy = rem(y + d, NY)
        m = x * 4 + yy
        recv(p.da, r.mid.at[m], d + 2)
        recv(p.db, r.xb.at[yy], d - 1)
        for e in (2, 1, 3):
            xx = rem(x + e, NX)
            at = r.mid.at[m, low] if e == 2 else r.xb.at[yy]
            send(p.dg, at, r.mid.at[m, low], at_xy(xx, y), (3 - e) * 3 + d - 1)
    sent(p.dg, r.mid.at[0:9])

    def line_step(i, carry):
        ffn_chunk(rem(x + 1 + i, NX) * 4 + y)
        ffn_chunk(x * 4 + rem(y + 1 + i, NY))
        return carry

    lax.fori_loop(0, 3, line_step, 0)

    def diag_step(i, carry):
        m = rem(x + 1 + i // 3, NX) * 4 + rem(y + 1 + i % 3, NY)
        recv(p.dg, r.mid.at[m], i)
        ffn_chunk(m)
        return carry

    lax.fori_loop(0, 9, diag_step, 0)
    scale = lax.rsqrt(jnp.sum(r.ssq[...], axis=1, keepdims=True) * (1.0 / D) + 1e-5)

    def by_member(k):
        return jnp.concatenate(
            [r.fhp[k, i : i + 1, :].reshape(1, 1, 1, 256) for i in range(2)], axis=1
        )

    gate = (r.accg[...] * scale).reshape(8, 2, 8, 256) * by_member(0)
    up = (r.accu[...] * scale).reshape(8, 2, 8, 256) * by_member(1)
    hidden = gate / (1.0 + jnp.exp(-gate)) * up * by_member(2)
    r.hid[...] = hidden.reshape(128, 256).astype(BF)

    def chunk(ch):
        return pl.ds(pl.multiple_of(ch * CW, CW), CW)

    def high(ch):
        return pl.ds(pl.multiple_of(HALF + ch * CW, CW), CW)

    other = 1 - xl
    opposite = at_xy(rem(x + 2, NX), y)

    def a1(ch):
        send(p.a1, r.p3.at[other, :, :, chunk(ch)], r.r1a.at[:, :, chunk(ch)], opposite, ch)

    def b1(ch, yy):
        at = r.p3.at[:, yy, :, high(ch)]
        send(p.b1, at, r.r1b.at[y, :, :, chunk(ch)], at_xy(x, yy), ch)

    def down_step(ch, carry):
        for cols in (chunk(ch), high(ch)):
            v = jnp.dot(r.hid[...], r.wd[:, cols], preferred_element_type=F32)
            r.p3[:, :, :, cols] = v.astype(BF).reshape(2, NY, 16, CW)
        a1(ch)
        for d in (2, 1, 3):
            b1(ch, rem(y + d, NY))
        return carry

    lax.fori_loop(0, NCH, down_step, 0)

    def a2(ch, yy):
        send(p.a2, r.s2a.at[yy, :, chunk(ch)], r.r2a.at[y, :, chunk(ch)], at_xy(x, yy))

    def b2(ch):
        send(p.b2, r.s2b.at[other, :, chunk(ch)], r.r2b.at[:, chunk(ch)], opposite)

    def second_step(ch, carry):
        recv(p.a1, r.r1a.at[:, :, chunk(ch)], ch)
        v = r.p3[xl, :, :, chunk(ch)].astype(F32) + r.r1a[:, :, chunk(ch)].astype(F32)
        r.s2a[:, :, chunk(ch)] = v.astype(BF)
        for d in (2, 1, 3):
            a2(ch, rem(y + d, NY))
        recv(p.b1, r.r1b.at[0:3, :, :, chunk(ch)], ch)
        v = r.p3[:, y, :, high(ch)].astype(F32)
        for d in near:
            v = v + r.r1b[rem(y + d, NY), :, :, chunk(ch)].astype(F32)
        r.s2b[:, :, chunk(ch)] = v.astype(BF)
        b2(ch)
        return carry

    lax.fori_loop(0, NCH, second_step, 0)
    sent(p.a1, r.r1a)
    sent(p.b1, r.r1b.at[0:3])
    done(p.a2, r.r2a.at[0:3])
    done(p.b2, r.r2b)

    row16 = lax.broadcasted_iota(jnp.int32, (16, 128), 0)
    own_row = rem(row16, 8) == z
    tile16 = pl.ds(pl.multiple_of((xl * 4 + y) * 16, 16), 16)
    for b in range(32):
        cols = slice((b % 16) * 128, (b % 16 + 1) * 128)
        if b < 16:
            v = r.s2a[y, :, cols].astype(F32)
            for d in near:
                v = v + r.r2a[rem(y + d, NY), :, cols].astype(F32)
        else:
            v = r.s2b[xl, :, cols].astype(F32) + r.r2b[:, cols].astype(F32)
        at = slice(b * 128, (b + 1) * 128)
        v = v * jnp.where(row16 < 8, r.fo[0:1, at], r.fo[1:2, at])
        m = r.mid[b // 2, tile16, (b % 2) * 128 : (b % 2 + 1) * 128].astype(F32)
        r.f3[b * 16 : (b + 1) * 16, :] = v + jnp.where(own_row, m, 0.0)

    for zz in range(NZ):
        for m in range(2):
            r.s13s[zz, m * 32 : (m + 1) * 32, :] = r.f3[
                pl.ds(m * 8 + zz, 32, stride=16), :
            ].astype(BF)
    z_send(p.s13, lambda zz: r.s13s.at[zz], r.s13r.at[z])
    owned = [r.f3[pl.ds(m * 8 + z, 32, stride=16), :] for m in range(2)]
    done(p.s13, r.s13r.at[0:7])
    both = jnp.zeros((32, 128), F32)
    for m in range(2):
        v = owned[m]
        for zz in zpeers:
            v = v + r.s13r[zz, m * 32 : (m + 1) * 32, :].astype(F32)
        v = v.astype(BF).astype(F32)
        mean = jnp.sum(jnp.sum(v * v, axis=1, keepdims=True), axis=0, keepdims=True) * (1.0 / D)
        both = both + (v * lax.rsqrt(mean + 1e-5) * r.g3[...]).astype(BF).astype(F32)
    r.fs[...] = both

    def half(k):
        return pl.ds(pl.multiple_of(k * 16, 16), 16)

    send(p.fx, r.fs.at[half(1 - c)], r.fr, partner)
    done(p.fx, r.fr)
    r.fb[own, z] = ((r.fs[half(c), :] + r.fr[...]) * 0.25).astype(BF)
    z_send(p.s14, lambda zz: r.fb.at[own, z], r.fb.at[own, z])
    local.lm.wait()
    local.tg.wait()
    wanted = jnp.broadcast_to(r.tg[...].astype(F32), (B, B)).T[:, 0:1]
    done(p.s14, r.fb.at[own, 0:7])
    xy_send(p.s15, lambda m: r.fb.at[own], r.fb.at[own])
    done(p.s15, r.fb.at[0:15])
    r.ff[...] = r.fb[...].reshape(2048, 128).astype(F32)
    for b in range(16):
        rows = [
            r.ff[pl.ds(h * 1024 + zz * 16 + b, 8, stride=128), :]
            for h in range(2)
            for zz in range(NZ)
        ]
        r.lh[:, b * 128 : (b + 1) * 128] = jnp.concatenate(rows, axis=0).astype(BF)
    r.lp[...] = jnp.dot(r.lh[...], r.lm[...], preferred_element_type=F32)
    send(p.lx, r.lp, r.lr, partner)
    done(p.lx, r.lr)
    mean_f = r.lp[...] + r.lr[...]
    r.logits_o[...] = mean_f.astype(BF)

    ids = (lax.broadcasted_iota(jnp.int32, (B, VD), 1) + t * VD).astype(F32)
    found = jnp.sum(jnp.where(ids == wanted, mean_f, 0.0), axis=1, keepdims=True)
    peak = jnp.max(mean_f, axis=1, keepdims=True)
    total = jnp.sum(jnp.exp(mean_f - peak), axis=1, keepdims=True)
    lane = lax.broadcasted_iota(jnp.int32, (B, B), 1)
    stat = jnp.where(lane == 0, peak, jnp.where(lane == 1, total, jnp.where(lane == 2, found, 0.0)))
    r.sz[z] = stat.T[:8]

    def combine(ref, count):
        peaks = [ref[k, 0:1, :] for k in range(count)]
        top_ = peaks[0]
        for k in range(1, count):
            top_ = jnp.maximum(top_, peaks[k])
        tot = ref[0, 1:2, :] * jnp.exp(peaks[0] - top_)
        hit = ref[0, 2:3, :]
        for k in range(1, count):
            tot = tot + ref[k, 1:2, :] * jnp.exp(peaks[k] - top_)
            hit = hit + ref[k, 2:3, :]
        return top_, tot, hit

    z_send(p.s16, lambda zz: r.sz.at[z], r.sz.at[z])
    done(p.s16, r.sz.at[0:7])
    a, b_, h = combine(r.sz, NZ)
    r.sx[n] = jnp.concatenate([a, b_, h, jnp.zeros((5, 128), F32)], axis=0)
    xy_send(p.s17, lambda m: r.sx.at[n], r.sx.at[n])
    done(p.s17, r.sx.at[0:15])
    a, b_, h = combine(r.sx, NP)
    r.lp_o[...] = h - (a + jnp.log(b_))

    for sem, ref in drains:
        wait_bytes(sem, ref)


def hand_on(logits, logprob, logits_o, logprob_o):
    logits_o[...] = logits[...]
    logprob_o[...] = logprob[...]


def body(
    stream_in, kv_cache, lengths, targets, norm_gains, w_qkv, w_out, w_gate_up, w_down, lm_head,
    fast_in, fast_hidden, fast_out,
):
    freq = np.float32(500000.0) ** (-np.arange(64, dtype=np.float32) * 2.0 / 128)
    freq = jnp.asarray(np.concatenate([freq, freq])[None, :], F32)
    args = dict(
        stream=stream_in, kv=kv_cache, lengths=lengths, targets=targets.reshape(1, B),
        gains=norm_gains, wqkv=w_qkv.T, wout=w_out,
        wgu=w_gate_up.swapaxes(1, 2), wdown=w_down, lmh=lm_head,
        fin=fast_in, fhid=fast_hidden.swapaxes(0, 1), fout=fast_out, freq=freq,
    )
    got = pl.pallas_call(
        functools.partial(kernel, list(args)),
        out_shape=list(OUTS.values()),
        in_specs=[
            pl.BlockSpec(memory_space=pltpu.SMEM if v is lengths else pl.ANY)
            for v in args.values()
        ],
        out_specs=[pl.BlockSpec(memory_space=VM)] * len(OUTS),
        scratch_shapes=[
            *SCRATCH.values(),
            *LS.values(),
            *(DMA((count,)) for n in PHASES.values() for count in (1, n)),
        ],
        compiler_params=pltpu.CompilerParams(
            collective_id=0, has_side_effects=True, vmem_limit_bytes=60 * 1024 * 1024
        ),
        name="step",
    )(*args.values())
    got = pl.pallas_call(hand_on, out_shape=list(OUTS.values()), name="result")(*got)
    return (got[0], got[1].reshape(B))


MEMBER_TP = ("member", "tp_0", "tp_1", "tp_2")
TP = ("tp_0", "tp_1", "tp_2")
IN_SPECS = (
    P(MEMBER_TP, None), P(MEMBER_TP, None, None), P(), P(), P(), P(None, TP), P(TP, None),
    P(None, None, TP), P(TP, None), P(None, TP), P("member", None, None), P("member", None, TP),
    P("member", None),
)


def solution(mesh):
    split = Mesh(
        mesh.devices.reshape(mesh.shape["member"], NX, NZ, NY), MEMBER_TP
    )
    return jax.shard_map(
        body, mesh=split, in_specs=IN_SPECS, out_specs=(P(None, TP), P()), check_vma=False
    )
```

```python
import functools
from types import SimpleNamespace

import jax
import jax.numpy as jnp
import numpy as np
from jax import lax
from jax.experimental import pallas as pl
from jax.experimental.pallas import tpu as pltpu
from jax.sharding import Mesh
from jax.sharding import PartitionSpec as P

MESH = pl.DeviceIdType.MESH
F32 = jnp.float32
BF = jnp.bfloat16
NX, NZ, NY = 4, 8, 4
NP = NX * NY
D, HEADS, KV, HD, CACHE, FFD, VD = 4096, 32, 8, 128, 512, 112, 512
B = 128
QN = 384
ZORDER = (4, 3, 5, 2, 6, 1, 7)
NCH, CW = 4, 512
HALF = D // 2
NT = (((1,), (1,)), ((), ()))

VM = pltpu.VMEM
DMA = pltpu.SemaphoreType.DMA

SCRATCH = dict(
    st=VM((2, D), BF),
    kvv=VM((2, CACHE, 2 * KV * HD), BF),
    tg=VM((1, B), jnp.int32),
    gn=VM((3, D), F32),
    fi=VM((2, 2, D), F32),
    fh=VM((3, 2, FFD), F32),
    fo=VM((2, D), F32),
    fq=VM((1, 128), F32),
    wq=VM((NZ, 48, 512), BF),
    wo=VM((NP, 32, 256), BF),
    wg=VM((2, 256, D), BF),
    wd=VM((256, D), BF),
    fhx=VM((2, 3, 2, FFD), F32),
    fhy=VM((2, 3, 2, FFD), F32),
    fhp=VM((3, 2, 256), F32),
    lm=VM((HALF, VD), BF),
    sc=VM((64, 128), F32),
    s1s=VM((64, 128), F32),
    s1r=VM((64, 128), F32),
    raw=VM((NP, 16, 512), BF),
    p1=VM((3, 256, 128), F32),
    s3s=VM((NZ, 32, QN), BF),
    s3r=VM((NZ, 32, QN), BF),
    q1=VM((3, 32, 128), F32),
    s4s=VM((128, 128), F32),
    s4r=VM((128, 128), F32),
    hs=VM((96, 128), F32),
    osc=VM((64, 128), F32),
    s5s=VM((64, 128), F32),
    s5r=VM((64, 128), F32),
    att=VM((NP, 16, 512), BF),
    s7s=VM((NZ, 32, 256), BF),
    s7r=VM((NZ, 32, 256), BF),
    mc=VM((2, 128, 256), BF),
    xb=VM((NY, 128, 128), BF),
    mid=VM((NP, 128, 256), BF),
    accg=VM((128, 256), F32),
    accu=VM((128, 256), F32),
    ssq=VM((128, 128), F32),
    hid=VM((128, 256), BF),
    p3=VM((2, NY, 16, D), BF),
    r1a=VM((NY, 16, HALF), BF),
    r1b=VM((NY, 2, 16, HALF), BF),
    s2a=VM((NY, 16, HALF), BF),
    s2b=VM((2, 16, HALF), BF),
    r2a=VM((NY, 16, HALF), BF),
    r2b=VM((16, HALF), BF),
    f3=VM((512, 128), F32),
    g3=VM((32, 128), F32),
    s13s=VM((NZ, NCH, 16, 128), BF),
    s13r=VM((NZ, NCH, 16, 128), BF),
    vs=VM((64, 128), F32),
    fs=VM((32, 128), F32),
    fr=VM((16, 128), F32),
    fb=VM((NP, NZ, 16, 128), BF),
    ff=VM((2048, 128), F32),
    lh=VM((B, HALF), BF),
    lp=VM((B, VD), F32),
    lr=VM((B, VD), F32),
    sz=VM((NZ, 8, 128), F32),
    sx=VM((NP, 8, 128), F32),
)
PHASES = dict(
    wq=1, wqf=1, wo=1, s1=1, s2=1, s3=1, s4=1, s5=1, s6=1, s7=1, s8=7, da=6, db=3, dg=9,
    xg=2, xd=2, fg=2, fd=2, xh=2, fi=1, fh=1, fo=1, fy=1,
    a1=NCH, b1=NCH, a2=NCH, b2=NCH, s13=NCH, fx=1, s14=1, s15=1, lx=2, s16=1, s17=1,
)
LS = dict(ls=DMA((16,)))
OUTS = dict(
    logits_o=jax.ShapeDtypeStruct((B, VD), BF), lp_o=jax.ShapeDtypeStruct((1, B), F32)
)


def kernel(inputs, *refs):
    names = [*inputs, *OUTS, *SCRATCH, *LS]
    r = SimpleNamespace(**dict(zip(names, refs)))
    sems = iter(refs[len(names) :])
    p = SimpleNamespace(**{k: (next(sems), next(sems)) for k in PHASES})
    c, x, z, y = (lax.axis_index(a) for a in MEMBER_TP)
    t = x * 32 + z * 4 + y
    n = x * 4 + y
    xl, par = x // 2, lax.rem(x, 2)
    own = xl * 8 + y * 2 + par
    drains = []
    def rem(v, k):
        return lax.rem(v, k)

    def at_z(zz):
        return (c, x, zz, y)

    def at_xy(xx, yy):
        return (c, xx, z, yy)

    partner = (1 - c, x, z, y)

    def across_z(zz):
        return (1 - c, x, zz, y)

    def copy(phase, src, dst, dev, slot=0):
        return pltpu.make_async_remote_copy(
            src_ref=src,
            dst_ref=dst,
            send_sem=phase[0].at[0],
            recv_sem=phase[1].at[slot],
            device_id=dev,
            device_id_type=MESH,
        )

    def send(phase, src, dst, dev, slot=0):
        copy(phase, src, dst, dev, slot).start()

    def wait_bytes(sem, ref):
        pltpu.make_async_copy(ref, ref, sem).wait()

    def recv(phase, ref, slot=0):
        wait_bytes(phase[1].at[slot], ref)

    def sent(phase, ref):
        drains.append((phase[0].at[0], ref))

    zpeers = [rem(z + d, NZ) for d in ZORDER]
    plane = [
        (rem(x + dx, NX), rem(y + dy, NY))
        for dx, dy in sorted(
            ((a, b) for a in range(NX) for b in range(NY) if a or b),
            key=lambda p: -(min(p[0], 4 - p[0]) + min(p[1], 4 - p[1])),
        )
    ]

    def z_send(phase, src_at, dst):
        for zz in zpeers:
            send(phase, src_at(zz), dst, at_z(zz))

    def xy_send(phase, src_at, dst):
        for xx, yy in plane:
            send(phase, src_at(xx * 4 + yy), dst, at_xy(xx, yy))

    def done(phase, ref):
        recv(phase, ref)
        sent(phase, ref)

    bar = pltpu.get_barrier_semaphore()
    peers = [at_z(zz) for zz in zpeers] + [at_xy(*k) for k in plane] + [partner]
    peers += [across_z(zz) for zz in zpeers]
    for dev in peers:
        pl.semaphore_signal(bar, inc=1, device_id=dev, device_id_type=MESH)

    def qcols(zz, k):
        return r.wqkv.at[:, pl.ds(pl.multiple_of(k * 1024 + zz * 128, 128), 128)]

    def half_cols(k):
        return pl.ds(pl.multiple_of((2 * c + k) * 128, 128), 128)

    local = SimpleNamespace()
    begun = []

    def fetch(src, dst):
        k = pltpu.make_async_copy(src, dst, r.ls.at[len(begun)])
        k.start()
        begun.append(k)
        return k

    local.st = fetch(r.stream, r.st)
    local.gn = fetch(r.gains, r.gn)
    local.fq = fetch(r.freq, r.fq)
    local_wq = [fetch(qcols(z, 2 * c + k), r.wq.at[z, :, half_cols(k)]) for k in range(2)]
    local.wo = fetch(r.wout.at[:, pl.ds(pl.multiple_of(n * 256, 256), 256)], r.wo.at[n])
    local.kvv = fetch(r.kv, r.kvv)
    local.tg = fetch(r.targets, r.tg)
    local.wg = fetch(r.wgu, r.wg.at[:, 0:FFD])
    local.wd = fetch(r.wdown, r.wd.at[0:FFD])
    local.lm = fetch(r.lmh.at[pl.ds(pl.multiple_of(c * HALF, HALF), HALF)], r.lm)

    right, left = at_xy(rem(x + 1, NX), y), at_xy(rem(x + 3, NX), y)

    def weight_piece(i):
        cols = pl.ds(pl.multiple_of(c * HALF + i * 256, 256), 256)
        for dev, a, b in ((right, 0, 64), (left, 64, FFD)):
            g = r.wg.at[:, 128 + a : 128 + b, cols]
            send(p.xg, r.wgu.at[:, a:b, cols], g, dev, i // 4)
            send(p.xd, r.wdown.at[a:b, cols], r.wd.at[128 + a : 128 + b, cols], dev, i // 4)

    def pass_weights(g):
        cols = pl.ds(pl.multiple_of(c * HALF + g * 1024, 1024), 1024)
        for came, went, at in (
            (p.xg, p.fg, r.wg.at[:, 128 : 128 + FFD, cols]),
            (p.xd, p.fd, r.wd.at[128 : 128 + FFD, cols]),
        ):
            recv(came, at, g)
            send(went, at, at, partner, g)

    def spread(scratch, dst):
        for zz in range(NZ):
            dst[zz * 8 : zz * 8 + 8] = scratch[pl.ds(zz, 8, stride=8), :]

    z8 = pl.ds(pl.multiple_of(z * 8, 8), 8)

    def z_then_plane(zphase, pphase, s, rr, buf, start=True, beside=lambda: None):
        def piece(zz):
            return pl.ds(pl.multiple_of(zz * 8, 8), 8)

        if start:
            z_send(zphase, lambda zz: s.at[piece(zz)], rr.at[z8])
        beside()
        rr[z8, :] = s[z8, :]
        done(zphase, rr.at[0:56])
        for k in range(4):
            rows = [rr[pl.ds(j * 4 + k, 8, stride=8), :] for j in range(2)]
            buf[n, :, k * 128 : (k + 1) * 128] = jnp.concatenate(rows, axis=0).astype(BF)
        xy_send(pphase, lambda m: buf.at[n], buf.at[n])
        return lambda: done(pphase, buf.at[0:15])

    local.st.wait()
    x32 = r.st[...].astype(F32)
    rs = lax.rsqrt(jnp.mean(x32 * x32, axis=-1, keepdims=True) + 1e-5)
    for b in range(32):
        for j in range(2):
            r.sc[j * 32 + b : j * 32 + b + 1, :] = x32[j : j + 1, b * 128 : (b + 1) * 128]
    spread(r.sc, r.s1s)
    r.s4s[...] = jnp.zeros((128, 128), F32)
    row8 = lax.broadcasted_iota(jnp.int32, (8, 128), 0)
    lane8 = lax.broadcasted_iota(jnp.int32, (8, 128), 1)
    rs8 = jnp.where(row8 < 4, rs[0:1, 0:1], rs[1:2, 0:1])

    pl.semaphore_wait(bar, len(peers))

    for zz in zpeers:
        send(p.s1, r.s1s.at[pl.ds(pl.multiple_of(zz * 8, 8), 8)], r.s1r.at[z8], at_z(zz))
    for zz in zpeers:
        for k in range(2):
            send(p.wq, qcols(zz, 2 * c + k), r.wq.at[z, :, half_cols(k)], at_z(zz))
    weight_piece(0)
    weight_piece(1)
    send(p.fi, r.fin, r.fi, partner)
    send(p.fh, r.fhid, r.fh, partner)
    send(p.fo, r.fout, r.fo, partner)
    send(p.xh, r.fhid, r.fhx.at[0], right, 0)
    send(p.xh, r.fhid, r.fhx.at[1], left, 1)
    finish = z_then_plane(p.s1, p.s2, r.s1s, r.s1r, r.raw, False)
    local.fq.wait()
    local.gn.wait()
    pos = [r.lengths[rem(2 * t + j, B)] for j in range(2)]
    ang = jnp.where(row8 < 4, pos[0], pos[1]).astype(F32) * r.fq[0:1, :]
    cos8 = jnp.cos(ang)
    sin8 = jnp.where(lane8 < 64, -jnp.sin(ang), jnp.sin(ang))
    for b in range(32):
        r.g3[b : b + 1, :] = r.gn[2:3, b * 128 : (b + 1) * 128]

    for k in range(2):
        local_wq[k].wait()
    done(p.wq, r.wq.at[0:7, :, 0:256])
    mine = r.wq.at[:, :, pl.ds(pl.multiple_of(c * 256, 256), 256)]
    send(p.wqf, mine, mine, partner)
    done(p.wqf, mine)
    gq = jnp.concatenate(
        [r.gn[0:1, pl.ds(pl.multiple_of(k * 1024 + z * 128, 128), 128)] for k in range(4)], axis=1
    )
    finish()
    lhs = (r.raw[...].reshape(256, 512).astype(F32) * gq).astype(BF)
    prod = lax.dot_general(lhs, r.wq[...].reshape(QN, 512), NT, preferred_element_type=F32)
    for l in range(3):
        r.p1[l] = prod[:, l * 128 : (l + 1) * 128]
    for zz in range(NZ):
        for l in range(3):
            r.s3s[zz, :, l * 128 : (l + 1) * 128] = r.p1.at[l][
                pl.ds(zz, 32, stride=8), :
            ].astype(BF)
    z_send(p.s3, lambda zz: r.s3s.at[zz], r.s3r.at[z])
    xy_send(
        p.wo,
        lambda m: r.wout.at[:, pl.ds(pl.multiple_of(m * 256, 256), 256)],
        r.wo.at[n],
    )
    weight_piece(2)
    weight_piece(3)
    r.s3r[z] = r.s3s[z]
    done(p.s3, r.s3r.at[0:7])
    acc = r.s3r[0].astype(F32)
    for s in range(1, NZ):
        acc = acc + r.s3r[s].astype(F32)
    for l in range(3):
        r.q1[l] = acc[:, l * 128 : (l + 1) * 128]
    for l in range(3):
        for j in range(2):
            r.s4s[pl.ds(l * 2 + j, 16, stride=8), :] = r.q1.at[l][pl.ds(j, 16, stride=2), :]

    def tile(m):
        return pl.ds(pl.multiple_of(m * 8, 8), 8)

    xy_send(p.s4, lambda m: r.s4s.at[tile(m)], r.s4r.at[tile(n)])
    r.s4r[tile(n), :] = r.s4s[tile(n), :]
    done(p.s4, r.s4r.at[0:120])

    blocks = {
        (yy, l): jnp.concatenate(
            [r.s4r[pl.ds(yy * 8 + l * 2 + j, 4, stride=32), :] for j in range(2)], axis=0
        )
        for yy in range(NY)
        for l in range(3)
    }
    for hh in range(12):
        val = jnp.zeros((8, 128), F32)
        lane = 0
        while lane < 128:
            col = hh * 128 + lane
            tt, i = divmod(col, 48)
            at = (tt // 4) * 48 + i
            l, src = divmod(at, 128)
            width = min(48 - i, 128 - src, 128 - lane)
            piece = blocks[(tt % 4, l)]
            shift = (lane - src) % 128
            if shift:
                piece = pltpu.roll(piece, shift, 1)
            val = jnp.where((lane8 >= lane) & (lane8 < lane + width), piece, val)
            lane += width
        val = (val * rs8).astype(BF).astype(F32)
        turned = (val * cos8 + pltpu.roll(val, 64, 1) * sin8).astype(BF).astype(F32)
        if hh >= 4:
            turned = jnp.where(row8 % 4 == 3, val, turned)
        r.hs[pl.ds(hh, 8, stride=12), :] = turned

    local.kvv.wait()
    inv_root = HD**-0.5
    group = lax.broadcasted_iota(jnp.int32, (32, 128), 0) // 4
    group8 = (
        lax.broadcasted_iota(jnp.int32, (32, 8), 0) // 4
        == lax.broadcasted_iota(jnp.int32, (32, 8), 1)
    )
    place = lax.broadcasted_iota(jnp.int32, (32, CACHE), 1)
    for j in range(2):
        q = r.hs[j * 48 : j * 48 + 32, :]
        kn = r.hs[j * 48 + 32 : j * 48 + 40, :].astype(BF)
        vn = r.hs[j * 48 + 40 : j * 48 + 48, :].astype(BF)
        qd = jnp.concatenate([jnp.where(group == k, q, 0.0) for k in range(KV)], axis=1).astype(BF)
        scores = (
            lax.dot_general(qd, r.kvv[j, :, : KV * HD], NT, preferred_element_type=F32) * inv_root
        )
        fresh = lax.dot_general(q.astype(BF), kn, NT, preferred_element_type=F32)
        fresh = jnp.sum(jnp.where(group8, fresh, 0.0), axis=1, keepdims=True) * inv_root
        scores = jnp.where(place < pos[j], scores, -1e30)
        peak = jnp.maximum(jnp.max(scores, axis=1, keepdims=True), fresh)
        weights = jnp.exp(scores - peak)
        fresh_w = jnp.exp(fresh - peak)
        total = jnp.sum(weights, axis=1, keepdims=True) + fresh_w
        probs = (weights / total).astype(BF)
        fresh_p = jnp.where(group8, fresh_w / total, 0.0).astype(BF)
        wide = jnp.dot(probs, r.kvv[j, :, KV * HD :], preferred_element_type=F32)
        out = jnp.dot(fresh_p, vn, preferred_element_type=F32)
        for k in range(KV):
            out = out + jnp.where(group == k, wide[:, k * 128 : (k + 1) * 128], 0.0)
        r.osc[j * 32 : j * 32 + 32, :] = out.astype(BF).astype(F32)

    spread(r.osc, r.s5s)

    def beside():
        weight_piece(4)
        weight_piece(5)

    finish = z_then_plane(p.s5, p.s6, r.s5s, r.s5r, r.att, beside=beside)
    pass_weights(0)
    local.wo.wait()
    done(p.wo, r.wo.at[0:15])
    resid = r.raw[:, :, pl.ds(pl.multiple_of(x * 128, 128), 128)].reshape(256, 128).astype(F32)
    lo = resid * jnp.where(z == 2 * y, 1.0, 0.0)
    hi = resid * jnp.where(z == 2 * y + 1, 1.0, 0.0)
    finish()
    prod = jnp.dot(
        r.att[...].reshape(256, 512), r.wo[...].reshape(512, 256), preferred_element_type=F32
    ) + jnp.concatenate([lo, hi], axis=1)
    for h in range(2):
        for ys in range(NY):
            for j in range(2):
                at = [((m * 2 + h) * 4 + ys) * 16 + j * 8 for m in range(2)]
                r.s7s[h * 4 + ys, j * 16 : j * 16 + 16, :] = jnp.concatenate(
                    [prod[a : a + 8] for a in at], axis=0
                ).astype(BF)
    for zz in zpeers:
        send(p.s7, r.s7s.at[zz], r.s7r.at[z], across_z(zz))
    send(p.s7, r.s7s.at[z], r.s7r.at[z], partner)
    weight_piece(6)
    weight_piece(7)
    recv(p.xh, r.fhx.at[0], 0)
    recv(p.xh, r.fhx.at[1], 1)
    sent(p.xh, r.fhx)
    send(p.fy, r.fhx, r.fhy, partner)
    done(p.s7, r.s7r)
    acc = r.s7r[0].astype(F32)
    for s in range(1, NZ):
        acc = acc + r.s7r[s].astype(F32)

    z16 = pl.ds(pl.multiple_of(z * 16, 16), 16)
    for j in range(2):
        r.mc[j, z16, :] = acc[j * 16 : j * 16 + 16].astype(BF)
    for d in ZORDER:
        send(p.s8, r.mc.at[:, z16], r.mc.at[:, z16], at_z(rem(z + d, NZ)), 7 - d)

    def tile_on(zz):
        rows = pl.ds(pl.multiple_of(zz * 16, 16), 16)
        for d in (2, 1, 3):
            xx, yy = rem(x + d, NX), rem(y + d, NY)
            send(p.da, r.mc.at[par, rows], r.mid.at[n, rows], at_xy(x, yy), 6 - d)
            send(p.da, r.mc.at[rem(xx, 2), rows], r.mid.at[n, rows], at_xy(xx, y), 3 - d)
            send(p.db, r.mc.at[1 - par, rows, right_cols], r.xb.at[y, rows], at_xy(x, yy), 3 - d)

    left_cols, right_cols = pl.ds(0, 128), pl.ds(128, 128)
    tile_on(z)
    pass_weights(1)
    r.accg[...] = jnp.zeros((128, 256), F32)
    r.accu[...] = jnp.zeros((128, 256), F32)
    r.ssq[...] = jnp.zeros((128, 128), F32)
    for a in (FFD, 128 + FFD):
        r.wg[:, a : a + 16, :] = jnp.zeros((2, 16, D), BF)
        r.wd[a : a + 16, :] = jnp.zeros((16, D), BF)
    done(p.fi, r.fi)
    done(p.fh, r.fh)
    done(p.fo, r.fo)
    done(p.fy, r.fhy)
    r.fhp[...] = jnp.zeros((3, 2, 256), F32)
    r.fhp[:, :, 0:FFD] = r.fh[...]
    lane_h = lax.broadcasted_iota(jnp.int32, (3, 2, FFD), 2)
    r.fhp[:, :, 128 : 128 + FFD] = jnp.where(lane_h < 64, r.fhy[0], r.fhy[1])
    mine_g = r.wg.at[:, 128 : 128 + FFD, 0:HALF]
    mine_d = r.wd.at[128 : 128 + FFD, 0:HALF]
    for k in (p.xg, p.fg):
        sent(k, mine_g)
    for k in (p.xd, p.fd):
        sent(k, mine_d)
    for k in (local.wg, local.wd):
        k.wait()
    for d in (1, 7, 2, 6, 3, 5, 4):
        recv(p.s8, r.mc.at[:, 0:16], d - 1)
        tile_on(rem(z + d, NZ))
    sent(p.s8, r.mc.at[:, 0:112])

    near = (1, 3, 2)
    sent(p.da, r.mid.at[0:6])
    sent(p.db, r.xb.at[0:3])
    r.mid[n] = r.mc[par]
    for g in range(2):
        cols = pl.ds(pl.multiple_of((1 - c) * HALF + g * 1024, 1024), 1024)
        recv(p.fg, r.wg.at[:, 128 : 128 + FFD, cols], g)
        recv(p.fd, r.wd.at[128 : 128 + FFD, cols], g)

    def ffn_chunk(m):
        v = r.mid[m].astype(F32)
        r.ssq[...] += v[:, :128] * v[:, :128] + v[:, 128:] * v[:, 128:]
        cols = pl.ds(pl.multiple_of(m * 256, 256), 256)
        g = r.gn[1:2, cols]
        v4 = v.reshape(8, 2, 8, 256)
        for k, total in enumerate((r.accg, r.accu)):
            f = jnp.concatenate(
                [
                    (r.fi[i, k : k + 1, cols] * g).reshape(1, 1, 1, 256)
                    for i in range(2)
                ],
                axis=1,
            )
            act = (v4 * f).reshape(128, 256).astype(BF)
            total[...] += lax.dot_general(
                act, r.wg[k, :, cols], NT, preferred_element_type=F32
            )

    ffn_chunk(n)
    for d in near:
        m = rem(x + d, NX) * 4 + y
        recv(p.da, r.mid.at[m], d - 1)
        for e in (2, 1, 3):
            yy = rem(y + e, NY)
            at = r.mid.at[m, :, left_cols]
            send(p.dg, at, at, at_xy(x, yy), (d - 1) * 3 + 3 - e)
        yy = rem(y + d, NY)
        m = x * 4 + yy
        recv(p.da, r.mid.at[m], d + 2)
        recv(p.db, r.xb.at[yy], d - 1)
        for e in (2, 1, 3):
            xx = rem(x + e, NX)
            to = r.mid.at[m, :, right_cols]
            at = to if e == 2 else r.xb.at[yy]
            send(p.dg, at, to, at_xy(xx, y), (3 - e) * 3 + d - 1)
    sent(p.dg, r.mid.at[0:9])

    def line_step(i, carry):
        ffn_chunk(rem(x + 1 + i, NX) * 4 + y)
        ffn_chunk(x * 4 + rem(y + 1 + i, NY))
        return carry

    lax.fori_loop(0, 3, line_step, 0)

    def diag_step(i, carry):
        m = rem(x + 1 + i // 3, NX) * 4 + rem(y + 1 + i % 3, NY)
        recv(p.dg, r.mid.at[m], i)
        ffn_chunk(m)
        return carry

    lax.fori_loop(0, 9, diag_step, 0)
    scale = lax.rsqrt(jnp.sum(r.ssq[...], axis=1, keepdims=True) * (1.0 / D) + 1e-5)

    def by_member(k):
        return jnp.concatenate(
            [r.fhp[k, i : i + 1, :].reshape(1, 1, 1, 256) for i in range(2)], axis=1
        )

    gate = (r.accg[...] * scale).reshape(8, 2, 8, 256) * by_member(0)
    up = (r.accu[...] * scale).reshape(8, 2, 8, 256) * by_member(1)
    hidden = gate / (1.0 + jnp.exp(-gate)) * up * by_member(2)
    r.hid[...] = hidden.reshape(128, 256).astype(BF)

    def chunk(ch):
        return pl.ds(pl.multiple_of(ch * CW, CW), CW)

    def high(ch):
        return pl.ds(pl.multiple_of(HALF + ch * CW, CW), CW)

    other = 1 - xl
    opposite = at_xy(rem(x + 2, NX), y)

    def a1(ch):
        send(p.a1, r.p3.at[other, :, :, chunk(ch)], r.r1a.at[:, :, chunk(ch)], opposite, ch)

    def b1(ch, yy):
        at = r.p3.at[:, yy, :, high(ch)]
        send(p.b1, at, r.r1b.at[y, :, :, chunk(ch)], at_xy(x, yy), ch)

    def down_step(ch, carry):
        for cols in (chunk(ch), high(ch)):
            v = jnp.dot(r.hid[...], r.wd[:, cols], preferred_element_type=F32)
            r.p3[:, :, :, cols] = v.astype(BF).reshape(2, NY, 16, CW)
        a1(ch)
        for d in (2, 1, 3):
            b1(ch, rem(y + d, NY))
        return carry

    lax.fori_loop(0, NCH, down_step, 0)

    def a2(ch, yy):
        send(p.a2, r.s2a.at[yy, :, chunk(ch)], r.r2a.at[y, :, chunk(ch)], at_xy(x, yy), ch)

    def b2(ch):
        send(p.b2, r.s2b.at[other, :, chunk(ch)], r.r2b.at[:, chunk(ch)], opposite, ch)

    def second_step(ch, carry):
        recv(p.a1, r.r1a.at[:, :, chunk(ch)], ch)
        v = r.p3[xl, :, :, chunk(ch)].astype(F32) + r.r1a[:, :, chunk(ch)].astype(F32)
        r.s2a[:, :, chunk(ch)] = v.astype(BF)
        for d in (2, 1, 3):
            a2(ch, rem(y + d, NY))
        recv(p.b1, r.r1b.at[0:3, :, :, chunk(ch)], ch)
        v = r.p3[:, y, :, high(ch)].astype(F32)
        for d in near:
            v = v + r.r1b[rem(y + d, NY), :, :, chunk(ch)].astype(F32)
        r.s2b[:, :, chunk(ch)] = v.astype(BF)
        b2(ch)
        return carry

    lax.fori_loop(0, NCH, second_step, 0)
    sent(p.a1, r.r1a)
    sent(p.b1, r.r1b.at[0:3])
    sent(p.a2, r.r2a.at[0:3])
    sent(p.b2, r.r2b)

    row16 = lax.broadcasted_iota(jnp.int32, (16, 128), 0)
    own_row = rem(row16, 8) == z
    tile16 = pl.ds(pl.multiple_of((xl * 4 + y) * 16, 16), 16)

    def last_step(ch):
        recv(p.a2, r.r2a.at[0:3, :, chunk(ch)], ch)
        recv(p.b2, r.r2b.at[:, chunk(ch)], ch)
        for b in [*range(ch * 4, ch * 4 + 4), *range(16 + ch * 4, 20 + ch * 4)]:
            cols = slice((b % 16) * 128, (b % 16 + 1) * 128)
            if b < 16:
                v = r.s2a[y, :, cols].astype(F32)
                for d in near:
                    v = v + r.r2a[rem(y + d, NY), :, cols].astype(F32)
            else:
                v = r.s2b[xl, :, cols].astype(F32) + r.r2b[:, cols].astype(F32)
            at = slice(b * 128, (b + 1) * 128)
            v = v * jnp.where(row16 < 8, r.fo[0:1, at], r.fo[1:2, at])
            m = r.mid[b // 2, tile16, (b % 2) * 128 : (b % 2 + 1) * 128].astype(F32)
            r.f3[b * 16 : (b + 1) * 16, :] = v + jnp.where(own_row, m, 0.0)
        for zz in range(NZ):
            r.s13s[zz, ch] = chunk_rows(zz, ch).astype(BF)
        for zz in zpeers:
            send(p.s13, r.s13s.at[zz, ch], r.s13r.at[z, ch], at_z(zz), ch)

    def chunk_rows(zz, ch):
        return jnp.concatenate(
            [
                r.f3[pl.ds(h * 256 + ch * 64 + m * 8 + zz, 4, stride=16), :]
                for m in range(2)
                for h in range(2)
            ],
            axis=0,
        )

    for ch in range(NCH):
        last_step(ch)
    for ch in range(NCH):
        v = chunk_rows(z, ch)
        recv(p.s13, r.s13r.at[0:7, ch], ch)
        for zz in zpeers:
            v = v + r.s13r[zz, ch].astype(F32)
        for m in range(2):
            for h in range(2):
                at = m * 32 + h * 16 + ch * 4
                r.vs[at : at + 4, :] = v[m * 8 + h * 4 : m * 8 + h * 4 + 4]
    sent(p.s13, r.s13r.at[0:7])
    both = jnp.zeros((32, 128), F32)
    for m in range(2):
        v = r.vs[m * 32 : m * 32 + 32, :]
        v = v.astype(BF).astype(F32)
        mean = jnp.sum(jnp.sum(v * v, axis=1, keepdims=True), axis=0, keepdims=True) * (1.0 / D)
        both = both + (v * lax.rsqrt(mean + 1e-5) * r.g3[...]).astype(BF).astype(F32)
    r.fs[...] = both

    def half(k):
        return pl.ds(pl.multiple_of(k * 16, 16), 16)

    send(p.fx, r.fs.at[half(1 - c)], r.fr, partner)
    done(p.fx, r.fr)
    r.fb[own, z] = ((r.fs[half(c), :] + r.fr[...]) * 0.25).astype(BF)
    z_send(p.s14, lambda zz: r.fb.at[own, z], r.fb.at[own, z])
    local.lm.wait()
    local.tg.wait()
    wanted = jnp.broadcast_to(r.tg[...].astype(F32), (B, B)).T[:, 0:1]
    done(p.s14, r.fb.at[own, 0:7])
    xy_send(p.s15, lambda m: r.fb.at[own], r.fb.at[own])
    done(p.s15, r.fb.at[0:15])
    r.ff[...] = r.fb[...].reshape(2048, 128).astype(F32)
    for b in range(16):
        rows = [
            r.ff[pl.ds(h * 1024 + zz * 16 + b, 8, stride=128), :]
            for h in range(2)
            for zz in range(NZ)
        ]
        r.lh[:, b * 128 : (b + 1) * 128] = jnp.concatenate(rows, axis=0).astype(BF)
    for h in range(2):
        at = slice(h * 256, (h + 1) * 256)
        r.lp[:, at] = jnp.dot(r.lh[...], r.lm[:, at], preferred_element_type=F32)
        send(p.lx, r.lp.at[:, at], r.lr.at[:, at], partner, h)
    for h in range(2):
        recv(p.lx, r.lr.at[:, h * 256 : (h + 1) * 256], h)
    sent(p.lx, r.lr)
    mean_f = r.lp[...] + r.lr[...]
    r.logits_o[...] = mean_f.astype(BF)

    ids = (lax.broadcasted_iota(jnp.int32, (B, VD), 1) + t * VD).astype(F32)
    found = jnp.sum(jnp.where(ids == wanted, mean_f, 0.0), axis=1, keepdims=True)
    peak = jnp.max(mean_f, axis=1, keepdims=True)
    total = jnp.sum(jnp.exp(mean_f - peak), axis=1, keepdims=True)
    lane = lax.broadcasted_iota(jnp.int32, (B, B), 1)
    stat = jnp.where(lane == 0, peak, jnp.where(lane == 1, total, jnp.where(lane == 2, found, 0.0)))
    r.sz[z] = stat.T[:8]

    def combine(ref, count):
        peaks = [ref[k, 0:1, :] for k in range(count)]
        top_ = peaks[0]
        for k in range(1, count):
            top_ = jnp.maximum(top_, peaks[k])
        tot = ref[0, 1:2, :] * jnp.exp(peaks[0] - top_)
        hit = ref[0, 2:3, :]
        for k in range(1, count):
            tot = tot + ref[k, 1:2, :] * jnp.exp(peaks[k] - top_)
            hit = hit + ref[k, 2:3, :]
        return top_, tot, hit

    z_send(p.s16, lambda zz: r.sz.at[z], r.sz.at[z])
    done(p.s16, r.sz.at[0:7])
    a, b_, h = combine(r.sz, NZ)
    r.sx[n] = jnp.concatenate([a, b_, h, jnp.zeros((5, 128), F32)], axis=0)
    xy_send(p.s17, lambda m: r.sx.at[n], r.sx.at[n])
    done(p.s17, r.sx.at[0:15])
    a, b_, h = combine(r.sx, NP)
    r.lp_o[...] = h - (a + jnp.log(b_))

    for sem, ref in drains:
        wait_bytes(sem, ref)


def hand_on(logits, logprob, logits_o, logprob_o):
    logits_o[...] = logits[...]
    logprob_o[...] = logprob[...]


def body(
    stream_in, kv_cache, lengths, targets, norm_gains, w_qkv, w_out, w_gate_up, w_down, lm_head,
    fast_in, fast_hidden, fast_out,
):
    freq = np.float32(500000.0) ** (-np.arange(64, dtype=np.float32) * 2.0 / 128)
    freq = jnp.asarray(np.concatenate([freq, freq])[None, :], F32)
    args = dict(
        stream=stream_in, kv=kv_cache, lengths=lengths, targets=targets.reshape(1, B),
        gains=norm_gains, wqkv=w_qkv.T, wout=w_out,
        wgu=w_gate_up.swapaxes(1, 2), wdown=w_down, lmh=lm_head,
        fin=fast_in, fhid=fast_hidden.swapaxes(0, 1), fout=fast_out, freq=freq,
    )
    got = pl.pallas_call(
        functools.partial(kernel, list(args)),
        out_shape=list(OUTS.values()),
        in_specs=[
            pl.BlockSpec(memory_space=pltpu.SMEM if v is lengths else pl.ANY)
            for v in args.values()
        ],
        out_specs=[pl.BlockSpec(memory_space=VM)] * len(OUTS),
        scratch_shapes=[
            *SCRATCH.values(),
            *LS.values(),
            *(DMA((count,)) for n in PHASES.values() for count in (1, n)),
        ],
        compiler_params=pltpu.CompilerParams(
            collective_id=0, has_side_effects=True, vmem_limit_bytes=60 * 1024 * 1024
        ),
        name="step",
    )(*args.values())
    got = pl.pallas_call(hand_on, out_shape=list(OUTS.values()), name="result")(*got)
    return (got[0], got[1].reshape(B))


MEMBER_TP = ("member", "tp_0", "tp_1", "tp_2")
TP = ("tp_0", "tp_1", "tp_2")
IN_SPECS = (
    P(MEMBER_TP, None), P(MEMBER_TP, None, None), P(), P(), P(), P(None, TP), P(TP, None),
    P(None, None, TP), P(TP, None), P(None, TP), P("member", None, None), P("member", None, TP),
    P("member", None),
)


def solution(mesh):
    split = Mesh(
        mesh.devices.reshape(mesh.shape["member"], NX, NZ, NY), MEMBER_TP
    )
    return jax.shard_map(
        body, mesh=split, in_specs=IN_SPECS, out_specs=(P(None, TP), P()), check_vma=False
    )
```

```python
import functools
from types import SimpleNamespace

import jax
import jax.numpy as jnp
import numpy as np
from jax import lax
from jax.experimental import pallas as pl
from jax.experimental.pallas import tpu as pltpu
from jax.sharding import Mesh
from jax.sharding import PartitionSpec as P

MESH = pl.DeviceIdType.MESH
F32 = jnp.float32
BF = jnp.bfloat16
NX, NZ, NY = 4, 8, 4
NP = NX * NY
D, HEADS, KV, HD, CACHE, FFD, VD = 4096, 32, 8, 128, 512, 112, 512
B = 128
QN = 384
ZORDER = (4, 3, 5, 2, 6, 1, 7)
NCH, CA, CB = 4, 640, 384
WA, WB = NCH * CA, NCH * CB
BA, BB = CA // 128, CB // 128
HALF = D // 2
NT = (((1,), (1,)), ((), ()))

VM = pltpu.VMEM
DMA = pltpu.SemaphoreType.DMA

SCRATCH = dict(
    st=VM((2, D), BF),
    kvv=VM((2, CACHE, 2 * KV * HD), BF),
    tg=VM((1, B), jnp.int32),
    gn=VM((3, D), F32),
    fi=VM((2, 2, D), F32),
    fh=VM((3, 2, FFD), F32),
    fo=VM((2, D), F32),
    fq=VM((1, 128), F32),
    wq=VM((NZ, 48, 512), BF),
    wo=VM((NP, 32, 256), BF),
    wg=VM((2, 256, D), BF),
    wd=VM((256, D), BF),
    fhx=VM((2, 3, 2, FFD), F32),
    fhy=VM((2, 3, 2, FFD), F32),
    fhp=VM((3, 2, 256), F32),
    lm=VM((HALF, VD), BF),
    sc=VM((64, 128), F32),
    s1s=VM((64, 128), F32),
    s1r=VM((64, 128), F32),
    raw=VM((NP, 16, 512), BF),
    p1=VM((3, 256, 128), F32),
    s3s=VM((NZ, 32, QN), BF),
    s3r=VM((NZ, 32, QN), BF),
    q1=VM((3, 32, 128), F32),
    s4s=VM((128, 128), F32),
    s4r=VM((128, 128), F32),
    hs=VM((96, 128), F32),
    osc=VM((64, 128), F32),
    s5s=VM((64, 128), F32),
    s5r=VM((64, 128), F32),
    att=VM((NP, 16, 512), BF),
    s7s=VM((NZ, 32, 256), BF),
    s7r=VM((NZ, 32, 256), BF),
    mc=VM((2, 128, 256), BF),
    xb=VM((NY, 128, 128), BF),
    mid=VM((NP, 128, 256), BF),
    accg=VM((128, 256), F32),
    accu=VM((128, 256), F32),
    ssq=VM((128, 128), F32),
    hid=VM((128, 256), BF),
    p3=VM((2, NY, 16, D), BF),
    r1a=VM((NY, 16, WA), BF),
    r1b=VM((NY, 2, 16, WB), BF),
    s2a=VM((NY, 16, WA), BF),
    s2b=VM((2, 16, WB), BF),
    r2a=VM((NY, 16, WA), BF),
    r2b=VM((16, WB), BF),
    f3=VM((512, 128), F32),
    g3=VM((32, 128), F32),
    s13s=VM((NZ, NCH, 16, 128), BF),
    s13r=VM((NZ, NCH, 16, 128), BF),
    vs=VM((64, 128), F32),
    fs=VM((32, 128), F32),
    fr=VM((16, 128), F32),
    fb=VM((NP, NZ, 16, 128), BF),
    ff=VM((2048, 128), F32),
    lh=VM((B, HALF), BF),
    lp=VM((B, VD), F32),
    lr=VM((B, VD), F32),
    sz=VM((NZ, 8, 128), F32),
    sx=VM((NP, 8, 128), F32),
)
PHASES = dict(
    wq=1, wqf=1, wo=1, s1=1, s2=1, s3=1, s4=1, s5=1, s6=1, s7=1, s8=7, da=6, db=3, dg=9,
    xg=2, xd=2, fg=2, fd=2, xh=2, fi=1, fh=1, fo=1, fy=1,
    a1=NCH, b1=NCH, a2=NCH, b2=NCH, s13=NCH, fx=1, s14=7, s15=1, lx=2, s16=1, s17=1,
)
LS = dict(ls=DMA((16,)))
OUTS = dict(
    logits_o=jax.ShapeDtypeStruct((B, VD), BF), lp_o=jax.ShapeDtypeStruct((1, B), F32)
)


def kernel(inputs, *refs):
    names = [*inputs, *OUTS, *SCRATCH, *LS]
    r = SimpleNamespace(**dict(zip(names, refs)))
    sems = iter(refs[len(names) :])
    p = SimpleNamespace(**{k: (next(sems), next(sems)) for k in PHASES})
    c, x, z, y = (lax.axis_index(a) for a in MEMBER_TP)
    t = x * 32 + z * 4 + y
    n = x * 4 + y
    xl, par = x // 2, lax.rem(x, 2)
    own = xl * 8 + y * 2 + par
    drains = []
    def rem(v, k):
        return lax.rem(v, k)

    def at_z(zz):
        return (c, x, zz, y)

    def at_xy(xx, yy):
        return (c, xx, z, yy)

    partner = (1 - c, x, z, y)

    def across_z(zz):
        return (1 - c, x, zz, y)

    def copy(phase, src, dst, dev, slot=0):
        return pltpu.make_async_remote_copy(
            src_ref=src,
            dst_ref=dst,
            send_sem=phase[0].at[0],
            recv_sem=phase[1].at[slot],
            device_id=dev,
            device_id_type=MESH,
        )

    def send(phase, src, dst, dev, slot=0):
        copy(phase, src, dst, dev, slot).start()

    def wait_bytes(sem, ref):
        pltpu.make_async_copy(ref, ref, sem).wait()

    def recv(phase, ref, slot=0):
        wait_bytes(phase[1].at[slot], ref)

    def sent(phase, ref):
        drains.append((phase[0].at[0], ref))

    zpeers = [rem(z + d, NZ) for d in ZORDER]
    plane = [
        (rem(x + dx, NX), rem(y + dy, NY))
        for dx, dy in sorted(
            ((a, b) for a in range(NX) for b in range(NY) if a or b),
            key=lambda p: -(min(p[0], 4 - p[0]) + min(p[1], 4 - p[1])),
        )
    ]

    def z_send(phase, src_at, dst):
        for zz in zpeers:
            send(phase, src_at(zz), dst, at_z(zz))

    def xy_send(phase, src_at, dst):
        for xx, yy in plane:
            send(phase, src_at(xx * 4 + yy), dst, at_xy(xx, yy))

    def done(phase, ref):
        recv(phase, ref)
        sent(phase, ref)

    bar = pltpu.get_barrier_semaphore()
    peers = [at_z(zz) for zz in zpeers] + [at_xy(*k) for k in plane] + [partner]
    peers += [across_z(zz) for zz in zpeers]
    for dev in peers:
        pl.semaphore_signal(bar, inc=1, device_id=dev, device_id_type=MESH)

    def qcols(zz, k):
        return r.wqkv.at[:, pl.ds(pl.multiple_of(k * 1024 + zz * 128, 128), 128)]

    def half_cols(k):
        return pl.ds(pl.multiple_of((2 * c + k) * 128, 128), 128)

    local = SimpleNamespace()
    begun = []

    def fetch(src, dst):
        k = pltpu.make_async_copy(src, dst, r.ls.at[len(begun)])
        k.start()
        begun.append(k)
        return k

    local.st = fetch(r.stream, r.st)
    local.gn = fetch(r.gains, r.gn)
    local.fq = fetch(r.freq, r.fq)
    local_wq = [fetch(qcols(z, 2 * c + k), r.wq.at[z, :, half_cols(k)]) for k in range(2)]
    local.wo = fetch(r.wout.at[:, pl.ds(pl.multiple_of(n * 256, 256), 256)], r.wo.at[n])
    local.kvv = fetch(r.kv, r.kvv)
    local.tg = fetch(r.targets, r.tg)
    local.wg = fetch(r.wgu, r.wg.at[:, 0:FFD])
    local.wd = fetch(r.wdown, r.wd.at[0:FFD])
    local.lm = fetch(r.lmh.at[pl.ds(pl.multiple_of(c * HALF, HALF), HALF)], r.lm)

    right, left = at_xy(rem(x + 1, NX), y), at_xy(rem(x + 3, NX), y)

    def weight_piece(i):
        cols = pl.ds(pl.multiple_of(c * HALF + i * 256, 256), 256)
        for dev, a, b in ((right, 0, 64), (left, 64, FFD)):
            g = r.wg.at[:, 128 + a : 128 + b, cols]
            send(p.xg, r.wgu.at[:, a:b, cols], g, dev, i // 4)
            send(p.xd, r.wdown.at[a:b, cols], r.wd.at[128 + a : 128 + b, cols], dev, i // 4)

    def pass_weights(g):
        cols = pl.ds(pl.multiple_of(c * HALF + g * 1024, 1024), 1024)
        for came, went, at in (
            (p.xg, p.fg, r.wg.at[:, 128 : 128 + FFD, cols]),
            (p.xd, p.fd, r.wd.at[128 : 128 + FFD, cols]),
        ):
            recv(came, at, g)
            send(went, at, at, partner, g)

    def spread(scratch, dst):
        for zz in range(NZ):
            dst[zz * 8 : zz * 8 + 8] = scratch[pl.ds(zz, 8, stride=8), :]

    z8 = pl.ds(pl.multiple_of(z * 8, 8), 8)

    def z_then_plane(zphase, pphase, s, rr, buf, start=True, beside=lambda: None):
        def piece(zz):
            return pl.ds(pl.multiple_of(zz * 8, 8), 8)

        if start:
            z_send(zphase, lambda zz: s.at[piece(zz)], rr.at[z8])
        beside()
        rr[z8, :] = s[z8, :]
        done(zphase, rr.at[0:56])
        for k in range(4):
            rows = [rr[pl.ds(j * 4 + k, 8, stride=8), :] for j in range(2)]
            buf[n, :, k * 128 : (k + 1) * 128] = jnp.concatenate(rows, axis=0).astype(BF)
        xy_send(pphase, lambda m: buf.at[n], buf.at[n])
        return lambda: done(pphase, buf.at[0:15])

    local.st.wait()
    x32 = r.st[...].astype(F32)
    rs = lax.rsqrt(jnp.mean(x32 * x32, axis=-1, keepdims=True) + 1e-5)
    for b in range(32):
        for j in range(2):
            r.sc[j * 32 + b : j * 32 + b + 1, :] = x32[j : j + 1, b * 128 : (b + 1) * 128]
    spread(r.sc, r.s1s)
    r.s4s[...] = jnp.zeros((128, 128), F32)
    row8 = lax.broadcasted_iota(jnp.int32, (8, 128), 0)
    lane8 = lax.broadcasted_iota(jnp.int32, (8, 128), 1)
    rs8 = jnp.where(row8 < 4, rs[0:1, 0:1], rs[1:2, 0:1])

    pl.semaphore_wait(bar, len(peers))

    for zz in zpeers:
        send(p.s1, r.s1s.at[pl.ds(pl.multiple_of(zz * 8, 8), 8)], r.s1r.at[z8], at_z(zz))
    for zz in zpeers:
        for k in range(2):
            send(p.wq, qcols(zz, 2 * c + k), r.wq.at[z, :, half_cols(k)], at_z(zz))
    weight_piece(0)
    weight_piece(1)
    send(p.fi, r.fin, r.fi, partner)
    send(p.fh, r.fhid, r.fh, partner)
    send(p.fo, r.fout, r.fo, partner)
    send(p.xh, r.fhid, r.fhx.at[0], right, 0)
    send(p.xh, r.fhid, r.fhx.at[1], left, 1)
    finish = z_then_plane(p.s1, p.s2, r.s1s, r.s1r, r.raw, False)
    local.fq.wait()
    local.gn.wait()
    pos = [r.lengths[rem(2 * t + j, B)] for j in range(2)]
    ang = jnp.where(row8 < 4, pos[0], pos[1]).astype(F32) * r.fq[0:1, :]
    cos8 = jnp.cos(ang)
    sin8 = jnp.where(lane8 < 64, -jnp.sin(ang), jnp.sin(ang))
    for b in range(32):
        r.g3[b : b + 1, :] = r.gn[2:3, b * 128 : (b + 1) * 128]

    for k in range(2):
        local_wq[k].wait()
    done(p.wq, r.wq.at[0:7, :, 0:256])
    mine = r.wq.at[:, :, pl.ds(pl.multiple_of(c * 256, 256), 256)]
    send(p.wqf, mine, mine, partner)
    done(p.wqf, mine)
    gq = jnp.concatenate(
        [r.gn[0:1, pl.ds(pl.multiple_of(k * 1024 + z * 128, 128), 128)] for k in range(4)], axis=1
    )
    finish()
    lhs = (r.raw[...].reshape(256, 512).astype(F32) * gq).astype(BF)
    prod = lax.dot_general(lhs, r.wq[...].reshape(QN, 512), NT, preferred_element_type=F32)
    for l in range(3):
        r.p1[l] = prod[:, l * 128 : (l + 1) * 128]
    for zz in range(NZ):
        for l in range(3):
            r.s3s[zz, :, l * 128 : (l + 1) * 128] = r.p1.at[l][
                pl.ds(zz, 32, stride=8), :
            ].astype(BF)
    z_send(p.s3, lambda zz: r.s3s.at[zz], r.s3r.at[z])
    weight_piece(2)
    weight_piece(3)
    r.s3r[z] = r.s3s[z]
    done(p.s3, r.s3r.at[0:7])
    acc = r.s3r[0].astype(F32)
    for s in range(1, NZ):
        acc = acc + r.s3r[s].astype(F32)
    for l in range(3):
        r.q1[l] = acc[:, l * 128 : (l + 1) * 128]
    for l in range(3):
        for j in range(2):
            r.s4s[pl.ds(l * 2 + j, 16, stride=8), :] = r.q1.at[l][pl.ds(j, 16, stride=2), :]

    def tile(m):
        return pl.ds(pl.multiple_of(m * 8, 8), 8)

    xy_send(p.s4, lambda m: r.s4s.at[tile(m)], r.s4r.at[tile(n)])
    xy_send(
        p.wo,
        lambda m: r.wout.at[:, pl.ds(pl.multiple_of(m * 256, 256), 256)],
        r.wo.at[n],
    )
    r.s4r[tile(n), :] = r.s4s[tile(n), :]
    done(p.s4, r.s4r.at[0:120])

    blocks = {
        (yy, l): jnp.concatenate(
            [r.s4r[pl.ds(yy * 8 + l * 2 + j, 4, stride=32), :] for j in range(2)], axis=0
        )
        for yy in range(NY)
        for l in range(3)
    }
    for hh in range(12):
        val = jnp.zeros((8, 128), F32)
        lane = 0
        while lane < 128:
            col = hh * 128 + lane
            tt, i = divmod(col, 48)
            at = (tt // 4) * 48 + i
            l, src = divmod(at, 128)
            width = min(48 - i, 128 - src, 128 - lane)
            piece = blocks[(tt % 4, l)]
            shift = (lane - src) % 128
            if shift:
                piece = pltpu.roll(piece, shift, 1)
            val = jnp.where((lane8 >= lane) & (lane8 < lane + width), piece, val)
            lane += width
        val = (val * rs8).astype(BF).astype(F32)
        turned = (val * cos8 + pltpu.roll(val, 64, 1) * sin8).astype(BF).astype(F32)
        if hh >= 4:
            turned = jnp.where(row8 % 4 == 3, val, turned)
        r.hs[pl.ds(hh, 8, stride=12), :] = turned

    local.kvv.wait()
    inv_root = HD**-0.5
    group = lax.broadcasted_iota(jnp.int32, (32, 128), 0) // 4
    group8 = (
        lax.broadcasted_iota(jnp.int32, (32, 8), 0) // 4
        == lax.broadcasted_iota(jnp.int32, (32, 8), 1)
    )
    place = lax.broadcasted_iota(jnp.int32, (32, CACHE), 1)
    for j in range(2):
        q = r.hs[j * 48 : j * 48 + 32, :]
        kn = r.hs[j * 48 + 32 : j * 48 + 40, :].astype(BF)
        vn = r.hs[j * 48 + 40 : j * 48 + 48, :].astype(BF)
        qd = jnp.concatenate([jnp.where(group == k, q, 0.0) for k in range(KV)], axis=1).astype(BF)
        scores = (
            lax.dot_general(qd, r.kvv[j, :, : KV * HD], NT, preferred_element_type=F32) * inv_root
        )
        fresh = lax.dot_general(q.astype(BF), kn, NT, preferred_element_type=F32)
        fresh = jnp.sum(jnp.where(group8, fresh, 0.0), axis=1, keepdims=True) * inv_root
        scores = jnp.where(place < pos[j], scores, -1e30)
        peak = jnp.maximum(jnp.max(scores, axis=1, keepdims=True), fresh)
        weights = jnp.exp(scores - peak)
        fresh_w = jnp.exp(fresh - peak)
        total = jnp.sum(weights, axis=1, keepdims=True) + fresh_w
        probs = (weights / total).astype(BF)
        fresh_p = jnp.where(group8, fresh_w / total, 0.0).astype(BF)
        wide = jnp.dot(probs, r.kvv[j, :, KV * HD :], preferred_element_type=F32)
        out = jnp.dot(fresh_p, vn, preferred_element_type=F32)
        for k in range(KV):
            out = out + jnp.where(group == k, wide[:, k * 128 : (k + 1) * 128], 0.0)
        r.osc[j * 32 : j * 32 + 32, :] = out.astype(BF).astype(F32)

    spread(r.osc, r.s5s)

    def beside():
        weight_piece(4)
        weight_piece(5)

    finish = z_then_plane(p.s5, p.s6, r.s5s, r.s5r, r.att, beside=beside)
    pass_weights(0)
    local.wo.wait()
    done(p.wo, r.wo.at[0:15])
    resid = r.raw[:, :, pl.ds(pl.multiple_of(x * 128, 128), 128)].reshape(256, 128).astype(F32)
    lo = resid * jnp.where(z == 2 * y, 1.0, 0.0)
    hi = resid * jnp.where(z == 2 * y + 1, 1.0, 0.0)
    finish()
    prod = jnp.dot(
        r.att[...].reshape(256, 512), r.wo[...].reshape(512, 256), preferred_element_type=F32
    ) + jnp.concatenate([lo, hi], axis=1)
    for h in range(2):
        for ys in range(NY):
            for j in range(2):
                at = [((m * 2 + h) * 4 + ys) * 16 + j * 8 for m in range(2)]
                r.s7s[h * 4 + ys, j * 16 : j * 16 + 16, :] = jnp.concatenate(
                    [prod[a : a + 8] for a in at], axis=0
                ).astype(BF)
    for zz in zpeers:
        send(p.s7, r.s7s.at[zz], r.s7r.at[z], across_z(zz))
    send(p.s7, r.s7s.at[z], r.s7r.at[z], partner)
    weight_piece(6)
    weight_piece(7)
    recv(p.xh, r.fhx.at[0], 0)
    recv(p.xh, r.fhx.at[1], 1)
    sent(p.xh, r.fhx)
    send(p.fy, r.fhx, r.fhy, partner)
    done(p.s7, r.s7r)
    acc = r.s7r[0].astype(F32)
    for s in range(1, NZ):
        acc = acc + r.s7r[s].astype(F32)

    z16 = pl.ds(pl.multiple_of(z * 16, 16), 16)
    for j in range(2):
        r.mc[j, z16, :] = acc[j * 16 : j * 16 + 16].astype(BF)
    for d in ZORDER:
        send(p.s8, r.mc.at[:, z16], r.mc.at[:, z16], at_z(rem(z + d, NZ)), 7 - d)

    def tile_on(zz):
        rows = pl.ds(pl.multiple_of(zz * 16, 16), 16)
        for d in (2, 1, 3):
            xx, yy = rem(x + d, NX), rem(y + d, NY)
            send(p.da, r.mc.at[par, rows], r.mid.at[n, rows], at_xy(x, yy), 6 - d)
            send(p.da, r.mc.at[rem(xx, 2), rows], r.mid.at[n, rows], at_xy(xx, y), 3 - d)
            send(p.db, r.mc.at[1 - par, rows, right_cols], r.xb.at[y, rows], at_xy(x, yy), 3 - d)

    left_cols, right_cols = pl.ds(0, 128), pl.ds(128, 128)
    tile_on(z)
    pass_weights(1)
    r.accg[...] = jnp.zeros((128, 256), F32)
    r.accu[...] = jnp.zeros((128, 256), F32)
    r.ssq[...] = jnp.zeros((128, 128), F32)
    for a in (FFD, 128 + FFD):
        r.wg[:, a : a + 16, :] = jnp.zeros((2, 16, D), BF)
        r.wd[a : a + 16, :] = jnp.zeros((16, D), BF)
    done(p.fi, r.fi)
    done(p.fh, r.fh)
    done(p.fo, r.fo)
    done(p.fy, r.fhy)
    r.fhp[...] = jnp.zeros((3, 2, 256), F32)
    r.fhp[:, :, 0:FFD] = r.fh[...]
    lane_h = lax.broadcasted_iota(jnp.int32, (3, 2, FFD), 2)
    r.fhp[:, :, 128 : 128 + FFD] = jnp.where(lane_h < 64, r.fhy[0], r.fhy[1])
    mine_g = r.wg.at[:, 128 : 128 + FFD, 0:HALF]
    mine_d = r.wd.at[128 : 128 + FFD, 0:HALF]
    for k in (p.xg, p.fg):
        sent(k, mine_g)
    for k in (p.xd, p.fd):
        sent(k, mine_d)
    for k in (local.wg, local.wd):
        k.wait()
    for d in (1, 7, 2, 6, 3, 5, 4):
        recv(p.s8, r.mc.at[:, 0:16], d - 1)
        tile_on(rem(z + d, NZ))
    sent(p.s8, r.mc.at[:, 0:112])

    near = (1, 3, 2)
    sent(p.da, r.mid.at[0:6])
    sent(p.db, r.xb.at[0:3])
    r.mid[n] = r.mc[par]
    for g in range(2):
        cols = pl.ds(pl.multiple_of((1 - c) * HALF + g * 1024, 1024), 1024)
        recv(p.fg, r.wg.at[:, 128 : 128 + FFD, cols], g)
        recv(p.fd, r.wd.at[128 : 128 + FFD, cols], g)

    def ffn_chunk(m):
        v = r.mid[m].astype(F32)
        r.ssq[...] += v[:, :128] * v[:, :128] + v[:, 128:] * v[:, 128:]
        cols = pl.ds(pl.multiple_of(m * 256, 256), 256)
        g = r.gn[1:2, cols]
        v4 = v.reshape(8, 2, 8, 256)
        for k, total in enumerate((r.accg, r.accu)):
            f = jnp.concatenate(
                [
                    (r.fi[i, k : k + 1, cols] * g).reshape(1, 1, 1, 256)
                    for i in range(2)
                ],
                axis=1,
            )
            act = (v4 * f).reshape(128, 256).astype(BF)
            total[...] += lax.dot_general(
                act, r.wg[k, :, cols], NT, preferred_element_type=F32
            )

    ffn_chunk(n)
    for d in near:
        m = rem(x + d, NX) * 4 + y
        recv(p.da, r.mid.at[m], d - 1)
        for e in (2, 1, 3):
            yy = rem(y + e, NY)
            at = r.mid.at[m, :, left_cols]
            send(p.dg, at, at, at_xy(x, yy), (d - 1) * 3 + 3 - e)
        yy = rem(y + d, NY)
        m = x * 4 + yy
        recv(p.da, r.mid.at[m], d + 2)
        recv(p.db, r.xb.at[yy], d - 1)
        for e in (2, 1, 3):
            xx = rem(x + e, NX)
            to = r.mid.at[m, :, right_cols]
            at = to if e == 2 else r.xb.at[yy]
            send(p.dg, at, to, at_xy(xx, y), (3 - e) * 3 + d - 1)
    sent(p.dg, r.mid.at[0:9])

    def line_step(i, carry):
        ffn_chunk(rem(x + 1 + i, NX) * 4 + y)
        ffn_chunk(x * 4 + rem(y + 1 + i, NY))
        return carry

    lax.fori_loop(0, 3, line_step, 0)

    def diag_step(i, carry):
        m = rem(x + 1 + i // 3, NX) * 4 + rem(y + 1 + i % 3, NY)
        recv(p.dg, r.mid.at[m], i)
        ffn_chunk(m)
        return carry

    lax.fori_loop(0, 9, diag_step, 0)
    scale = lax.rsqrt(jnp.sum(r.ssq[...], axis=1, keepdims=True) * (1.0 / D) + 1e-5)

    def by_member(k):
        return jnp.concatenate(
            [r.fhp[k, i : i + 1, :].reshape(1, 1, 1, 256) for i in range(2)], axis=1
        )

    gate = (r.accg[...] * scale).reshape(8, 2, 8, 256) * by_member(0)
    up = (r.accu[...] * scale).reshape(8, 2, 8, 256) * by_member(1)
    hidden = gate / (1.0 + jnp.exp(-gate)) * up * by_member(2)
    r.hid[...] = hidden.reshape(128, 256).astype(BF)

    def chunk(ch):
        return pl.ds(pl.multiple_of(ch * CA, CA), CA)

    def chunk_b(ch):
        return pl.ds(pl.multiple_of(ch * CB, CB), CB)

    def high(ch):
        return pl.ds(pl.multiple_of(WA + ch * CB, 128), CB)

    other = 1 - xl
    opposite = at_xy(rem(x + 2, NX), y)

    def a1(ch):
        send(p.a1, r.p3.at[other, :, :, chunk(ch)], r.r1a.at[:, :, chunk(ch)], opposite, ch)

    def b1(ch, yy):
        at = r.p3.at[:, yy, :, high(ch)]
        send(p.b1, at, r.r1b.at[y, :, :, chunk_b(ch)], at_xy(x, yy), ch)

    def down_step(ch, carry):
        for cols, width in ((chunk(ch), CA), (high(ch), CB)):
            v = jnp.dot(r.hid[...], r.wd[:, cols], preferred_element_type=F32)
            r.p3[:, :, :, cols] = v.astype(BF).reshape(2, NY, 16, width)
        a1(ch)
        for d in (2, 1, 3):
            b1(ch, rem(y + d, NY))
        return carry

    lax.fori_loop(0, NCH, down_step, 0)

    def a2(ch, yy):
        send(p.a2, r.s2a.at[yy, :, chunk(ch)], r.r2a.at[y, :, chunk(ch)], at_xy(x, yy), ch)

    def b2(ch):
        send(p.b2, r.s2b.at[other, :, chunk_b(ch)], r.r2b.at[:, chunk_b(ch)], opposite, ch)

    def second_step(ch, carry):
        recv(p.a1, r.r1a.at[:, :, chunk(ch)], ch)
        v = r.p3[xl, :, :, chunk(ch)].astype(F32) + r.r1a[:, :, chunk(ch)].astype(F32)
        r.s2a[:, :, chunk(ch)] = v.astype(BF)
        for d in (2, 1, 3):
            a2(ch, rem(y + d, NY))
        recv(p.b1, r.r1b.at[0:3, :, :, chunk_b(ch)], ch)
        v = r.p3[:, y, :, high(ch)].astype(F32)
        for d in near:
            v = v + r.r1b[rem(y + d, NY), :, :, chunk_b(ch)].astype(F32)
        r.s2b[:, :, chunk_b(ch)] = v.astype(BF)
        b2(ch)
        return carry

    lax.fori_loop(0, NCH, second_step, 0)
    sent(p.a1, r.r1a)
    sent(p.b1, r.r1b.at[0:3])
    sent(p.a2, r.r2a.at[0:3])
    sent(p.b2, r.r2b)

    row16 = lax.broadcasted_iota(jnp.int32, (16, 128), 0)
    own_row = rem(row16, 8) == z
    tile16 = pl.ds(pl.multiple_of((xl * 4 + y) * 16, 16), 16)

    def parts(ch):
        return (ch * BA, BA), (NCH * BA + ch * BB, BB)

    def last_step(ch):
        recv(p.a2, r.r2a.at[0:3, :, chunk(ch)], ch)
        recv(p.b2, r.r2b.at[:, chunk_b(ch)], ch)
        for b in [b for start, length in parts(ch) for b in range(start, start + length)]:
            if b < NCH * BA:
                cols = slice(b * 128, (b + 1) * 128)
                v = r.s2a[y, :, cols].astype(F32)
                for d in near:
                    v = v + r.r2a[rem(y + d, NY), :, cols].astype(F32)
            else:
                cols = slice((b - NCH * BA) * 128, (b - NCH * BA + 1) * 128)
                v = r.s2b[xl, :, cols].astype(F32) + r.r2b[:, cols].astype(F32)
            at = slice(b * 128, (b + 1) * 128)
            v = v * jnp.where(row16 < 8, r.fo[0:1, at], r.fo[1:2, at])
            m = r.mid[b // 2, tile16, (b % 2) * 128 : (b % 2 + 1) * 128].astype(F32)
            r.f3[b * 16 : (b + 1) * 16, :] = v + jnp.where(own_row, m, 0.0)
        for zz in range(NZ):
            r.s13s[zz, ch] = chunk_rows(zz, ch).astype(BF)
        for zz in zpeers:
            send(p.s13, r.s13s.at[zz, ch], r.s13r.at[z, ch], at_z(zz), ch)

    def chunk_rows(zz, ch):
        return jnp.concatenate(
            [
                r.f3[pl.ds(start * 16 + m * 8 + zz, length, stride=16), :]
                for m in range(2)
                for start, length in parts(ch)
            ],
            axis=0,
        )

    for ch in range(NCH):
        last_step(ch)
    for ch in range(NCH):
        v = chunk_rows(z, ch)
        recv(p.s13, r.s13r.at[0:7, ch], ch)
        for zz in zpeers:
            v = v + r.s13r[zz, ch].astype(F32)
        for m in range(2):
            row = m * 8
            for start, length in parts(ch):
                at = m * 32 + start
                r.vs[at : at + length, :] = v[row : row + length]
                row += length
    sent(p.s13, r.s13r.at[0:7])
    both = jnp.zeros((32, 128), F32)
    for m in range(2):
        v = r.vs[m * 32 : m * 32 + 32, :]
        v = v.astype(BF).astype(F32)
        mean = jnp.sum(jnp.sum(v * v, axis=1, keepdims=True), axis=0, keepdims=True) * (1.0 / D)
        both = both + (v * lax.rsqrt(mean + 1e-5) * r.g3[...]).astype(BF).astype(F32)
    r.fs[...] = both

    def half(k):
        return pl.ds(pl.multiple_of(k * 16, 16), 16)

    send(p.fx, r.fs.at[half(1 - c)], r.fr, partner)
    done(p.fx, r.fr)
    r.fb[own, z] = ((r.fs[half(c), :] + r.fr[...]) * 0.25).astype(BF)
    for d in ZORDER:
        send(p.s14, r.fb.at[own, z], r.fb.at[own, z], at_z(rem(z + d, NZ)), 7 - d)
    xy_send(p.s15, lambda m: r.fb.at[own, z], r.fb.at[own, z])
    local.lm.wait()
    local.tg.wait()
    wanted = jnp.broadcast_to(r.tg[...].astype(F32), (B, B)).T[:, 0:1]
    for d in (1, 7, 2, 6, 3, 5, 4):
        zz = rem(z + d, NZ)
        recv(p.s14, r.fb.at[own, zz], d - 1)
        xy_send(p.s15, lambda m: r.fb.at[own, zz], r.fb.at[own, zz])
    sent(p.s14, r.fb.at[own, 0:7])
    done(p.s15, r.fb.at[0:15])
    r.ff[...] = r.fb[...].reshape(2048, 128).astype(F32)
    for b in range(16):
        rows = [
            r.ff[pl.ds(h * 1024 + zz * 16 + b, 8, stride=128), :]
            for h in range(2)
            for zz in range(NZ)
        ]
        r.lh[:, b * 128 : (b + 1) * 128] = jnp.concatenate(rows, axis=0).astype(BF)
    for h in range(2):
        at = slice(h * 256, (h + 1) * 256)
        r.lp[:, at] = jnp.dot(r.lh[...], r.lm[:, at], preferred_element_type=F32)
        send(p.lx, r.lp.at[:, at], r.lr.at[:, at], partner, h)
    for h in range(2):
        recv(p.lx, r.lr.at[:, h * 256 : (h + 1) * 256], h)
    sent(p.lx, r.lr)
    mean_f = r.lp[...] + r.lr[...]
    r.logits_o[...] = mean_f.astype(BF)

    ids = (lax.broadcasted_iota(jnp.int32, (B, VD), 1) + t * VD).astype(F32)
    found = jnp.sum(jnp.where(ids == wanted, mean_f, 0.0), axis=1, keepdims=True)
    peak = jnp.max(mean_f, axis=1, keepdims=True)
    total = jnp.sum(jnp.exp(mean_f - peak), axis=1, keepdims=True)
    lane = lax.broadcasted_iota(jnp.int32, (B, B), 1)
    stat = jnp.where(lane == 0, peak, jnp.where(lane == 1, total, jnp.where(lane == 2, found, 0.0)))
    r.sz[z] = stat.T[:8]

    def combine(ref, count):
        peaks = [ref[k, 0:1, :] for k in range(count)]
        top_ = peaks[0]
        for k in range(1, count):
            top_ = jnp.maximum(top_, peaks[k])
        tot = ref[0, 1:2, :] * jnp.exp(peaks[0] - top_)
        hit = ref[0, 2:3, :]
        for k in range(1, count):
            tot = tot + ref[k, 1:2, :] * jnp.exp(peaks[k] - top_)
            hit = hit + ref[k, 2:3, :]
        return top_, tot, hit

    z_send(p.s16, lambda zz: r.sz.at[z], r.sz.at[z])
    done(p.s16, r.sz.at[0:7])
    a, b_, h = combine(r.sz, NZ)
    r.sx[n] = jnp.concatenate([a, b_, h, jnp.zeros((5, 128), F32)], axis=0)
    xy_send(p.s17, lambda m: r.sx.at[n], r.sx.at[n])
    done(p.s17, r.sx.at[0:15])
    a, b_, h = combine(r.sx, NP)
    r.lp_o[...] = h - (a + jnp.log(b_))

    for sem, ref in drains:
        wait_bytes(sem, ref)


def hand_on(logits, logprob, logits_o, logprob_o):
    logits_o[...] = logits[...]
    logprob_o[...] = logprob[...]


def body(
    stream_in, kv_cache, lengths, targets, norm_gains, w_qkv, w_out, w_gate_up, w_down, lm_head,
    fast_in, fast_hidden, fast_out,
):
    freq = np.float32(500000.0) ** (-np.arange(64, dtype=np.float32) * 2.0 / 128)
    freq = jnp.asarray(np.concatenate([freq, freq])[None, :], F32)
    args = dict(
        stream=stream_in, kv=kv_cache, lengths=lengths, targets=targets.reshape(1, B),
        gains=norm_gains, wqkv=w_qkv.T, wout=w_out,
        wgu=w_gate_up.swapaxes(1, 2), wdown=w_down, lmh=lm_head,
        fin=fast_in, fhid=fast_hidden.swapaxes(0, 1), fout=fast_out, freq=freq,
    )
    got = pl.pallas_call(
        functools.partial(kernel, list(args)),
        out_shape=[VM(k.shape, k.dtype) for k in OUTS.values()],
        in_specs=[
            pl.BlockSpec(memory_space=pltpu.SMEM if v is lengths else pl.ANY)
            for v in args.values()
        ],
        out_specs=[pl.BlockSpec(memory_space=VM)] * len(OUTS),
        scratch_shapes=[
            *SCRATCH.values(),
            *LS.values(),
            *(DMA((count,)) for n in PHASES.values() for count in (1, n)),
        ],
        compiler_params=pltpu.CompilerParams(
            collective_id=0, has_side_effects=True, vmem_limit_bytes=60 * 1024 * 1024
        ),
        name="step",
    )(*args.values())
    got = [pltpu.with_memory_space_constraint(k, VM) for k in got]
    got = pl.pallas_call(
        hand_on,
        out_shape=list(OUTS.values()),
        in_specs=[pl.BlockSpec(memory_space=VM)] * 2,
        name="result",
    )(*got)
    return (got[0], got[1].reshape(B))


MEMBER_TP = ("member", "tp_0", "tp_1", "tp_2")
TP = ("tp_0", "tp_1", "tp_2")
IN_SPECS = (
    P(MEMBER_TP, None), P(MEMBER_TP, None, None), P(), P(), P(), P(None, TP), P(TP, None),
    P(None, None, TP), P(TP, None), P(None, TP), P("member", None, None), P("member", None, TP),
    P("member", None),
)


def solution(mesh):
    split = Mesh(
        mesh.devices.reshape(mesh.shape["member"], NX, NZ, NY), MEMBER_TP
    )
    return jax.shard_map(
        body, mesh=split, in_specs=IN_SPECS, out_specs=(P(None, TP), P()), check_vma=False
    )
```

```python
import functools
from types import SimpleNamespace

import jax
import jax.numpy as jnp
import numpy as np
from jax import lax
from jax.experimental import pallas as pl
from jax.experimental.pallas import tpu as pltpu
from jax.sharding import Mesh
from jax.sharding import PartitionSpec as P

MESH = pl.DeviceIdType.MESH
F32 = jnp.float32
BF = jnp.bfloat16
NX, NZ, NY = 4, 8, 4
NP = NX * NY
D, HEADS, KV, HD, CACHE, FFD, VD = 4096, 32, 8, 128, 512, 112, 512
B = 128
QN = 384
ZORDER = (4, 3, 5, 2, 6, 1, 7)
NEAR_Z = (7, 0, 1)
NCH, CA, CB = 4, 512, 512
WA, WB = NCH * CA, NCH * CB
BA, BB = CA // 128, CB // 128
HALF = D // 2
NT = (((1,), (1,)), ((), ()))

VM = pltpu.VMEM
DMA = pltpu.SemaphoreType.DMA

SCRATCH = dict(
    st=VM((2, D), BF),
    kvv=VM((2, CACHE, 2 * KV * HD), BF),
    tg=VM((1, B), jnp.int32),
    gn=VM((3, D), F32),
    fi=VM((2, 2, D), F32),
    fh=VM((3, 2, FFD), F32),
    fo=VM((2, D), F32),
    fq=VM((1, 128), F32),
    wq=VM((NZ, 48, 512), BF),
    wo=VM((NP, 32, 256), BF),
    wg=VM((2, 256, D), BF),
    wd=VM((256, D), BF),
    fhx=VM((2, 3, 2, FFD), F32),
    fhy=VM((2, 3, 2, FFD), F32),
    fhp=VM((3, 2, 256), F32),
    lm=VM((HALF, VD), BF),
    sc=VM((64, 128), F32),
    s1s=VM((64, 128), F32),
    s1r=VM((64, 128), F32),
    raw=VM((NP, 16, 512), BF),
    p1=VM((3, 256, 128), F32),
    s3s=VM((NZ, 32, QN), BF),
    s3r=VM((NZ, 32, QN), BF),
    q1=VM((3, 32, 128), F32),
    s4s=VM((128, 128), F32),
    s4r=VM((128, 128), F32),
    hs=VM((96, 128), F32),
    osc=VM((64, 128), F32),
    s5s=VM((64, 128), F32),
    s5r=VM((64, 128), F32),
    att=VM((NP, 16, 512), BF),
    s7s=VM((NZ, 32, 256), BF),
    s7r=VM((NZ, 32, 256), BF),
    mc=VM((2, 128, 256), BF),
    xb=VM((NY, 128, 128), BF),
    mid=VM((NP, 128, 256), BF),
    accg=VM((128, 256), F32),
    accu=VM((128, 256), F32),
    ssq=VM((128, 128), F32),
    hid=VM((128, 256), BF),
    p3=VM((8, 16, D), BF),
    r1a=VM((NY, 16, WA), BF),
    r1b=VM((NY, 2, 16, WB), BF),
    s2a=VM((NY, 16, WA), BF),
    s2b=VM((2, 16, WB), BF),
    r2a=VM((NY, 16, WA), BF),
    r2b=VM((16, WB), BF),
    f3=VM((512, 128), F32),
    g3=VM((32, 128), F32),
    s13s=VM((NZ, NCH, 16, 128), BF),
    s13r=VM((NZ, NCH, 16, 128), BF),
    vs=VM((64, 128), F32),
    fs=VM((32, 128), F32),
    fr=VM((16, 128), F32),
    fb=VM((NP, NZ, 16, 128), BF),
    ff=VM((2048, 128), F32),
    lh=VM((B, HALF), BF),
    lp=VM((B, VD), F32),
    lr=VM((B, VD), F32),
    sz=VM((NZ, 8, 128), F32),
    sx=VM((NP, 8, 128), F32),
)
PHASES = dict(
    wq=1, wqf=1, wo=1, s1=1, s2=1, s3=1, s4=1, s5=1, s6=1, s7=1, s8=7, da=12, db=6, dg=9,
    xg=2, xd=2, fg=2, fd=2, xh=2, fi=1, fh=1, fo=1, fy=1,
    a1=NCH, b1=NCH, a2=NCH, b2=NCH, s13=NCH, fx=1, s14=7, s15=8, lx=1, s16=1, s17=1,
)
LS = dict(ls=DMA((16,)))
OUTS = dict(
    logits_o=jax.ShapeDtypeStruct((B, VD), BF), lp_o=jax.ShapeDtypeStruct((1, B), F32)
)


def kernel(inputs, *refs):
    names = [*inputs, *OUTS, *SCRATCH, *LS]
    r = SimpleNamespace(**dict(zip(names, refs)))
    sems = iter(refs[len(names) :])
    p = SimpleNamespace(**{k: (next(sems), next(sems)) for k in PHASES})
    c, x, z, y = (lax.axis_index(a) for a in MEMBER_TP)
    t = x * 32 + z * 4 + y
    n = x * 4 + y
    xl, par = x // 2, lax.rem(x, 2)
    own = xl * 8 + y * 2 + par
    drains = []
    def rem(v, k):
        return lax.rem(v, k)

    def at_z(zz):
        return (c, x, zz, y)

    def at_xy(xx, yy):
        return (c, xx, z, yy)

    partner = (1 - c, x, z, y)

    def across_z(zz):
        return (1 - c, x, zz, y)

    def copy(phase, src, dst, dev, slot=0):
        return pltpu.make_async_remote_copy(
            src_ref=src,
            dst_ref=dst,
            send_sem=phase[0].at[0],
            recv_sem=phase[1].at[slot],
            device_id=dev,
            device_id_type=MESH,
        )

    def send(phase, src, dst, dev, slot=0):
        copy(phase, src, dst, dev, slot).start()

    def wait_bytes(sem, ref):
        pltpu.make_async_copy(ref, ref, sem).wait()

    def recv(phase, ref, slot=0):
        wait_bytes(phase[1].at[slot], ref)

    def sent(phase, ref):
        drains.append((phase[0].at[0], ref))

    zpeers = [rem(z + d, NZ) for d in ZORDER]
    plane = [
        (rem(x + dx, NX), rem(y + dy, NY))
        for dx, dy in sorted(
            ((a, b) for a in range(NX) for b in range(NY) if a or b),
            key=lambda p: -(min(p[0], 4 - p[0]) + min(p[1], 4 - p[1])),
        )
    ]

    def z_send(phase, src_at, dst):
        for zz in zpeers:
            send(phase, src_at(zz), dst, at_z(zz))

    def xy_send(phase, src_at, dst, slot=0):
        for xx, yy in plane:
            send(phase, src_at(xx * 4 + yy), dst, at_xy(xx, yy), slot)

    def done(phase, ref):
        recv(phase, ref)
        sent(phase, ref)

    bar = pltpu.get_barrier_semaphore()
    peers = [at_z(zz) for zz in zpeers] + [at_xy(*k) for k in plane] + [partner]
    peers += [across_z(zz) for zz in zpeers]
    for dev in peers:
        pl.semaphore_signal(bar, inc=1, device_id=dev, device_id_type=MESH)

    def qcols(zz, k):
        return r.wqkv.at[:, pl.ds(pl.multiple_of(k * 1024 + zz * 128, 128), 128)]

    def half_cols(k):
        return pl.ds(pl.multiple_of((2 * c + k) * 128, 128), 128)

    local = SimpleNamespace()
    begun = []

    def fetch(src, dst):
        k = pltpu.make_async_copy(src, dst, r.ls.at[len(begun)])
        k.start()
        begun.append(k)
        return k

    local.st = fetch(r.stream, r.st)
    local.gn = fetch(r.gains, r.gn)
    local.fq = fetch(r.freq, r.fq)
    local_wq = [fetch(qcols(z, 2 * c + k), r.wq.at[z, :, half_cols(k)]) for k in range(2)]
    local.wo = fetch(r.wout.at[:, pl.ds(pl.multiple_of(n * 256, 256), 256)], r.wo.at[n])
    local.kvv = fetch(r.kv, r.kvv)
    local.tg = fetch(r.targets, r.tg)
    local.wg = fetch(r.wgu, r.wg.at[:, 0:FFD])
    local.wd = fetch(r.wdown, r.wd.at[0:FFD])
    local.lm = fetch(r.lmh.at[pl.ds(pl.multiple_of(c * HALF, HALF), HALF)], r.lm)

    right, left = at_xy(rem(x + 1, NX), y), at_xy(rem(x + 3, NX), y)

    def weight_piece(i):
        cols = pl.ds(pl.multiple_of(c * HALF + i * 256, 256), 256)
        for dev, a, b in ((right, 0, 64), (left, 64, FFD)):
            g = r.wg.at[:, 128 + a : 128 + b, cols]
            send(p.xg, r.wgu.at[:, a:b, cols], g, dev, i // 4)
            send(p.xd, r.wdown.at[a:b, cols], r.wd.at[128 + a : 128 + b, cols], dev, i // 4)

    def pass_weights(g):
        cols = pl.ds(pl.multiple_of(c * HALF + g * 1024, 1024), 1024)
        for came, went, at in (
            (p.xg, p.fg, r.wg.at[:, 128 : 128 + FFD, cols]),
            (p.xd, p.fd, r.wd.at[128 : 128 + FFD, cols]),
        ):
            recv(came, at, g)
            send(went, at, at, partner, g)

    def spread(scratch, dst):
        for zz in range(NZ):
            dst[zz * 8 : zz * 8 + 8] = scratch[pl.ds(zz, 8, stride=8), :]

    z8 = pl.ds(pl.multiple_of(z * 8, 8), 8)

    def z_then_plane(zphase, pphase, s, rr, buf, start=True, beside=lambda: None):
        def piece(zz):
            return pl.ds(pl.multiple_of(zz * 8, 8), 8)

        if start:
            z_send(zphase, lambda zz: s.at[piece(zz)], rr.at[z8])
        beside()
        rr[z8, :] = s[z8, :]
        done(zphase, rr.at[0:56])
        for k in range(4):
            rows = [rr[pl.ds(j * 4 + k, 8, stride=8), :] for j in range(2)]
            buf[n, :, k * 128 : (k + 1) * 128] = jnp.concatenate(rows, axis=0).astype(BF)
        xy_send(pphase, lambda m: buf.at[n], buf.at[n])
        return lambda: done(pphase, buf.at[0:15])

    local.st.wait()
    x32 = r.st[...].astype(F32)
    rs = lax.rsqrt(jnp.mean(x32 * x32, axis=-1, keepdims=True) + 1e-5)
    for b in range(32):
        for j in range(2):
            r.sc[j * 32 + b : j * 32 + b + 1, :] = x32[j : j + 1, b * 128 : (b + 1) * 128]
    spread(r.sc, r.s1s)
    r.s4s[...] = jnp.zeros((128, 128), F32)
    row8 = lax.broadcasted_iota(jnp.int32, (8, 128), 0)
    lane8 = lax.broadcasted_iota(jnp.int32, (8, 128), 1)
    rs8 = jnp.where(row8 < 4, rs[0:1, 0:1], rs[1:2, 0:1])

    pl.semaphore_wait(bar, len(peers))

    for zz in zpeers:
        send(p.s1, r.s1s.at[pl.ds(pl.multiple_of(zz * 8, 8), 8)], r.s1r.at[z8], at_z(zz))
    for zz in zpeers:
        for k in range(2):
            send(p.wq, qcols(zz, 2 * c + k), r.wq.at[z, :, half_cols(k)], at_z(zz))
    weight_piece(0)
    weight_piece(1)
    send(p.fi, r.fin, r.fi, partner)
    send(p.fh, r.fhid, r.fh, partner)
    send(p.fo, r.fout, r.fo, partner)
    send(p.xh, r.fhid, r.fhx.at[0], right, 0)
    send(p.xh, r.fhid, r.fhx.at[1], left, 1)
    finish = z_then_plane(p.s1, p.s2, r.s1s, r.s1r, r.raw, False)
    local.fq.wait()
    local.gn.wait()
    pos = [r.lengths[rem(2 * t + j, B)] for j in range(2)]
    ang = jnp.where(row8 < 4, pos[0], pos[1]).astype(F32) * r.fq[0:1, :]
    cos8 = jnp.cos(ang)
    sin8 = jnp.where(lane8 < 64, -jnp.sin(ang), jnp.sin(ang))
    for b in range(32):
        r.g3[b : b + 1, :] = r.gn[2:3, b * 128 : (b + 1) * 128]

    for k in range(2):
        local_wq[k].wait()
    done(p.wq, r.wq.at[0:7, :, 0:256])
    mine = r.wq.at[:, :, pl.ds(pl.multiple_of(c * 256, 256), 256)]
    send(p.wqf, mine, mine, partner)
    done(p.wqf, mine)
    gq = jnp.concatenate(
        [r.gn[0:1, pl.ds(pl.multiple_of(k * 1024 + z * 128, 128), 128)] for k in range(4)], axis=1
    )
    finish()
    lhs = (r.raw[...].reshape(256, 512).astype(F32) * gq).astype(BF)
    prod = lax.dot_general(lhs, r.wq[...].reshape(QN, 512), NT, preferred_element_type=F32)
    for l in range(3):
        r.p1[l] = prod[:, l * 128 : (l + 1) * 128]
    for zz in range(NZ):
        for l in range(3):
            r.s3s[zz, :, l * 128 : (l + 1) * 128] = r.p1.at[l][
                pl.ds(zz, 32, stride=8), :
            ].astype(BF)
    z_send(p.s3, lambda zz: r.s3s.at[zz], r.s3r.at[z])
    weight_piece(2)
    weight_piece(3)
    r.s3r[z] = r.s3s[z]
    done(p.s3, r.s3r.at[0:7])
    acc = r.s3r[0].astype(F32)
    for s in range(1, NZ):
        acc = acc + r.s3r[s].astype(F32)
    for l in range(3):
        r.q1[l] = acc[:, l * 128 : (l + 1) * 128]
    for l in range(3):
        for j in range(2):
            r.s4s[pl.ds(l * 2 + j, 16, stride=8), :] = r.q1.at[l][pl.ds(j, 16, stride=2), :]

    def tile(m):
        return pl.ds(pl.multiple_of(m * 8, 8), 8)

    xy_send(p.s4, lambda m: r.s4s.at[tile(m)], r.s4r.at[tile(n)])
    xy_send(
        p.wo,
        lambda m: r.wout.at[:, pl.ds(pl.multiple_of(m * 256, 256), 256)],
        r.wo.at[n],
    )
    r.s4r[tile(n), :] = r.s4s[tile(n), :]
    done(p.s4, r.s4r.at[0:120])

    blocks = {
        (yy, l): jnp.concatenate(
            [r.s4r[pl.ds(yy * 8 + l * 2 + j, 4, stride=32), :] for j in range(2)], axis=0
        )
        for yy in range(NY)
        for l in range(3)
    }
    for hh in range(12):
        val = jnp.zeros((8, 128), F32)
        lane = 0
        while lane < 128:
            col = hh * 128 + lane
            tt, i = divmod(col, 48)
            at = (tt // 4) * 48 + i
            l, src = divmod(at, 128)
            width = min(48 - i, 128 - src, 128 - lane)
            piece = blocks[(tt % 4, l)]
            shift = (lane - src) % 128
            if shift:
                piece = pltpu.roll(piece, shift, 1)
            val = jnp.where((lane8 >= lane) & (lane8 < lane + width), piece, val)
            lane += width
        val = (val * rs8).astype(BF).astype(F32)
        turned = (val * cos8 + pltpu.roll(val, 64, 1) * sin8).astype(BF).astype(F32)
        if hh >= 4:
            turned = jnp.where(row8 % 4 == 3, val, turned)
        r.hs[pl.ds(hh, 8, stride=12), :] = turned

    local.kvv.wait()
    inv_root = HD**-0.5
    group = lax.broadcasted_iota(jnp.int32, (32, 128), 0) // 4
    group8 = (
        lax.broadcasted_iota(jnp.int32, (32, 8), 0) // 4
        == lax.broadcasted_iota(jnp.int32, (32, 8), 1)
    )
    place = lax.broadcasted_iota(jnp.int32, (32, CACHE), 1)
    for j in range(2):
        q = r.hs[j * 48 : j * 48 + 32, :]
        kn = r.hs[j * 48 + 32 : j * 48 + 40, :].astype(BF)
        vn = r.hs[j * 48 + 40 : j * 48 + 48, :].astype(BF)
        qd = jnp.concatenate([jnp.where(group == k, q, 0.0) for k in range(KV)], axis=1).astype(BF)
        scores = (
            lax.dot_general(qd, r.kvv[j, :, : KV * HD], NT, preferred_element_type=F32) * inv_root
        )
        fresh = lax.dot_general(q.astype(BF), kn, NT, preferred_element_type=F32)
        fresh = jnp.sum(jnp.where(group8, fresh, 0.0), axis=1, keepdims=True) * inv_root
        scores = jnp.where(place < pos[j], scores, -1e30)
        peak = jnp.maximum(jnp.max(scores, axis=1, keepdims=True), fresh)
        weights = jnp.exp(scores - peak)
        fresh_w = jnp.exp(fresh - peak)
        total = jnp.sum(weights, axis=1, keepdims=True) + fresh_w
        probs = (weights / total).astype(BF)
        fresh_p = jnp.where(group8, fresh_w / total, 0.0).astype(BF)
        wide = jnp.dot(probs, r.kvv[j, :, KV * HD :], preferred_element_type=F32)
        out = jnp.dot(fresh_p, vn, preferred_element_type=F32)
        for k in range(KV):
            out = out + jnp.where(group == k, wide[:, k * 128 : (k + 1) * 128], 0.0)
        r.osc[j * 32 : j * 32 + 32, :] = out.astype(BF).astype(F32)

    spread(r.osc, r.s5s)

    def beside():
        weight_piece(4)
        weight_piece(5)

    finish = z_then_plane(p.s5, p.s6, r.s5s, r.s5r, r.att, beside=beside)
    pass_weights(0)
    local.wo.wait()
    done(p.wo, r.wo.at[0:15])
    resid = r.raw[:, :, pl.ds(pl.multiple_of(x * 128, 128), 128)].reshape(256, 128).astype(F32)
    lo = resid * jnp.where(z == 2 * y, 1.0, 0.0)
    hi = resid * jnp.where(z == 2 * y + 1, 1.0, 0.0)
    finish()
    prod = jnp.dot(
        r.att[...].reshape(256, 512), r.wo[...].reshape(512, 256), preferred_element_type=F32
    ) + jnp.concatenate([lo, hi], axis=1)
    for h in range(2):
        for ys in range(NY):
            for j in range(2):
                at = [((m * 2 + h) * 4 + ys) * 16 + j * 8 for m in range(2)]
                r.s7s[h * 4 + ys, j * 16 : j * 16 + 16, :] = jnp.concatenate(
                    [prod[a : a + 8] for a in at], axis=0
                ).astype(BF)
    for zz in zpeers:
        send(p.s7, r.s7s.at[zz], r.s7r.at[z], across_z(zz))
    send(p.s7, r.s7s.at[z], r.s7r.at[z], partner)
    weight_piece(6)
    weight_piece(7)
    recv(p.xh, r.fhx.at[0], 0)
    recv(p.xh, r.fhx.at[1], 1)
    sent(p.xh, r.fhx)
    send(p.fy, r.fhx, r.fhy, partner)
    done(p.s7, r.s7r)
    acc = r.s7r[0].astype(F32)
    for s in range(1, NZ):
        acc = acc + r.s7r[s].astype(F32)

    def tile_rows(d):
        return pl.ds((d + 1) % NZ * 16, 16)

    for j in range(2):
        r.mc[j, tile_rows(0), :] = acc[j * 16 : j * 16 + 16].astype(BF)
    for d in ZORDER:
        at = r.mc.at[:, tile_rows(0)]
        send(p.s8, at, r.mc.at[:, tile_rows(-d)], at_z(rem(z + d, NZ)), 7 - d)

    def tile_on(k):
        rows = tile_rows(k)
        late = 0 if k in NEAR_Z else 1
        for d in (2, 1, 3):
            xx, yy = rem(x + d, NX), rem(y + d, NY)
            at = r.mid.at[n, rows]
            send(p.da, r.mc.at[par, rows], at, at_xy(x, yy), 6 - d + 6 * late)
            send(p.da, r.mc.at[rem(xx, 2), rows], at, at_xy(xx, y), 3 - d + 6 * late)
            at = r.mc.at[1 - par, rows, right_cols]
            send(p.db, at, r.xb.at[y, rows], at_xy(x, yy), 3 - d + 3 * late)

    left_cols, right_cols = pl.ds(0, 128), pl.ds(128, 128)
    tile_on(0)
    pass_weights(1)
    r.accg[...] = jnp.zeros((128, 256), F32)
    r.accu[...] = jnp.zeros((128, 256), F32)
    r.ssq[...] = jnp.zeros((128, 128), F32)
    for a in (FFD, 128 + FFD):
        r.wg[:, a : a + 16, :] = jnp.zeros((2, 16, D), BF)
        r.wd[a : a + 16, :] = jnp.zeros((16, D), BF)
    done(p.fi, r.fi)
    done(p.fh, r.fh)
    done(p.fo, r.fo)
    done(p.fy, r.fhy)
    r.fhp[...] = jnp.zeros((3, 2, 256), F32)
    r.fhp[:, :, 0:FFD] = r.fh[...]
    lane_h = lax.broadcasted_iota(jnp.int32, (3, 2, FFD), 2)
    r.fhp[:, :, 128 : 128 + FFD] = jnp.where(lane_h < 64, r.fhy[0], r.fhy[1])
    mine_g = r.wg.at[:, 128 : 128 + FFD, 0:HALF]
    mine_d = r.wd.at[128 : 128 + FFD, 0:HALF]
    for k in (p.xg, p.fg):
        sent(k, mine_g)
    for k in (p.xd, p.fd):
        sent(k, mine_d)
    for k in (local.wg, local.wd):
        k.wait()
    for d in (1, 7, 2, 6, 3, 5, 4):
        recv(p.s8, r.mc.at[:, 0:16], d - 1)
        tile_on(d)
    sent(p.s8, r.mc.at[:, 0:112])

    near = (1, 3, 2)
    sent(p.da, r.mid.at[0:6])
    sent(p.db, r.xb.at[0:3])
    r.mid[n] = r.mc[par]
    for g in range(2):
        cols = pl.ds(pl.multiple_of((1 - c) * HALF + g * 1024, 1024), 1024)
        recv(p.fg, r.wg.at[:, 128 : 128 + FFD, cols], g)
        recv(p.fd, r.wd.at[128 : 128 + FFD, cols], g)

    def ffn_chunk(m):
        v = r.mid[m].astype(F32)
        r.ssq[...] += v[:, :128] * v[:, :128] + v[:, 128:] * v[:, 128:]
        cols = pl.ds(pl.multiple_of(m * 256, 256), 256)
        g = r.gn[1:2, cols]
        v4 = v.reshape(8, 2, 8, 256)
        for k, total in enumerate((r.accg, r.accu)):
            f = jnp.concatenate(
                [
                    (r.fi[i, k : k + 1, cols] * g).reshape(1, 1, 1, 256)
                    for i in range(2)
                ],
                axis=1,
            )
            act = (v4 * f).reshape(128, 256).astype(BF)
            total[...] += lax.dot_general(
                act, r.wg[k, :, cols], NT, preferred_element_type=F32
            )

    ffn_chunk(n)
    for late, rows in enumerate((pl.ds(0, 48), pl.ds(48, 80))):
        for d in near:
            m = rem(x + d, NX) * 4 + y
            recv(p.da, r.mid.at[m, rows], d - 1 + 6 * late)
            at = r.mid.at[m, rows, left_cols]
            for e in (2, 1, 3):
                yy = rem(y + e, NY)
                send(p.dg, at, at, at_xy(x, yy), (d - 1) * 3 + 3 - e)
            yy = rem(y + d, NY)
            m = x * 4 + yy
            recv(p.da, r.mid.at[m, rows], d + 2 + 6 * late)
            recv(p.db, r.xb.at[yy, rows], d - 1 + 3 * late)
            to = r.mid.at[m, rows, right_cols]
            for e in (2, 1, 3):
                xx = rem(x + e, NX)
                at = to if e == 2 else r.xb.at[yy, rows]
                send(p.dg, at, to, at_xy(xx, y), (3 - e) * 3 + d - 1)
    sent(p.dg, r.mid.at[0:9])

    def line_step(i, carry):
        ffn_chunk(rem(x + 1 + i, NX) * 4 + y)
        ffn_chunk(x * 4 + rem(y + 1 + i, NY))
        return carry

    lax.fori_loop(0, 3, line_step, 0)

    def diag_step(i, carry):
        m = rem(x + 1 + i // 3, NX) * 4 + rem(y + 1 + i % 3, NY)
        recv(p.dg, r.mid.at[m], i)
        ffn_chunk(m)
        return carry

    lax.fori_loop(0, 9, diag_step, 0)
    scale = lax.rsqrt(jnp.sum(r.ssq[...], axis=1, keepdims=True) * (1.0 / D) + 1e-5)

    def by_member(k):
        return jnp.concatenate(
            [r.fhp[k, i : i + 1, :].reshape(1, 1, 1, 256) for i in range(2)], axis=1
        )

    gate = (r.accg[...] * scale).reshape(8, 2, 8, 256) * by_member(0)
    up = (r.accu[...] * scale).reshape(8, 2, 8, 256) * by_member(1)
    hidden = gate / (1.0 + jnp.exp(-gate)) * up * by_member(2)
    r.hid[...] = hidden.reshape(128, 256).astype(BF)

    def chunk(ch):
        return pl.ds(pl.multiple_of(ch * CA, CA), CA)

    def chunk_b(ch):
        return pl.ds(pl.multiple_of(ch * CB, CB), CB)

    def high(ch):
        return pl.ds(pl.multiple_of(WA + ch * CB, 128), CB)

    other = 1 - xl
    opposite = at_xy(rem(x + 2, NX), y)

    def a1(ch):
        send(p.a1, r.p3.at[pl.ds(other * 4, 4), :, chunk(ch)], r.r1a.at[:, :, chunk(ch)], opposite, ch)

    def b1(ch, yy):
        for h in range(2):
            at = r.p3.at[h * 4 + yy, :, high(ch)]
            send(p.b1, at, r.r1b.at[y, h, :, chunk_b(ch)], at_xy(x, yy), ch)

    def down_step(ch, carry):
        for cols in (chunk(ch), high(ch)):
            v = jnp.dot(r.hid[...], r.wd[:, cols], preferred_element_type=F32)
            for k in range(NZ):
                r.p3[rem(z + k + NZ - 1, NZ), :, cols] = v[k * 16 : k * 16 + 16].astype(BF)
        a1(ch)
        for d in (2, 1, 3):
            b1(ch, rem(y + d, NY))
        return carry

    lax.fori_loop(0, NCH, down_step, 0)

    def a2(ch, yy):
        send(p.a2, r.s2a.at[yy, :, chunk(ch)], r.r2a.at[y, :, chunk(ch)], at_xy(x, yy), ch)

    def b2(ch):
        send(p.b2, r.s2b.at[other, :, chunk_b(ch)], r.r2b.at[:, chunk_b(ch)], opposite, ch)

    def second_step(ch, carry):
        recv(p.a1, r.r1a.at[:, :, chunk(ch)], ch)
        v = r.p3[pl.ds(xl * 4, 4), :, chunk(ch)].astype(F32) + r.r1a[:, :, chunk(ch)].astype(F32)
        r.s2a[:, :, chunk(ch)] = v.astype(BF)
        for d in (2, 1, 3):
            a2(ch, rem(y + d, NY))
        recv(p.b1, r.r1b.at[0:3, :, :, chunk_b(ch)], ch)
        v = jnp.concatenate(
            [r.p3[pl.ds(h * 4 + y, 1), :, high(ch)].astype(F32) for h in range(2)], axis=0
        )
        for d in near:
            v = v + r.r1b[rem(y + d, NY), :, :, chunk_b(ch)].astype(F32)
        r.s2b[:, :, chunk_b(ch)] = v.astype(BF)
        b2(ch)
        return carry

    lax.fori_loop(0, NCH, second_step, 0)
    sent(p.a1, r.r1a)
    sent(p.b1, r.r1b.at[0:3])
    sent(p.a2, r.r2a.at[0:3])
    sent(p.b2, r.r2b)

    row16 = lax.broadcasted_iota(jnp.int32, (16, 128), 0)
    own_row = rem(row16, 8) == z
    tile16 = pl.ds(pl.multiple_of(rem(xl * 4 + y - z + NZ + 1, NZ) * 16, 16), 16)

    def parts(ch):
        return (ch * BA, BA), (NCH * BA + ch * BB, BB)

    def last_step(ch):
        recv(p.a2, r.r2a.at[0:3, :, chunk(ch)], ch)
        recv(p.b2, r.r2b.at[:, chunk_b(ch)], ch)
        for b in [b for start, length in parts(ch) for b in range(start, start + length)]:
            if b < NCH * BA:
                cols = slice(b * 128, (b + 1) * 128)
                v = r.s2a[y, :, cols].astype(F32)
                for d in near:
                    v = v + r.r2a[rem(y + d, NY), :, cols].astype(F32)
            else:
                cols = slice((b - NCH * BA) * 128, (b - NCH * BA + 1) * 128)
                v = r.s2b[xl, :, cols].astype(F32) + r.r2b[:, cols].astype(F32)
            at = slice(b * 128, (b + 1) * 128)
            v = v * jnp.where(row16 < 8, r.fo[0:1, at], r.fo[1:2, at])
            m = r.mid[b // 2, tile16, (b % 2) * 128 : (b % 2 + 1) * 128].astype(F32)
            r.f3[b * 16 : (b + 1) * 16, :] = v + jnp.where(own_row, m, 0.0)
        for zz in range(NZ):
            r.s13s[zz, ch] = chunk_rows(zz, ch).astype(BF)
        for zz in zpeers:
            send(p.s13, r.s13s.at[zz, ch], r.s13r.at[z, ch], at_z(zz), ch)

    def chunk_rows(zz, ch):
        return jnp.concatenate(
            [
                r.f3[pl.ds(start * 16 + m * 8 + zz, length, stride=16), :]
                for m in range(2)
                for start, length in parts(ch)
            ],
            axis=0,
        )

    for ch in range(NCH):
        last_step(ch)
    for ch in range(NCH):
        v = chunk_rows(z, ch)
        recv(p.s13, r.s13r.at[0:7, ch], ch)
        for zz in zpeers:
            v = v + r.s13r[zz, ch].astype(F32)
        for m in range(2):
            row = m * 8
            for start, length in parts(ch):
                at = m * 32 + start
                r.vs[at : at + length, :] = v[row : row + length]
                row += length
    sent(p.s13, r.s13r.at[0:7])
    both = jnp.zeros((32, 128), F32)
    for m in range(2):
        v = r.vs[m * 32 : m * 32 + 32, :]
        v = v.astype(BF).astype(F32)
        mean = jnp.sum(jnp.sum(v * v, axis=1, keepdims=True), axis=0, keepdims=True) * (1.0 / D)
        both = both + (v * lax.rsqrt(mean + 1e-5) * r.g3[...]).astype(BF).astype(F32)
    r.fs[...] = both

    def half(k):
        return pl.ds(pl.multiple_of(k * 16, 16), 16)

    send(p.fx, r.fs.at[half(1 - c)], r.fr, partner)
    done(p.fx, r.fr)
    r.fb[own, z] = ((r.fs[half(c), :] + r.fr[...]) * 0.25).astype(BF)
    for d in ZORDER:
        send(p.s14, r.fb.at[own, z], r.fb.at[own, z], at_z(rem(z + d, NZ)), 7 - d)
    xy_send(p.s15, lambda m: r.fb.at[own, z], r.fb.at[own, z], 0)
    local.lm.wait()
    local.tg.wait()
    wanted = jnp.broadcast_to(r.tg[...].astype(F32), (B, B)).T[:, 0:1]
    for d in (1, 7, 2, 6, 3, 5, 4):
        zz = rem(z + d, NZ)
        recv(p.s14, r.fb.at[own, zz], d - 1)
        xy_send(p.s15, lambda m: r.fb.at[own, zz], r.fb.at[own, zz], d)
    sent(p.s14, r.fb.at[own, 0:7])
    for d in (0, 1, 7, 2, 6, 3, 5, 4):
        zz = rem(z + d, NZ)
        recv(p.s15, r.fb.at[0:15, zz], d)
        for k in range(NP):
            at = pl.ds(pl.multiple_of(k * 128 + zz * 16, 16), 16)
            r.ff[at, :] = r.fb[k, zz].astype(F32)
    sent(p.s15, r.fb.at[0:15])
    for b in range(16):
        rows = [
            r.ff[pl.ds(h * 1024 + zz * 16 + b, 8, stride=128), :]
            for h in range(2)
            for zz in range(NZ)
        ]
        r.lh[:, b * 128 : (b + 1) * 128] = jnp.concatenate(rows, axis=0).astype(BF)
    r.lp[...] = jnp.dot(r.lh[...], r.lm[...], preferred_element_type=F32)
    send(p.lx, r.lp, r.lr, partner)
    done(p.lx, r.lr)
    mean_f = r.lp[...] + r.lr[...]
    r.logits_o[...] = mean_f.astype(BF)

    ids = (lax.broadcasted_iota(jnp.int32, (B, VD), 1) + t * VD).astype(F32)
    found = jnp.sum(jnp.where(ids == wanted, mean_f, 0.0), axis=1, keepdims=True)
    peak = jnp.max(mean_f, axis=1, keepdims=True)
    total = jnp.sum(jnp.exp(mean_f - peak), axis=1, keepdims=True)
    lane = lax.broadcasted_iota(jnp.int32, (B, B), 1)
    stat = jnp.where(lane == 0, peak, jnp.where(lane == 1, total, jnp.where(lane == 2, found, 0.0)))
    r.sz[z] = stat.T[:8]

    def combine(ref, count):
        peaks = [ref[k, 0:1, :] for k in range(count)]
        top_ = peaks[0]
        for k in range(1, count):
            top_ = jnp.maximum(top_, peaks[k])
        tot = ref[0, 1:2, :] * jnp.exp(peaks[0] - top_)
        hit = ref[0, 2:3, :]
        for k in range(1, count):
            tot = tot + ref[k, 1:2, :] * jnp.exp(peaks[k] - top_)
            hit = hit + ref[k, 2:3, :]
        return top_, tot, hit

    z_send(p.s16, lambda zz: r.sz.at[z], r.sz.at[z])
    done(p.s16, r.sz.at[0:7])
    a, b_, h = combine(r.sz, NZ)
    r.sx[n] = jnp.concatenate([a, b_, h, jnp.zeros((5, 128), F32)], axis=0)
    xy_send(p.s17, lambda m: r.sx.at[n], r.sx.at[n])
    done(p.s17, r.sx.at[0:15])
    a, b_, h = combine(r.sx, NP)
    r.lp_o[...] = h - (a + jnp.log(b_))

    for sem, ref in drains:
        wait_bytes(sem, ref)


def hand_on(logits, logprob, logits_o, logprob_o):
    logits_o[...] = logits[...]
    logprob_o[...] = logprob[...]


def body(
    stream_in, kv_cache, lengths, targets, norm_gains, w_qkv, w_out, w_gate_up, w_down, lm_head,
    fast_in, fast_hidden, fast_out,
):
    freq = np.float32(500000.0) ** (-np.arange(64, dtype=np.float32) * 2.0 / 128)
    freq = jnp.asarray(np.concatenate([freq, freq])[None, :], F32)
    args = dict(
        stream=stream_in, kv=kv_cache, lengths=lengths, targets=targets.reshape(1, B),
        gains=norm_gains, wqkv=w_qkv.T, wout=w_out,
        wgu=w_gate_up.swapaxes(1, 2), wdown=w_down, lmh=lm_head,
        fin=fast_in, fhid=fast_hidden.swapaxes(0, 1), fout=fast_out, freq=freq,
    )
    got = pl.pallas_call(
        functools.partial(kernel, list(args)),
        out_shape=[VM(k.shape, k.dtype) for k in OUTS.values()],
        in_specs=[
            pl.BlockSpec(memory_space=pltpu.SMEM if v is lengths else pl.ANY)
            for v in args.values()
        ],
        out_specs=[pl.BlockSpec(memory_space=VM)] * len(OUTS),
        scratch_shapes=[
            *SCRATCH.values(),
            *LS.values(),
            *(DMA((count,)) for n in PHASES.values() for count in (1, n)),
        ],
        compiler_params=pltpu.CompilerParams(
            collective_id=0, has_side_effects=True, vmem_limit_bytes=60 * 1024 * 1024
        ),
        name="step",
    )(*args.values())
    got = [pltpu.with_memory_space_constraint(k, VM) for k in got]
    got = pl.pallas_call(
        hand_on,
        out_shape=list(OUTS.values()),
        in_specs=[pl.BlockSpec(memory_space=VM)] * 2,
        name="result",
    )(*got)
    return (got[0], got[1].reshape(B))


MEMBER_TP = ("member", "tp_0", "tp_1", "tp_2")
TP = ("tp_0", "tp_1", "tp_2")
IN_SPECS = (
    P(MEMBER_TP, None), P(MEMBER_TP, None, None), P(), P(), P(), P(None, TP), P(TP, None),
    P(None, None, TP), P(TP, None), P(None, TP), P("member", None, None), P("member", None, TP),
    P("member", None),
)


def solution(mesh):
    split = Mesh(
        mesh.devices.reshape(mesh.shape["member"], NX, NZ, NY), MEMBER_TP
    )
    return jax.shard_map(
        body, mesh=split, in_specs=IN_SPECS, out_specs=(P(None, TP), P()), check_vma=False
    )
```

```python
import functools
from types import SimpleNamespace

import jax
import jax.numpy as jnp
import numpy as np
from jax import lax
from jax.experimental import pallas as pl
from jax.experimental.pallas import tpu as pltpu
from jax.sharding import Mesh
from jax.sharding import PartitionSpec as P

MESH = pl.DeviceIdType.MESH
F32 = jnp.float32
BF = jnp.bfloat16
NX, NZ, NY = 4, 8, 4
NP = NX * NY
D, HEADS, KV, HD, CACHE, FFD, VD = 4096, 32, 8, 128, 512, 112, 512
B = 128
QN = 384
ZORDER = (4, 3, 5, 2, 6, 1, 7)
ARRIVAL = (0, 1, 7, 2, 6, 3, 5, 4)
GROUPS = ((0, 3), (3, 2), (5, 3))
NCH, CA, CB = 4, 512, 512
WA, WB = NCH * CA, NCH * CB
BA, BB = CA // 128, CB // 128
HALF = D // 2
NT = (((1,), (1,)), ((), ()))

VM = pltpu.VMEM
DMA = pltpu.SemaphoreType.DMA

SCRATCH = dict(
    st=VM((2, D), BF),
    kvv=VM((2, CACHE, 2 * KV * HD), BF),
    tg=VM((1, B), jnp.int32),
    gn=VM((3, D), F32),
    fi=VM((2, 2, D), F32),
    fh=VM((3, 2, FFD), F32),
    fo=VM((2, D), F32),
    fq=VM((1, 128), F32),
    wq=VM((NZ, 48, 512), BF),
    wo=VM((NP, 32, 256), BF),
    wg=VM((2, 256, D), BF),
    wd=VM((256, D), BF),
    fhx=VM((2, 3, 2, FFD), F32),
    fhy=VM((2, 3, 2, FFD), F32),
    fhp=VM((3, 2, 256), F32),
    lm=VM((HALF, VD), BF),
    sc=VM((64, 128), F32),
    s1s=VM((64, 128), F32),
    s1r=VM((64, 128), F32),
    raw=VM((NP, 16, 512), BF),
    p1=VM((3, 256, 128), F32),
    s3s=VM((NZ, 32, QN), BF),
    s3r=VM((NZ, 32, QN), BF),
    q1=VM((3, 32, 128), F32),
    s4s=VM((128, 128), F32),
    s4r=VM((128, 128), F32),
    hs=VM((96, 128), F32),
    osc=VM((64, 128), F32),
    s5s=VM((64, 128), F32),
    s5r=VM((64, 128), F32),
    att=VM((NP, 16, 512), BF),
    s7s=VM((NZ, 32, 256), BF),
    s7r=VM((NZ, 32, 256), BF),
    mc=VM((2, 128, 256), BF),
    xb=VM((NY, 128, 128), BF),
    mid=VM((NP, 128, 256), BF),
    accg=VM((128, 256), F32),
    accu=VM((128, 256), F32),
    ssq=VM((128, 128), F32),
    hid=VM((128, 256), BF),
    p3=VM((8, 16, D), BF),
    r1a=VM((NY, 16, WA), BF),
    r1b=VM((NY, 2, 16, WB), BF),
    s2a=VM((NY, 16, WA), BF),
    s2b=VM((2, 16, WB), BF),
    r2a=VM((NY, 16, WA), BF),
    r2b=VM((16, WB), BF),
    f3=VM((512, 128), F32),
    g3=VM((32, 128), F32),
    s13s=VM((NZ, NCH, 16, 128), BF),
    s13r=VM((NZ, NCH, 16, 128), BF),
    vs=VM((64, 128), F32),
    fs=VM((32, 128), F32),
    fr=VM((16, 128), F32),
    fb=VM((NP, NZ, 16, 128), BF),
    ff=VM((2048, 128), F32),
    lh=VM((B, HALF), F32),
    lp=VM((B, VD), F32),
    lr=VM((B, VD), F32),
    sz=VM((NZ, 8, 128), F32),
    sx=VM((NP, 8, 128), F32),
)
PHASES = dict(
    wq=1, wqf=1, wo=1, s1=1, s2=1, s3=1, s4=1, s5=1, s6=1, s7=1, s8=7, da=18, db=9, dg=9,
    xg=2, xd=2, fg=2, fd=2, xh=2, fi=1, fh=1, fo=1, fy=1,
    a1=NCH, b1=NCH, a2=NCH, b2=NCH, s13=NCH, fx=1, s14=7, s15=8, lx=1, s16=1, s17=1,
)
LS = dict(ls=DMA((16,)))
OUTS = dict(
    logits_o=jax.ShapeDtypeStruct((B, VD), BF), lp_o=jax.ShapeDtypeStruct((1, B), F32)
)


def kernel(inputs, *refs):
    names = [*inputs, *OUTS, *SCRATCH, *LS]
    r = SimpleNamespace(**dict(zip(names, refs)))
    sems = iter(refs[len(names) :])
    p = SimpleNamespace(**{k: (next(sems), next(sems)) for k in PHASES})
    c, x, z, y = (lax.axis_index(a) for a in MEMBER_TP)
    t = x * 32 + z * 4 + y
    n = x * 4 + y
    xl, par = x // 2, lax.rem(x, 2)
    own = xl * 8 + y * 2 + par
    drains = []
    def rem(v, k):
        return lax.rem(v, k)

    def at_z(zz):
        return (c, x, zz, y)

    def at_xy(xx, yy):
        return (c, xx, z, yy)

    partner = (1 - c, x, z, y)

    def across_z(zz):
        return (1 - c, x, zz, y)

    def copy(phase, src, dst, dev, slot=0):
        return pltpu.make_async_remote_copy(
            src_ref=src,
            dst_ref=dst,
            send_sem=phase[0].at[0],
            recv_sem=phase[1].at[slot],
            device_id=dev,
            device_id_type=MESH,
        )

    def send(phase, src, dst, dev, slot=0):
        copy(phase, src, dst, dev, slot).start()

    def wait_bytes(sem, ref):
        pltpu.make_async_copy(ref, ref, sem).wait()

    def recv(phase, ref, slot=0):
        wait_bytes(phase[1].at[slot], ref)

    def sent(phase, ref):
        drains.append((phase[0].at[0], ref))

    zpeers = [rem(z + d, NZ) for d in ZORDER]
    plane = [
        (rem(x + dx, NX), rem(y + dy, NY))
        for dx, dy in sorted(
            ((a, b) for a in range(NX) for b in range(NY) if a or b),
            key=lambda p: -(min(p[0], 4 - p[0]) + min(p[1], 4 - p[1])),
        )
    ]

    def z_send(phase, src_at, dst):
        for zz in zpeers:
            send(phase, src_at(zz), dst, at_z(zz))

    def xy_send(phase, src_at, dst, slot=0):
        for xx, yy in plane:
            send(phase, src_at(xx * 4 + yy), dst, at_xy(xx, yy), slot)

    def done(phase, ref):
        recv(phase, ref)
        sent(phase, ref)

    bar = pltpu.get_barrier_semaphore()
    peers = [dev for zz in zpeers for dev in (at_z(zz), across_z(zz))]
    peers = peers[:6] + [at_xy(*k) for k in plane] + peers[6:] + [partner]
    for dev in peers:
        pl.semaphore_signal(bar, inc=1, device_id=dev, device_id_type=MESH)

    def qcols(zz, k):
        return r.wqkv.at[:, pl.ds(pl.multiple_of(k * 1024 + zz * 128, 128), 128)]

    def half_cols(k):
        return pl.ds(pl.multiple_of((2 * c + k) * 128, 128), 128)

    local = SimpleNamespace()
    begun = []

    def fetch(src, dst):
        k = pltpu.make_async_copy(src, dst, r.ls.at[len(begun)])
        k.start()
        begun.append(k)
        return k

    local.st = fetch(r.stream, r.st)
    local.gn = fetch(r.gains, r.gn)
    local.fq = fetch(r.freq, r.fq)
    local_wq = [fetch(qcols(z, 2 * c + k), r.wq.at[z, :, half_cols(k)]) for k in range(2)]
    local.wo = fetch(r.wout.at[:, pl.ds(pl.multiple_of(n * 256, 256), 256)], r.wo.at[n])
    local.kvv = fetch(r.kv, r.kvv)
    local.tg = fetch(r.targets, r.tg)
    local.wg = fetch(r.wgu, r.wg.at[:, 0:FFD])
    local.wd = fetch(r.wdown, r.wd.at[0:FFD])
    local.lm = fetch(r.lmh.at[pl.ds(pl.multiple_of(c * HALF, HALF), HALF)], r.lm)

    right, left = at_xy(rem(x + 1, NX), y), at_xy(rem(x + 3, NX), y)

    def weight_piece(i):
        cols = pl.ds(pl.multiple_of(c * HALF + i * 256, 256), 256)
        for dev, a, b in ((right, 0, 64), (left, 64, FFD)):
            g = r.wg.at[:, 128 + a : 128 + b, cols]
            send(p.xg, r.wgu.at[:, a:b, cols], g, dev, i // 4)
            send(p.xd, r.wdown.at[a:b, cols], r.wd.at[128 + a : 128 + b, cols], dev, i // 4)

    def pass_weights(g):
        cols = pl.ds(pl.multiple_of(c * HALF + g * 1024, 1024), 1024)
        for came, went, at in (
            (p.xg, p.fg, r.wg.at[:, 128 : 128 + FFD, cols]),
            (p.xd, p.fd, r.wd.at[128 : 128 + FFD, cols]),
        ):
            recv(came, at, g)
            send(went, at, at, partner, g)

    def spread(scratch, dst):
        for zz in range(NZ):
            dst[zz * 8 : zz * 8 + 8] = scratch[pl.ds(zz, 8, stride=8), :]

    z8 = pl.ds(pl.multiple_of(z * 8, 8), 8)

    def z_then_plane(zphase, pphase, s, rr, buf, start=True, beside=lambda: None):
        def piece(zz):
            return pl.ds(pl.multiple_of(zz * 8, 8), 8)

        if start:
            z_send(zphase, lambda zz: s.at[piece(zz)], rr.at[z8])
        beside()
        rr[z8, :] = s[z8, :]
        done(zphase, rr.at[0:56])
        for k in range(4):
            rows = [rr[pl.ds(j * 4 + k, 8, stride=8), :] for j in range(2)]
            buf[n, :, k * 128 : (k + 1) * 128] = jnp.concatenate(rows, axis=0).astype(BF)
        xy_send(pphase, lambda m: buf.at[n], buf.at[n])
        return lambda: done(pphase, buf.at[0:15])

    local.st.wait()
    x32 = r.st[...].astype(F32)
    rs = lax.rsqrt(jnp.mean(x32 * x32, axis=-1, keepdims=True) + 1e-5)
    for b in range(32):
        for j in range(2):
            r.sc[j * 32 + b : j * 32 + b + 1, :] = x32[j : j + 1, b * 128 : (b + 1) * 128]
    spread(r.sc, r.s1s)
    r.s4s[...] = jnp.zeros((128, 128), F32)
    row8 = lax.broadcasted_iota(jnp.int32, (8, 128), 0)
    lane8 = lax.broadcasted_iota(jnp.int32, (8, 128), 1)
    rs8 = jnp.where(row8 < 4, rs[0:1, 0:1], rs[1:2, 0:1])

    pl.semaphore_wait(bar, len(peers))

    for zz in zpeers:
        send(p.s1, r.s1s.at[pl.ds(pl.multiple_of(zz * 8, 8), 8)], r.s1r.at[z8], at_z(zz))
    for zz in zpeers:
        for k in range(2):
            send(p.wq, qcols(zz, 2 * c + k), r.wq.at[z, :, half_cols(k)], at_z(zz))
    weight_piece(0)
    weight_piece(1)
    send(p.fi, r.fin, r.fi, partner)
    send(p.fh, r.fhid, r.fh, partner)
    send(p.fo, r.fout, r.fo, partner)
    send(p.xh, r.fhid, r.fhx.at[0], right, 0)
    send(p.xh, r.fhid, r.fhx.at[1], left, 1)
    finish = z_then_plane(p.s1, p.s2, r.s1s, r.s1r, r.raw, False)
    local.fq.wait()
    local.gn.wait()
    pos = [r.lengths[rem(2 * t + j, B)] for j in range(2)]
    ang = jnp.where(row8 < 4, pos[0], pos[1]).astype(F32) * r.fq[0:1, :]
    cos8 = jnp.cos(ang)
    sin8 = jnp.where(lane8 < 64, -jnp.sin(ang), jnp.sin(ang))
    for b in range(32):
        r.g3[b : b + 1, :] = r.gn[2:3, b * 128 : (b + 1) * 128]

    for k in range(2):
        local_wq[k].wait()
    done(p.wq, r.wq.at[0:7, :, 0:256])
    mine = r.wq.at[:, :, pl.ds(pl.multiple_of(c * 256, 256), 256)]
    send(p.wqf, mine, mine, partner)
    done(p.wqf, mine)
    gq = jnp.concatenate(
        [r.gn[0:1, pl.ds(pl.multiple_of(k * 1024 + z * 128, 128), 128)] for k in range(4)], axis=1
    )
    finish()
    lhs = (r.raw[...].reshape(256, 512).astype(F32) * gq).astype(BF)
    prod = lax.dot_general(lhs, r.wq[...].reshape(QN, 512), NT, preferred_element_type=F32)
    for l in range(3):
        r.p1[l] = prod[:, l * 128 : (l + 1) * 128]
    for zz in range(NZ):
        for l in range(3):
            r.s3s[zz, :, l * 128 : (l + 1) * 128] = r.p1.at[l][
                pl.ds(zz, 32, stride=8), :
            ].astype(BF)
    z_send(p.s3, lambda zz: r.s3s.at[zz], r.s3r.at[z])
    weight_piece(2)
    weight_piece(3)
    r.s3r[z] = r.s3s[z]
    done(p.s3, r.s3r.at[0:7])
    acc = r.s3r[0].astype(F32)
    for s in range(1, NZ):
        acc = acc + r.s3r[s].astype(F32)
    for l in range(3):
        r.q1[l] = acc[:, l * 128 : (l + 1) * 128]
    for l in range(3):
        for j in range(2):
            r.s4s[pl.ds(l * 2 + j, 16, stride=8), :] = r.q1.at[l][pl.ds(j, 16, stride=2), :]

    def tile(m):
        return pl.ds(pl.multiple_of(m * 8, 8), 8)

    xy_send(p.s4, lambda m: r.s4s.at[tile(m)], r.s4r.at[tile(n)])
    xy_send(
        p.wo,
        lambda m: r.wout.at[:, pl.ds(pl.multiple_of(m * 256, 256), 256)],
        r.wo.at[n],
    )
    r.s4r[tile(n), :] = r.s4s[tile(n), :]
    done(p.s4, r.s4r.at[0:120])

    blocks = {
        (yy, l): jnp.concatenate(
            [r.s4r[pl.ds(yy * 8 + l * 2 + j, 4, stride=32), :] for j in range(2)], axis=0
        )
        for yy in range(NY)
        for l in range(3)
    }
    for hh in range(12):
        val = jnp.zeros((8, 128), F32)
        lane = 0
        while lane < 128:
            col = hh * 128 + lane
            tt, i = divmod(col, 48)
            at = (tt // 4) * 48 + i
            l, src = divmod(at, 128)
            width = min(48 - i, 128 - src, 128 - lane)
            piece = blocks[(tt % 4, l)]
            shift = (lane - src) % 128
            if shift:
                piece = pltpu.roll(piece, shift, 1)
            val = jnp.where((lane8 >= lane) & (lane8 < lane + width), piece, val)
            lane += width
        val = (val * rs8).astype(BF).astype(F32)
        turned = (val * cos8 + pltpu.roll(val, 64, 1) * sin8).astype(BF).astype(F32)
        if hh >= 4:
            turned = jnp.where(row8 % 4 == 3, val, turned)
        r.hs[pl.ds(hh, 8, stride=12), :] = turned

    local.kvv.wait()
    inv_root = HD**-0.5
    group = lax.broadcasted_iota(jnp.int32, (32, 128), 0) // 4
    group8 = (
        lax.broadcasted_iota(jnp.int32, (32, 8), 0) // 4
        == lax.broadcasted_iota(jnp.int32, (32, 8), 1)
    )
    place = lax.broadcasted_iota(jnp.int32, (32, CACHE), 1)
    for j in range(2):
        q = r.hs[j * 48 : j * 48 + 32, :]
        kn = r.hs[j * 48 + 32 : j * 48 + 40, :].astype(BF)
        vn = r.hs[j * 48 + 40 : j * 48 + 48, :].astype(BF)
        qd = jnp.concatenate([jnp.where(group == k, q, 0.0) for k in range(KV)], axis=1).astype(BF)
        scores = (
            lax.dot_general(qd, r.kvv[j, :, : KV * HD], NT, preferred_element_type=F32) * inv_root
        )
        fresh = lax.dot_general(q.astype(BF), kn, NT, preferred_element_type=F32)
        fresh = jnp.sum(jnp.where(group8, fresh, 0.0), axis=1, keepdims=True) * inv_root
        scores = jnp.where(place < pos[j], scores, -1e30)
        peak = jnp.maximum(jnp.max(scores, axis=1, keepdims=True), fresh)
        weights = jnp.exp(scores - peak)
        fresh_w = jnp.exp(fresh - peak)
        total = jnp.sum(weights, axis=1, keepdims=True) + fresh_w
        probs = (weights / total).astype(BF)
        fresh_p = jnp.where(group8, fresh_w / total, 0.0).astype(BF)
        wide = jnp.dot(probs, r.kvv[j, :, KV * HD :], preferred_element_type=F32)
        out = jnp.dot(fresh_p, vn, preferred_element_type=F32)
        for k in range(KV):
            out = out + jnp.where(group == k, wide[:, k * 128 : (k + 1) * 128], 0.0)
        r.osc[j * 32 : j * 32 + 32, :] = out.astype(BF).astype(F32)

    spread(r.osc, r.s5s)

    def beside():
        weight_piece(4)
        weight_piece(5)

    finish = z_then_plane(p.s5, p.s6, r.s5s, r.s5r, r.att, beside=beside)
    pass_weights(0)
    local.wo.wait()
    done(p.wo, r.wo.at[0:15])
    resid = r.raw[:, :, pl.ds(pl.multiple_of(x * 128, 128), 128)].reshape(256, 128).astype(F32)
    lo = resid * jnp.where(z == 2 * y, 1.0, 0.0)
    hi = resid * jnp.where(z == 2 * y + 1, 1.0, 0.0)
    finish()
    prod = jnp.dot(
        r.att[...].reshape(256, 512), r.wo[...].reshape(512, 256), preferred_element_type=F32
    ) + jnp.concatenate([lo, hi], axis=1)
    for h in range(2):
        for ys in range(NY):
            for j in range(2):
                at = [((m * 2 + h) * 4 + ys) * 16 + j * 8 for m in range(2)]
                r.s7s[h * 4 + ys, j * 16 : j * 16 + 16, :] = jnp.concatenate(
                    [prod[a : a + 8] for a in at], axis=0
                ).astype(BF)
    for zz in zpeers:
        send(p.s7, r.s7s.at[zz], r.s7r.at[z], across_z(zz))
    send(p.s7, r.s7s.at[z], r.s7r.at[z], partner)
    weight_piece(6)
    weight_piece(7)
    recv(p.xh, r.fhx.at[0], 0)
    recv(p.xh, r.fhx.at[1], 1)
    sent(p.xh, r.fhx)
    send(p.fy, r.fhx, r.fhy, partner)
    done(p.s7, r.s7r)
    acc = r.s7r[0].astype(F32)
    for s in range(1, NZ):
        acc = acc + r.s7r[s].astype(F32)

    def tile_rows(d):
        return pl.ds(ARRIVAL.index(d % NZ) * 16, 16)

    for j in range(2):
        r.mc[j, tile_rows(0), :] = acc[j * 16 : j * 16 + 16].astype(BF)
    for d in ZORDER:
        at = r.mc.at[:, tile_rows(0)]
        send(p.s8, at, r.mc.at[:, tile_rows(-d)], at_z(rem(z + d, NZ)), 7 - d)

    def tile_on(k):
        rows = tile_rows(k)
        at = ARRIVAL.index(k)
        late = next(i for i, (a, b) in enumerate(GROUPS) if a <= at < a + b)
        for d in (2, 1, 3):
            xx, yy = rem(x + d, NX), rem(y + d, NY)
            at = r.mid.at[n, rows]
            send(p.da, r.mc.at[par, rows], at, at_xy(x, yy), 6 - d + 6 * late)
            send(p.da, r.mc.at[rem(xx, 2), rows], at, at_xy(xx, y), 3 - d + 6 * late)
            at = r.mc.at[1 - par, rows, right_cols]
            send(p.db, at, r.xb.at[y, rows], at_xy(x, yy), 3 - d + 3 * late)

    left_cols, right_cols = pl.ds(0, 128), pl.ds(128, 128)
    tile_on(0)
    pass_weights(1)
    r.accg[...] = jnp.zeros((128, 256), F32)
    r.accu[...] = jnp.zeros((128, 256), F32)
    r.ssq[...] = jnp.zeros((128, 128), F32)
    for a in (FFD, 128 + FFD):
        r.wg[:, a : a + 16, :] = jnp.zeros((2, 16, D), BF)
        r.wd[a : a + 16, :] = jnp.zeros((16, D), BF)
    done(p.fi, r.fi)
    done(p.fh, r.fh)
    done(p.fo, r.fo)
    done(p.fy, r.fhy)
    r.fhp[...] = jnp.zeros((3, 2, 256), F32)
    r.fhp[:, :, 0:FFD] = r.fh[...]
    lane_h = lax.broadcasted_iota(jnp.int32, (3, 2, FFD), 2)
    r.fhp[:, :, 128 : 128 + FFD] = jnp.where(lane_h < 64, r.fhy[0], r.fhy[1])
    mine_g = r.wg.at[:, 128 : 128 + FFD, 0:HALF]
    mine_d = r.wd.at[128 : 128 + FFD, 0:HALF]
    for k in (p.xg, p.fg):
        sent(k, mine_g)
    for k in (p.xd, p.fd):
        sent(k, mine_d)
    for k in (local.wg, local.wd):
        k.wait()
    for d in ARRIVAL[1:]:
        recv(p.s8, r.mc.at[:, 0:16], d - 1)
        tile_on(d)
    sent(p.s8, r.mc.at[:, 0:112])

    near = (1, 3, 2)
    sent(p.da, r.mid.at[0:6])
    sent(p.db, r.xb.at[0:3])
    r.mid[n] = r.mc[par]
    for g in range(2):
        cols = pl.ds(pl.multiple_of((1 - c) * HALF + g * 1024, 1024), 1024)
        recv(p.fg, r.wg.at[:, 128 : 128 + FFD, cols], g)
        recv(p.fd, r.wd.at[128 : 128 + FFD, cols], g)

    def ffn_chunk(m):
        v = r.mid[m].astype(F32)
        r.ssq[...] += v[:, :128] * v[:, :128] + v[:, 128:] * v[:, 128:]
        cols = pl.ds(pl.multiple_of(m * 256, 256), 256)
        g = r.gn[1:2, cols]
        v4 = v.reshape(8, 2, 8, 256)
        for k, total in enumerate((r.accg, r.accu)):
            f = jnp.concatenate(
                [
                    (r.fi[i, k : k + 1, cols] * g).reshape(1, 1, 1, 256)
                    for i in range(2)
                ],
                axis=1,
            )
            act = (v4 * f).reshape(128, 256).astype(BF)
            total[...] += lax.dot_general(
                act, r.wg[k, :, cols], NT, preferred_element_type=F32
            )

    ffn_chunk(n)
    for late, rows in enumerate(pl.ds(a * 16, b * 16) for a, b in GROUPS):
        for d in near:
            m = rem(x + d, NX) * 4 + y
            recv(p.da, r.mid.at[m, rows], d - 1 + 6 * late)
            at = r.mid.at[m, rows, left_cols]
            for e in (2, 1, 3):
                yy = rem(y + e, NY)
                send(p.dg, at, at, at_xy(x, yy), (d - 1) * 3 + 3 - e)
            yy = rem(y + d, NY)
            m = x * 4 + yy
            recv(p.da, r.mid.at[m, rows], d + 2 + 6 * late)
            recv(p.db, r.xb.at[yy, rows], d - 1 + 3 * late)
            to = r.mid.at[m, rows, right_cols]
            for e in (2, 1, 3):
                xx = rem(x + e, NX)
                at = to if e == 2 else r.xb.at[yy, rows]
                send(p.dg, at, to, at_xy(xx, y), (3 - e) * 3 + d - 1)
    sent(p.dg, r.mid.at[0:9])

    def line_step(i, carry):
        ffn_chunk(rem(x + 1 + i, NX) * 4 + y)
        ffn_chunk(x * 4 + rem(y + 1 + i, NY))
        return carry

    lax.fori_loop(0, 3, line_step, 0)

    def diag_step(i, carry):
        m = rem(x + 1 + i // 3, NX) * 4 + rem(y + 1 + i % 3, NY)
        recv(p.dg, r.mid.at[m], i)
        ffn_chunk(m)
        return carry

    lax.fori_loop(0, 9, diag_step, 0)
    scale = lax.rsqrt(jnp.sum(r.ssq[...], axis=1, keepdims=True) * (1.0 / D) + 1e-5)

    def by_member(k):
        return jnp.concatenate(
            [r.fhp[k, i : i + 1, :].reshape(1, 1, 1, 256) for i in range(2)], axis=1
        )

    gate = (r.accg[...] * scale).reshape(8, 2, 8, 256) * by_member(0)
    up = (r.accu[...] * scale).reshape(8, 2, 8, 256) * by_member(1)
    hidden = gate / (1.0 + jnp.exp(-gate)) * up * by_member(2)
    r.hid[...] = hidden.reshape(128, 256).astype(BF)

    def chunk(ch):
        return pl.ds(pl.multiple_of(ch * CA, CA), CA)

    def chunk_b(ch):
        return pl.ds(pl.multiple_of(ch * CB, CB), CB)

    def high(ch):
        return pl.ds(pl.multiple_of(WA + ch * CB, 128), CB)

    other = 1 - xl
    opposite = at_xy(rem(x + 2, NX), y)

    def a1(ch):
        send(p.a1, r.p3.at[pl.ds(other * 4, 4), :, chunk(ch)], r.r1a.at[:, :, chunk(ch)], opposite, ch)

    def b1(ch, yy):
        for h in range(2):
            at = r.p3.at[h * 4 + yy, :, high(ch)]
            send(p.b1, at, r.r1b.at[y, h, :, chunk_b(ch)], at_xy(x, yy), ch)

    def down_step(ch, carry):
        for cols in (chunk(ch), high(ch)):
            v = jnp.dot(r.hid[...], r.wd[:, cols], preferred_element_type=F32)
            for k in range(NZ):
                r.p3[rem(z + ARRIVAL[k], NZ), :, cols] = v[k * 16 : k * 16 + 16].astype(BF)
        a1(ch)
        for d in (2, 1, 3):
            b1(ch, rem(y + d, NY))
        return carry

    lax.fori_loop(0, NCH, down_step, 0)

    def a2(ch, yy):
        send(p.a2, r.s2a.at[yy, :, chunk(ch)], r.r2a.at[y, :, chunk(ch)], at_xy(x, yy), ch)

    def b2(ch):
        send(p.b2, r.s2b.at[other, :, chunk_b(ch)], r.r2b.at[:, chunk_b(ch)], opposite, ch)

    def second_step(ch, carry):
        recv(p.a1, r.r1a.at[:, :, chunk(ch)], ch)
        v = r.p3[pl.ds(xl * 4, 4), :, chunk(ch)].astype(F32) + r.r1a[:, :, chunk(ch)].astype(F32)
        r.s2a[:, :, chunk(ch)] = v.astype(BF)
        for d in (2, 1, 3):
            a2(ch, rem(y + d, NY))
        recv(p.b1, r.r1b.at[0:3, :, :, chunk_b(ch)], ch)
        v = jnp.concatenate(
            [r.p3[pl.ds(h * 4 + y, 1), :, high(ch)].astype(F32) for h in range(2)], axis=0
        )
        for d in near:
            v = v + r.r1b[rem(y + d, NY), :, :, chunk_b(ch)].astype(F32)
        r.s2b[:, :, chunk_b(ch)] = v.astype(BF)
        b2(ch)
        return carry

    lax.fori_loop(0, NCH, second_step, 0)
    sent(p.a1, r.r1a)
    sent(p.b1, r.r1b.at[0:3])
    sent(p.a2, r.r2a.at[0:3])
    sent(p.b2, r.r2b)

    row16 = lax.broadcasted_iota(jnp.int32, (16, 128), 0)
    own_row = rem(row16, 8) == z
    away = rem(xl * 4 + y - z + NZ, NZ)
    turn = (away + 3) // 4
    slot = turn * (2 - turn) * (2 * away - 1) + turn * (turn - 1) // 2 * (16 - 2 * away)
    tile16 = pl.ds(pl.multiple_of(slot * 16, 16), 16)

    def parts(ch):
        return (ch * BA, BA), (NCH * BA + ch * BB, BB)

    def last_step(ch):
        recv(p.a2, r.r2a.at[0:3, :, chunk(ch)], ch)
        recv(p.b2, r.r2b.at[:, chunk_b(ch)], ch)
        for b in [b for start, length in parts(ch) for b in range(start, start + length)]:
            if b < NCH * BA:
                cols = slice(b * 128, (b + 1) * 128)
                v = r.s2a[y, :, cols].astype(F32)
                for d in near:
                    v = v + r.r2a[rem(y + d, NY), :, cols].astype(F32)
            else:
                cols = slice((b - NCH * BA) * 128, (b - NCH * BA + 1) * 128)
                v = r.s2b[xl, :, cols].astype(F32) + r.r2b[:, cols].astype(F32)
            at = slice(b * 128, (b + 1) * 128)
            v = v * jnp.where(row16 < 8, r.fo[0:1, at], r.fo[1:2, at])
            m = r.mid[b // 2, tile16, (b % 2) * 128 : (b % 2 + 1) * 128].astype(F32)
            r.f3[b * 16 : (b + 1) * 16, :] = v + jnp.where(own_row, m, 0.0)
        for zz in range(NZ):
            r.s13s[zz, ch] = chunk_rows(zz, ch).astype(BF)
        for zz in zpeers:
            send(p.s13, r.s13s.at[zz, ch], r.s13r.at[z, ch], at_z(zz), ch)

    def chunk_rows(zz, ch):
        return jnp.concatenate(
            [
                r.f3[pl.ds(start * 16 + m * 8 + zz, length, stride=16), :]
                for m in range(2)
                for start, length in parts(ch)
            ],
            axis=0,
        )

    for ch in range(NCH):
        last_step(ch)
    for ch in range(NCH):
        v = chunk_rows(z, ch)
        recv(p.s13, r.s13r.at[0:7, ch], ch)
        for zz in zpeers:
            v = v + r.s13r[zz, ch].astype(F32)
        for m in range(2):
            row = m * 8
            for start, length in parts(ch):
                at = m * 32 + start
                r.vs[at : at + length, :] = v[row : row + length]
                row += length
    sent(p.s13, r.s13r.at[0:7])
    both = jnp.zeros((32, 128), F32)
    for m in range(2):
        v = r.vs[m * 32 : m * 32 + 32, :]
        v = v.astype(BF).astype(F32)
        mean = jnp.sum(jnp.sum(v * v, axis=1, keepdims=True), axis=0, keepdims=True) * (1.0 / D)
        both = both + (v * lax.rsqrt(mean + 1e-5) * r.g3[...]).astype(BF).astype(F32)
    r.fs[...] = both

    def half(k):
        return pl.ds(pl.multiple_of(k * 16, 16), 16)

    send(p.fx, r.fs.at[half(1 - c)], r.fr, partner)
    done(p.fx, r.fr)
    r.fb[own, z] = ((r.fs[half(c), :] + r.fr[...]) * 0.25).astype(BF)
    for d in ZORDER:
        send(p.s14, r.fb.at[own, z], r.fb.at[own, z], at_z(rem(z + d, NZ)), 7 - d)
    xy_send(p.s15, lambda m: r.fb.at[own, z], r.fb.at[own, z], 0)
    local.lm.wait()
    local.tg.wait()
    wanted = jnp.broadcast_to(r.tg[...].astype(F32), (B, B)).T[:, 0:1]
    for d in ARRIVAL[1:]:
        zz = rem(z + d, NZ)
        recv(p.s14, r.fb.at[own, zz], d - 1)
        xy_send(p.s15, lambda m: r.fb.at[own, zz], r.fb.at[own, zz], d)
    sent(p.s14, r.fb.at[own, 0:7])
    for d in ARRIVAL:
        zz = rem(z + d, NZ)
        recv(p.s15, r.fb.at[0:15, zz], d)
        for k in range(NP):
            at = pl.ds(pl.multiple_of(k * 128 + zz * 16, 16), 16)
            r.ff[at, :] = r.fb[k, zz].astype(F32)
        for h in range(2):
            to = pl.ds(pl.multiple_of(h * 64 + zz * 8, 8), 8)
            for b in range(16):
                r.lh[to, b * 128 : (b + 1) * 128] = r.ff[
                    pl.ds(h * 1024 + zz * 16 + b, 8, stride=128), :
                ]
    sent(p.s15, r.fb.at[0:15])
    r.lp[...] = jnp.dot(r.lh[...].astype(BF), r.lm[...], preferred_element_type=F32)
    send(p.lx, r.lp, r.lr, partner)
    done(p.lx, r.lr)
    mean_f = r.lp[...] + r.lr[...]
    r.logits_o[...] = mean_f.astype(BF)

    ids = (lax.broadcasted_iota(jnp.int32, (B, VD), 1) + t * VD).astype(F32)
    found = jnp.sum(jnp.where(ids == wanted, mean_f, 0.0), axis=1, keepdims=True)
    peak = jnp.max(mean_f, axis=1, keepdims=True)
    total = jnp.sum(jnp.exp(mean_f - peak), axis=1, keepdims=True)
    lane = lax.broadcasted_iota(jnp.int32, (B, B), 1)
    stat = jnp.where(lane == 0, peak, jnp.where(lane == 1, total, jnp.where(lane == 2, found, 0.0)))
    r.sz[z] = stat.T[:8]

    def combine(ref, count):
        peaks = [ref[k, 0:1, :] for k in range(count)]
        top_ = peaks[0]
        for k in range(1, count):
            top_ = jnp.maximum(top_, peaks[k])
        tot = ref[0, 1:2, :] * jnp.exp(peaks[0] - top_)
        hit = ref[0, 2:3, :]
        for k in range(1, count):
            tot = tot + ref[k, 1:2, :] * jnp.exp(peaks[k] - top_)
            hit = hit + ref[k, 2:3, :]
        return top_, tot, hit

    z_send(p.s16, lambda zz: r.sz.at[z], r.sz.at[z])
    done(p.s16, r.sz.at[0:7])
    a, b_, h = combine(r.sz, NZ)
    r.sx[n] = jnp.concatenate([a, b_, h, jnp.zeros((5, 128), F32)], axis=0)
    xy_send(p.s17, lambda m: r.sx.at[n], r.sx.at[n])
    done(p.s17, r.sx.at[0:15])
    a, b_, h = combine(r.sx, NP)
    r.lp_o[...] = h - (a + jnp.log(b_))

    for sem, ref in drains:
        wait_bytes(sem, ref)


def hand_on(logits, logprob, logits_o, logprob_o):
    logits_o[...] = logits[...]
    logprob_o[...] = logprob[...]


def body(
    stream_in, kv_cache, lengths, targets, norm_gains, w_qkv, w_out, w_gate_up, w_down, lm_head,
    fast_in, fast_hidden, fast_out,
):
    freq = np.float32(500000.0) ** (-np.arange(64, dtype=np.float32) * 2.0 / 128)
    freq = jnp.asarray(np.concatenate([freq, freq])[None, :], F32)
    args = dict(
        stream=stream_in, kv=kv_cache, lengths=lengths, targets=targets.reshape(1, B),
        gains=norm_gains, wqkv=w_qkv.T, wout=w_out,
        wgu=w_gate_up.swapaxes(1, 2), wdown=w_down, lmh=lm_head,
        fin=fast_in, fhid=fast_hidden.swapaxes(0, 1), fout=fast_out, freq=freq,
    )
    got = pl.pallas_call(
        functools.partial(kernel, list(args)),
        out_shape=[VM(k.shape, k.dtype) for k in OUTS.values()],
        in_specs=[
            pl.BlockSpec(memory_space=pltpu.SMEM if v is lengths else pl.ANY)
            for v in args.values()
        ],
        out_specs=[pl.BlockSpec(memory_space=VM)] * len(OUTS),
        scratch_shapes=[
            *SCRATCH.values(),
            *LS.values(),
            *(DMA((count,)) for n in PHASES.values() for count in (1, n)),
        ],
        compiler_params=pltpu.CompilerParams(
            collective_id=0, has_side_effects=True, vmem_limit_bytes=60 * 1024 * 1024
        ),
        name="step",
    )(*args.values())
    got = [pltpu.with_memory_space_constraint(k, VM) for k in got]
    got = pl.pallas_call(
        hand_on,
        out_shape=list(OUTS.values()),
        in_specs=[pl.BlockSpec(memory_space=VM)] * 2,
        name="result",
    )(*got)
    return (got[0], got[1].reshape(B))


MEMBER_TP = ("member", "tp_0", "tp_1", "tp_2")
TP = ("tp_0", "tp_1", "tp_2")
IN_SPECS = (
    P(MEMBER_TP, None), P(MEMBER_TP, None, None), P(), P(), P(), P(None, TP), P(TP, None),
    P(None, None, TP), P(TP, None), P(None, TP), P("member", None, None), P("member", None, TP),
    P("member", None),
)


def solution(mesh):
    split = Mesh(
        mesh.devices.reshape(mesh.shape["member"], NX, NZ, NY), MEMBER_TP
    )
    return jax.shard_map(
        body, mesh=split, in_specs=IN_SPECS, out_specs=(P(None, TP), P()), check_vma=False
    )
```

```python
import functools
from types import SimpleNamespace

import jax
import jax.numpy as jnp
import numpy as np
from jax import lax
from jax.experimental import pallas as pl
from jax.experimental.pallas import tpu as pltpu
from jax.sharding import Mesh
from jax.sharding import PartitionSpec as P

MESH = pl.DeviceIdType.MESH
F32 = jnp.float32
BF = jnp.bfloat16
NX, NZ, NY = 4, 8, 4
NP = NX * NY
D, HEADS, KV, HD, CACHE, FFD, VD = 4096, 32, 8, 128, 512, 112, 512
B = 128
QN = 384
ZORDER = (4, 3, 5, 2, 6, 1, 7)
FAR_Z = (3, 5, 4)
ARRIVAL = (0, 1, 7, 2, 6, 3, 5, 4)
GROUPS = ((0, 3), (3, 2), (5, 3))
NCH, CA, CB = 4, 512, 512
WA, WB = NCH * CA, NCH * CB
BA, BB = CA // 128, CB // 128
HALF = D // 2
NT = (((1,), (1,)), ((), ()))

VM = pltpu.VMEM
DMA = pltpu.SemaphoreType.DMA

SCRATCH = dict(
    st=VM((2, D), BF),
    kvv=VM((2, CACHE, 2 * KV * HD), BF),
    tg=VM((1, B), jnp.int32),
    gn=VM((3, D), F32),
    fi=VM((2, 2, D), F32),
    fh=VM((3, 2, FFD), F32),
    fo=VM((2, D), F32),
    fq=VM((1, 128), F32),
    wq=VM((NZ, 48, 512), BF),
    wo=VM((NP, 32, 256), BF),
    wg=VM((2, 256, D), BF),
    wd=VM((256, D), BF),
    fhx=VM((2, 3, 2, FFD), F32),
    fhy=VM((2, 3, 2, FFD), F32),
    fhp=VM((3, 2, 256), F32),
    lm=VM((HALF, VD), BF),
    sc=VM((64, 128), F32),
    s1s=VM((64, 128), F32),
    s1r=VM((64, 128), F32),
    raw=VM((NP, 16, 512), BF),
    p1=VM((3, 256, 128), F32),
    s3s=VM((NZ, 32, QN), BF),
    s3r=VM((NZ, 32, QN), BF),
    q1=VM((3, 32, 128), F32),
    s4s=VM((128, 128), F32),
    s4r=VM((128, 128), F32),
    hs=VM((96, 128), F32),
    osc=VM((64, 128), F32),
    s5s=VM((64, 128), F32),
    s5r=VM((64, 128), F32),
    att=VM((NP, 16, 512), BF),
    s7s=VM((NZ, 32, 256), BF),
    s7r=VM((NZ, 32, 256), BF),
    mc=VM((2, 128, 256), BF),
    xb=VM((NY, 128, 128), BF),
    mid=VM((NP, 128, 256), BF),
    accg=VM((128, 256), F32),
    accu=VM((128, 256), F32),
    ssq=VM((128, 128), F32),
    hid=VM((128, 256), BF),
    p3=VM((8, 16, D), BF),
    r1a=VM((NY, 16, WA), BF),
    r1b=VM((NY, 2, 16, WB), BF),
    s2a=VM((NY, 16, WA), BF),
    s2b=VM((2, 16, WB), BF),
    r2a=VM((NY, 16, WA), BF),
    r2b=VM((16, WB), BF),
    f3=VM((512, 128), F32),
    g3=VM((32, 128), F32),
    s13s=VM((NZ, NCH, 16, 128), BF),
    s13r=VM((NZ, NCH, 16, 128), BF),
    vs=VM((64, 128), F32),
    fs=VM((32, 128), F32),
    fr=VM((16, 128), F32),
    fb=VM((NP, NZ, 16, 128), BF),
    ff=VM((2048, 128), F32),
    lh=VM((B, HALF), F32),
    lp=VM((B, VD), F32),
    lr=VM((B, VD), F32),
    sz=VM((NZ, 8, 128), F32),
    sx=VM((NP, 8, 128), F32),
)
PHASES = dict(
    wq=1, wqf=1, wo=1, s1=1, s2=1, s3=1, s4=1, s5=1, s6=1, s7=1, s8=7, da=18, db=9, dg=9,
    xg=2, xd=2, fg=2, fd=2, xh=2, fi=1, fh=1, fo=1, fy=1,
    a1=NCH, b1=NCH, a2=NCH, b2=NCH, s13=NCH, fx=1, s14=7, s15=8, pz=8, lx=1, s16=1, s17=1,
)
LS = dict(ls=DMA((16,)))
OUTS = dict(
    logits_o=jax.ShapeDtypeStruct((B, VD), BF), lp_o=jax.ShapeDtypeStruct((1, B), F32)
)


def kernel(inputs, *refs):
    names = [*inputs, *OUTS, *SCRATCH, *LS]
    r = SimpleNamespace(**dict(zip(names, refs)))
    sems = iter(refs[len(names) :])
    p = SimpleNamespace(**{k: (next(sems), next(sems)) for k in PHASES})
    c, x, z, y = (lax.axis_index(a) for a in MEMBER_TP)
    t = x * 32 + z * 4 + y
    n = x * 4 + y
    xl, par = x // 2, lax.rem(x, 2)
    own = xl * 8 + y * 2 + par
    drains = []
    def rem(v, k):
        return lax.rem(v, k)

    def at_z(zz):
        return (c, x, zz, y)

    def at_xy(xx, yy):
        return (c, xx, z, yy)

    partner = (1 - c, x, z, y)

    def across_z(zz):
        return (1 - c, x, zz, y)

    def copy(phase, src, dst, dev, slot=0):
        return pltpu.make_async_remote_copy(
            src_ref=src,
            dst_ref=dst,
            send_sem=phase[0].at[0],
            recv_sem=phase[1].at[slot],
            device_id=dev,
            device_id_type=MESH,
        )

    def send(phase, src, dst, dev, slot=0):
        copy(phase, src, dst, dev, slot).start()

    def wait_bytes(sem, ref):
        pltpu.make_async_copy(ref, ref, sem).wait()

    def recv(phase, ref, slot=0):
        wait_bytes(phase[1].at[slot], ref)

    def sent(phase, ref):
        drains.append((phase[0].at[0], ref))

    zpeers = [rem(z + d, NZ) for d in ZORDER]
    plane = [
        (rem(x + dx, NX), rem(y + dy, NY))
        for dx, dy in sorted(
            ((a, b) for a in range(NX) for b in range(NY) if a or b),
            key=lambda p: -(min(p[0], 4 - p[0]) + min(p[1], 4 - p[1])),
        )
    ]

    def z_send(phase, src_at, dst):
        for zz in zpeers:
            send(phase, src_at(zz), dst, at_z(zz))

    def xy_send(phase, src_at, dst, slot=0):
        for xx, yy in plane:
            send(phase, src_at(xx * 4 + yy), dst, at_xy(xx, yy), slot)

    def done(phase, ref):
        recv(phase, ref)
        sent(phase, ref)

    bar = pltpu.get_barrier_semaphore()
    peers = [dev for zz in zpeers for dev in (at_z(zz), across_z(zz))]
    peers = peers[:6] + [at_xy(*k) for k in plane] + peers[6:] + [partner]
    for dev in peers:
        pl.semaphore_signal(bar, inc=1, device_id=dev, device_id_type=MESH)

    def qcols(zz, k):
        return r.wqkv.at[:, pl.ds(pl.multiple_of(k * 1024 + zz * 128, 128), 128)]

    def half_cols(k):
        return pl.ds(pl.multiple_of((2 * c + k) * 128, 128), 128)

    local = SimpleNamespace()
    begun = []

    def fetch(src, dst):
        k = pltpu.make_async_copy(src, dst, r.ls.at[len(begun)])
        k.start()
        begun.append(k)
        return k

    local.st = fetch(r.stream, r.st)
    local.gn = fetch(r.gains, r.gn)
    local.fq = fetch(r.freq, r.fq)
    local_wq = [fetch(qcols(z, 2 * c + k), r.wq.at[z, :, half_cols(k)]) for k in range(2)]
    local.wo = fetch(r.wout.at[:, pl.ds(pl.multiple_of(n * 256, 256), 256)], r.wo.at[n])
    local.kvv = fetch(r.kv, r.kvv)
    local.tg = fetch(r.targets, r.tg)
    local.wg = fetch(r.wgu, r.wg.at[:, 0:FFD])
    local.wd = fetch(r.wdown, r.wd.at[0:FFD])
    local.lm = fetch(r.lmh.at[pl.ds(pl.multiple_of(c * HALF, HALF), HALF)], r.lm)

    right, left = at_xy(rem(x + 1, NX), y), at_xy(rem(x + 3, NX), y)

    def weight_piece(i):
        cols = pl.ds(pl.multiple_of(c * HALF + i * 256, 256), 256)
        for dev, a, b in ((right, 0, 64), (left, 64, FFD)):
            g = r.wg.at[:, 128 + a : 128 + b, cols]
            send(p.xg, r.wgu.at[:, a:b, cols], g, dev, i // 4)
            send(p.xd, r.wdown.at[a:b, cols], r.wd.at[128 + a : 128 + b, cols], dev, i // 4)

    def pass_weights(g):
        cols = pl.ds(pl.multiple_of(c * HALF + g * 1024, 1024), 1024)
        for came, went, at in (
            (p.xg, p.fg, r.wg.at[:, 128 : 128 + FFD, cols]),
            (p.xd, p.fd, r.wd.at[128 : 128 + FFD, cols]),
        ):
            recv(came, at, g)
            send(went, at, at, partner, g)

    def spread(scratch, dst):
        for zz in range(NZ):
            dst[zz * 8 : zz * 8 + 8] = scratch[pl.ds(zz, 8, stride=8), :]

    z8 = pl.ds(pl.multiple_of(z * 8, 8), 8)

    def z_then_plane(zphase, pphase, s, rr, buf, start=True, beside=lambda: None):
        def piece(zz):
            return pl.ds(pl.multiple_of(zz * 8, 8), 8)

        if start:
            z_send(zphase, lambda zz: s.at[piece(zz)], rr.at[z8])
        beside()
        rr[z8, :] = s[z8, :]
        done(zphase, rr.at[0:56])
        for k in range(4):
            rows = [rr[pl.ds(j * 4 + k, 8, stride=8), :] for j in range(2)]
            buf[n, :, k * 128 : (k + 1) * 128] = jnp.concatenate(rows, axis=0).astype(BF)
        xy_send(pphase, lambda m: buf.at[n], buf.at[n])
        return lambda: done(pphase, buf.at[0:15])

    local.st.wait()
    x32 = r.st[...].astype(F32)
    rs = lax.rsqrt(jnp.mean(x32 * x32, axis=-1, keepdims=True) + 1e-5)
    for b in range(32):
        for j in range(2):
            r.sc[j * 32 + b : j * 32 + b + 1, :] = x32[j : j + 1, b * 128 : (b + 1) * 128]
    spread(r.sc, r.s1s)
    r.s4s[...] = jnp.zeros((128, 128), F32)
    row8 = lax.broadcasted_iota(jnp.int32, (8, 128), 0)
    lane8 = lax.broadcasted_iota(jnp.int32, (8, 128), 1)
    rs8 = jnp.where(row8 < 4, rs[0:1, 0:1], rs[1:2, 0:1])

    pl.semaphore_wait(bar, len(peers))

    for zz in zpeers:
        send(p.s1, r.s1s.at[pl.ds(pl.multiple_of(zz * 8, 8), 8)], r.s1r.at[z8], at_z(zz))
    for zz in zpeers:
        for k in range(2):
            send(p.wq, qcols(zz, 2 * c + k), r.wq.at[z, :, half_cols(k)], at_z(zz))
    weight_piece(0)
    weight_piece(1)
    send(p.fi, r.fin, r.fi, partner)
    send(p.fh, r.fhid, r.fh, partner)
    send(p.fo, r.fout, r.fo, partner)
    send(p.xh, r.fhid, r.fhx.at[0], right, 0)
    send(p.xh, r.fhid, r.fhx.at[1], left, 1)
    finish = z_then_plane(p.s1, p.s2, r.s1s, r.s1r, r.raw, False)
    local.fq.wait()
    local.gn.wait()
    pos = [r.lengths[rem(2 * t + j, B)] for j in range(2)]
    ang = jnp.where(row8 < 4, pos[0], pos[1]).astype(F32) * r.fq[0:1, :]
    cos8 = jnp.cos(ang)
    sin8 = jnp.where(lane8 < 64, -jnp.sin(ang), jnp.sin(ang))
    for b in range(32):
        r.g3[b : b + 1, :] = r.gn[2:3, b * 128 : (b + 1) * 128]

    for k in range(2):
        local_wq[k].wait()
    done(p.wq, r.wq.at[0:7, :, 0:256])
    mine = r.wq.at[:, :, pl.ds(pl.multiple_of(c * 256, 256), 256)]
    send(p.wqf, mine, mine, partner)
    done(p.wqf, mine)
    gq = jnp.concatenate(
        [r.gn[0:1, pl.ds(pl.multiple_of(k * 1024 + z * 128, 128), 128)] for k in range(4)], axis=1
    )
    finish()
    lhs = (r.raw[...].reshape(256, 512).astype(F32) * gq).astype(BF)
    prod = lax.dot_general(lhs, r.wq[...].reshape(QN, 512), NT, preferred_element_type=F32)
    for l in range(3):
        r.p1[l] = prod[:, l * 128 : (l + 1) * 128]
    for zz in range(NZ):
        for l in range(3):
            r.s3s[zz, :, l * 128 : (l + 1) * 128] = r.p1.at[l][
                pl.ds(zz, 32, stride=8), :
            ].astype(BF)
    z_send(p.s3, lambda zz: r.s3s.at[zz], r.s3r.at[z])
    weight_piece(2)
    weight_piece(3)
    r.s3r[z] = r.s3s[z]
    done(p.s3, r.s3r.at[0:7])
    acc = r.s3r[0].astype(F32)
    for s in range(1, NZ):
        acc = acc + r.s3r[s].astype(F32)
    for l in range(3):
        r.q1[l] = acc[:, l * 128 : (l + 1) * 128]
    for l in range(3):
        for j in range(2):
            r.s4s[pl.ds(l * 2 + j, 16, stride=8), :] = r.q1.at[l][pl.ds(j, 16, stride=2), :]

    def tile(m):
        return pl.ds(pl.multiple_of(m * 8, 8), 8)

    xy_send(p.s4, lambda m: r.s4s.at[tile(m)], r.s4r.at[tile(n)])
    xy_send(
        p.wo,
        lambda m: r.wout.at[:, pl.ds(pl.multiple_of(m * 256, 256), 256)],
        r.wo.at[n],
    )
    r.s4r[tile(n), :] = r.s4s[tile(n), :]
    done(p.s4, r.s4r.at[0:120])

    blocks = {
        (yy, l): jnp.concatenate(
            [r.s4r[pl.ds(yy * 8 + l * 2 + j, 4, stride=32), :] for j in range(2)], axis=0
        )
        for yy in range(NY)
        for l in range(3)
    }
    for hh in range(12):
        val = jnp.zeros((8, 128), F32)
        lane = 0
        while lane < 128:
            col = hh * 128 + lane
            tt, i = divmod(col, 48)
            at = (tt // 4) * 48 + i
            l, src = divmod(at, 128)
            width = min(48 - i, 128 - src, 128 - lane)
            piece = blocks[(tt % 4, l)]
            shift = (lane - src) % 128
            if shift:
                piece = pltpu.roll(piece, shift, 1)
            val = jnp.where((lane8 >= lane) & (lane8 < lane + width), piece, val)
            lane += width
        val = (val * rs8).astype(BF).astype(F32)
        turned = (val * cos8 + pltpu.roll(val, 64, 1) * sin8).astype(BF).astype(F32)
        if hh >= 4:
            turned = jnp.where(row8 % 4 == 3, val, turned)
        r.hs[pl.ds(hh, 8, stride=12), :] = turned

    local.kvv.wait()
    inv_root = HD**-0.5
    group = lax.broadcasted_iota(jnp.int32, (32, 128), 0) // 4
    group8 = (
        lax.broadcasted_iota(jnp.int32, (32, 8), 0) // 4
        == lax.broadcasted_iota(jnp.int32, (32, 8), 1)
    )
    place = lax.broadcasted_iota(jnp.int32, (32, CACHE), 1)
    for j in range(2):
        q = r.hs[j * 48 : j * 48 + 32, :]
        kn = r.hs[j * 48 + 32 : j * 48 + 40, :].astype(BF)
        vn = r.hs[j * 48 + 40 : j * 48 + 48, :].astype(BF)
        qd = jnp.concatenate([jnp.where(group == k, q, 0.0) for k in range(KV)], axis=1).astype(BF)
        scores = (
            lax.dot_general(qd, r.kvv[j, :, : KV * HD], NT, preferred_element_type=F32) * inv_root
        )
        fresh = lax.dot_general(q.astype(BF), kn, NT, preferred_element_type=F32)
        fresh = jnp.sum(jnp.where(group8, fresh, 0.0), axis=1, keepdims=True) * inv_root
        scores = jnp.where(place < pos[j], scores, -1e30)
        peak = jnp.maximum(jnp.max(scores, axis=1, keepdims=True), fresh)
        weights = jnp.exp(scores - peak)
        fresh_w = jnp.exp(fresh - peak)
        total = jnp.sum(weights, axis=1, keepdims=True) + fresh_w
        probs = (weights / total).astype(BF)
        fresh_p = jnp.where(group8, fresh_w / total, 0.0).astype(BF)
        wide = jnp.dot(probs, r.kvv[j, :, KV * HD :], preferred_element_type=F32)
        out = jnp.dot(fresh_p, vn, preferred_element_type=F32)
        for k in range(KV):
            out = out + jnp.where(group == k, wide[:, k * 128 : (k + 1) * 128], 0.0)
        r.osc[j * 32 : j * 32 + 32, :] = out.astype(BF).astype(F32)

    spread(r.osc, r.s5s)

    def beside():
        weight_piece(4)
        weight_piece(5)

    finish = z_then_plane(p.s5, p.s6, r.s5s, r.s5r, r.att, beside=beside)
    pass_weights(0)
    local.wo.wait()
    done(p.wo, r.wo.at[0:15])
    resid = r.raw[:, :, pl.ds(pl.multiple_of(x * 128, 128), 128)].reshape(256, 128).astype(F32)
    lo = resid * jnp.where(z == 2 * y, 1.0, 0.0)
    hi = resid * jnp.where(z == 2 * y + 1, 1.0, 0.0)
    finish()
    prod = jnp.dot(
        r.att[...].reshape(256, 512), r.wo[...].reshape(512, 256), preferred_element_type=F32
    ) + jnp.concatenate([lo, hi], axis=1)
    for h in range(2):
        for ys in range(NY):
            for j in range(2):
                at = [((m * 2 + h) * 4 + ys) * 16 + j * 8 for m in range(2)]
                r.s7s[h * 4 + ys, j * 16 : j * 16 + 16, :] = jnp.concatenate(
                    [prod[a : a + 8] for a in at], axis=0
                ).astype(BF)
    for zz in zpeers:
        send(p.s7, r.s7s.at[zz], r.s7r.at[z], across_z(zz))
    send(p.s7, r.s7s.at[z], r.s7r.at[z], partner)
    weight_piece(6)
    weight_piece(7)
    recv(p.xh, r.fhx.at[0], 0)
    recv(p.xh, r.fhx.at[1], 1)
    sent(p.xh, r.fhx)
    send(p.fy, r.fhx, r.fhy, partner)
    done(p.s7, r.s7r)
    acc = r.s7r[0].astype(F32)
    for s in range(1, NZ):
        acc = acc + r.s7r[s].astype(F32)

    def tile_rows(d):
        return pl.ds(ARRIVAL.index(d % NZ) * 16, 16)

    for j in range(2):
        r.mc[j, tile_rows(0), :] = acc[j * 16 : j * 16 + 16].astype(BF)
    for d in ZORDER:
        at = r.mc.at[:, tile_rows(0)]
        send(p.s8, at, r.mc.at[:, tile_rows(-d)], at_z(rem(z + d, NZ)), 7 - d)

    def tile_on(k):
        rows = tile_rows(k)
        at = ARRIVAL.index(k)
        late = next(i for i, (a, b) in enumerate(GROUPS) if a <= at < a + b)
        for d in (2, 1, 3):
            xx, yy = rem(x + d, NX), rem(y + d, NY)
            at = r.mid.at[n, rows]
            send(p.da, r.mc.at[par, rows], at, at_xy(x, yy), 6 - d + 6 * late)
            send(p.da, r.mc.at[rem(xx, 2), rows], at, at_xy(xx, y), 3 - d + 6 * late)
            at = r.mc.at[1 - par, rows, right_cols]
            send(p.db, at, r.xb.at[y, rows], at_xy(x, yy), 3 - d + 3 * late)

    left_cols, right_cols = pl.ds(0, 128), pl.ds(128, 128)
    tile_on(0)
    pass_weights(1)
    r.accg[...] = jnp.zeros((128, 256), F32)
    r.accu[...] = jnp.zeros((128, 256), F32)
    r.ssq[...] = jnp.zeros((128, 128), F32)
    for a in (FFD, 128 + FFD):
        r.wg[:, a : a + 16, :] = jnp.zeros((2, 16, D), BF)
        r.wd[a : a + 16, :] = jnp.zeros((16, D), BF)
    done(p.fi, r.fi)
    done(p.fh, r.fh)
    done(p.fo, r.fo)
    done(p.fy, r.fhy)
    r.fhp[...] = jnp.zeros((3, 2, 256), F32)
    r.fhp[:, :, 0:FFD] = r.fh[...]
    lane_h = lax.broadcasted_iota(jnp.int32, (3, 2, FFD), 2)
    r.fhp[:, :, 128 : 128 + FFD] = jnp.where(lane_h < 64, r.fhy[0], r.fhy[1])
    mine_g = r.wg.at[:, 128 : 128 + FFD, 0:HALF]
    mine_d = r.wd.at[128 : 128 + FFD, 0:HALF]
    for k in (p.xg, p.fg):
        sent(k, mine_g)
    for k in (p.xd, p.fd):
        sent(k, mine_d)
    for k in (local.wg, local.wd):
        k.wait()
    for d in ARRIVAL[1:]:
        recv(p.s8, r.mc.at[:, 0:16], d - 1)
        tile_on(d)
    sent(p.s8, r.mc.at[:, 0:112])

    near = (1, 3, 2)
    sent(p.da, r.mid.at[0:6])
    sent(p.db, r.xb.at[0:3])
    r.mid[n] = r.mc[par]
    for g in range(2):
        cols = pl.ds(pl.multiple_of((1 - c) * HALF + g * 1024, 1024), 1024)
        recv(p.fg, r.wg.at[:, 128 : 128 + FFD, cols], g)
        recv(p.fd, r.wd.at[128 : 128 + FFD, cols], g)

    def ffn_chunk(m):
        v = r.mid[m].astype(F32)
        r.ssq[...] += v[:, :128] * v[:, :128] + v[:, 128:] * v[:, 128:]
        cols = pl.ds(pl.multiple_of(m * 256, 256), 256)
        g = r.gn[1:2, cols]
        v4 = v.reshape(8, 2, 8, 256)
        for k, total in enumerate((r.accg, r.accu)):
            f = jnp.concatenate(
                [
                    (r.fi[i, k : k + 1, cols] * g).reshape(1, 1, 1, 256)
                    for i in range(2)
                ],
                axis=1,
            )
            act = (v4 * f).reshape(128, 256).astype(BF)
            total[...] += lax.dot_general(
                act, r.wg[k, :, cols], NT, preferred_element_type=F32
            )

    ffn_chunk(n)
    for late, rows in enumerate(pl.ds(a * 16, b * 16) for a, b in GROUPS):
        for d in near:
            m = rem(x + d, NX) * 4 + y
            recv(p.da, r.mid.at[m, rows], d - 1 + 6 * late)
            at = r.mid.at[m, rows, left_cols]
            for e in (2, 1, 3):
                yy = rem(y + e, NY)
                send(p.dg, at, at, at_xy(x, yy), (d - 1) * 3 + 3 - e)
            yy = rem(y + d, NY)
            m = x * 4 + yy
            recv(p.da, r.mid.at[m, rows], d + 2 + 6 * late)
            recv(p.db, r.xb.at[yy, rows], d - 1 + 3 * late)
            to = r.mid.at[m, rows, right_cols]
            for e in (2, 1, 3):
                xx = rem(x + e, NX)
                at = to if e == 2 else r.xb.at[yy, rows]
                send(p.dg, at, to, at_xy(xx, y), (3 - e) * 3 + d - 1)
    sent(p.dg, r.mid.at[0:9])

    def line_step(i, carry):
        ffn_chunk(rem(x + 1 + i, NX) * 4 + y)
        ffn_chunk(x * 4 + rem(y + 1 + i, NY))
        return carry

    lax.fori_loop(0, 3, line_step, 0)

    for dx, dy in sorted(((a, b) for a in near for b in near), key=lambda k: k.count(2)):
        m = rem(x + dx, NX) * 4 + rem(y + dy, NY)
        recv(p.dg, r.mid.at[m], (dx - 1) * 3 + dy - 1)
        ffn_chunk(m)
    scale = lax.rsqrt(jnp.sum(r.ssq[...], axis=1, keepdims=True) * (1.0 / D) + 1e-5)

    def by_member(k):
        return jnp.concatenate(
            [r.fhp[k, i : i + 1, :].reshape(1, 1, 1, 256) for i in range(2)], axis=1
        )

    gate = (r.accg[...] * scale).reshape(8, 2, 8, 256) * by_member(0)
    up = (r.accu[...] * scale).reshape(8, 2, 8, 256) * by_member(1)
    hidden = gate / (1.0 + jnp.exp(-gate)) * up * by_member(2)
    r.hid[...] = hidden.reshape(128, 256).astype(BF)

    def chunk(ch):
        return pl.ds(pl.multiple_of(ch * CA, CA), CA)

    def chunk_b(ch):
        return pl.ds(pl.multiple_of(ch * CB, CB), CB)

    def high(ch):
        return pl.ds(pl.multiple_of(WA + ch * CB, 128), CB)

    other = 1 - xl
    opposite = at_xy(rem(x + 2, NX), y)

    def a1(ch):
        send(p.a1, r.p3.at[pl.ds(other * 4, 4), :, chunk(ch)], r.r1a.at[:, :, chunk(ch)], opposite, ch)

    def b1(ch, yy):
        for h in range(2):
            at = r.p3.at[h * 4 + yy, :, high(ch)]
            send(p.b1, at, r.r1b.at[y, h, :, chunk_b(ch)], at_xy(x, yy), ch)

    def down_step(ch, carry):
        for cols in (chunk(ch), high(ch)):
            v = jnp.dot(r.hid[...], r.wd[:, cols], preferred_element_type=F32)
            for k in range(NZ):
                r.p3[rem(z + ARRIVAL[k], NZ), :, cols] = v[k * 16 : k * 16 + 16].astype(BF)
        a1(ch)
        for d in (2, 1, 3):
            b1(ch, rem(y + d, NY))
        return carry

    lax.fori_loop(0, NCH, down_step, 0)

    def a2(ch, yy):
        send(p.a2, r.s2a.at[yy, :, chunk(ch)], r.r2a.at[y, :, chunk(ch)], at_xy(x, yy), ch)

    def b2(ch):
        send(p.b2, r.s2b.at[other, :, chunk_b(ch)], r.r2b.at[:, chunk_b(ch)], opposite, ch)

    def second_step(ch, carry):
        recv(p.a1, r.r1a.at[:, :, chunk(ch)], ch)
        v = r.p3[pl.ds(xl * 4, 4), :, chunk(ch)].astype(F32) + r.r1a[:, :, chunk(ch)].astype(F32)
        r.s2a[:, :, chunk(ch)] = v.astype(BF)
        for d in (2, 1, 3):
            a2(ch, rem(y + d, NY))
        recv(p.b1, r.r1b.at[0:3, :, :, chunk_b(ch)], ch)
        v = jnp.concatenate(
            [r.p3[pl.ds(h * 4 + y, 1), :, high(ch)].astype(F32) for h in range(2)], axis=0
        )
        for d in near:
            v = v + r.r1b[rem(y + d, NY), :, :, chunk_b(ch)].astype(F32)
        r.s2b[:, :, chunk_b(ch)] = v.astype(BF)
        b2(ch)
        return carry

    lax.fori_loop(0, NCH, second_step, 0)
    sent(p.a1, r.r1a)
    sent(p.b1, r.r1b.at[0:3])
    sent(p.a2, r.r2a.at[0:3])
    sent(p.b2, r.r2b)

    row16 = lax.broadcasted_iota(jnp.int32, (16, 128), 0)
    own_row = rem(row16, 8) == z
    away = rem(xl * 4 + y - z + NZ, NZ)
    turn = (away + 3) // 4
    slot = turn * (2 - turn) * (2 * away - 1) + turn * (turn - 1) // 2 * (16 - 2 * away)
    tile16 = pl.ds(pl.multiple_of(slot * 16, 16), 16)

    def parts(ch):
        return (ch * BA, BA), (NCH * BA + ch * BB, BB)

    def last_step(ch):
        recv(p.a2, r.r2a.at[0:3, :, chunk(ch)], ch)
        recv(p.b2, r.r2b.at[:, chunk_b(ch)], ch)
        for b in [b for start, length in parts(ch) for b in range(start, start + length)]:
            if b < NCH * BA:
                cols = slice(b * 128, (b + 1) * 128)
                v = r.s2a[y, :, cols].astype(F32)
                for d in near:
                    v = v + r.r2a[rem(y + d, NY), :, cols].astype(F32)
            else:
                cols = slice((b - NCH * BA) * 128, (b - NCH * BA + 1) * 128)
                v = r.s2b[xl, :, cols].astype(F32) + r.r2b[:, cols].astype(F32)
            at = slice(b * 128, (b + 1) * 128)
            v = v * jnp.where(row16 < 8, r.fo[0:1, at], r.fo[1:2, at])
            m = r.mid[b // 2, tile16, (b % 2) * 128 : (b % 2 + 1) * 128].astype(F32)
            r.f3[b * 16 : (b + 1) * 16, :] = v + jnp.where(own_row, m, 0.0)
        for zz in range(NZ):
            r.s13s[zz, ch] = chunk_rows(zz, ch).astype(BF)
        for zz in zpeers:
            send(p.s13, r.s13s.at[zz, ch], r.s13r.at[z, ch], at_z(zz), ch)

    def chunk_rows(zz, ch):
        return jnp.concatenate(
            [
                r.f3[pl.ds(start * 16 + m * 8 + zz, length, stride=16), :]
                for m in range(2)
                for start, length in parts(ch)
            ],
            axis=0,
        )

    for ch in range(NCH):
        last_step(ch)
    for ch in range(NCH):
        v = chunk_rows(z, ch)
        recv(p.s13, r.s13r.at[0:7, ch], ch)
        for zz in zpeers:
            v = v + r.s13r[zz, ch].astype(F32)
        for m in range(2):
            row = m * 8
            for start, length in parts(ch):
                at = m * 32 + start
                r.vs[at : at + length, :] = v[row : row + length]
                row += length
    sent(p.s13, r.s13r.at[0:7])
    both = jnp.zeros((32, 128), F32)
    for m in range(2):
        v = r.vs[m * 32 : m * 32 + 32, :]
        v = v.astype(BF).astype(F32)
        mean = jnp.sum(jnp.sum(v * v, axis=1, keepdims=True), axis=0, keepdims=True) * (1.0 / D)
        both = both + (v * lax.rsqrt(mean + 1e-5) * r.g3[...]).astype(BF).astype(F32)
    r.fs[...] = both

    def half(k):
        return pl.ds(pl.multiple_of(k * 16, 16), 16)

    send(p.fx, r.fs.at[half(1 - c)], r.fr, partner)
    done(p.fx, r.fr)
    r.fb[own, z] = ((r.fs[half(c), :] + r.fr[...]) * 0.25).astype(BF)
    for d in FAR_Z:
        send(p.s14, r.fb.at[own, z], r.fb.at[own, z], at_z(rem(z + d, NZ)), 7 - d)
    xy_send(p.s15, lambda m: r.fb.at[own, z], r.fb.at[own, z], 0)
    local.lm.wait()
    local.tg.wait()
    wanted = jnp.broadcast_to(r.tg[...].astype(F32), (B, B)).T[:, 0:1]
    for d in FAR_Z:
        zz = rem(z + d, NZ)
        recv(p.s14, r.fb.at[own, zz], d - 1)
        xy_send(p.s15, lambda m: r.fb.at[own, zz], r.fb.at[own, zz], d)
    sent(p.s14, r.fb.at[own, 0:3])
    recv(p.s15, r.fb.at[0:15, z], 0)
    for d in (2, 6, 1, 7):
        send(p.pz, r.fb.at[:, z], r.fb.at[:, z], at_z(rem(z + d, NZ)), 8 - d)
    sent(p.pz, r.fb.at[:, 0:4])
    for d in ARRIVAL:
        zz = rem(z + d, NZ)
        if d in FAR_Z:
            recv(p.s15, r.fb.at[0:15, zz], d)
        elif d:
            recv(p.pz, r.fb.at[:, zz], d)
        for k in range(NP):
            at = pl.ds(pl.multiple_of(k * 128 + zz * 16, 16), 16)
            r.ff[at, :] = r.fb[k, zz].astype(F32)
        for h in range(2):
            to = pl.ds(pl.multiple_of(h * 64 + zz * 8, 8), 8)
            for b in range(16):
                r.lh[to, b * 128 : (b + 1) * 128] = r.ff[
                    pl.ds(h * 1024 + zz * 16 + b, 8, stride=128), :
                ]
    sent(p.s15, r.fb.at[0:15, 0:4])
    r.lp[...] = jnp.dot(r.lh[...].astype(BF), r.lm[...], preferred_element_type=F32)
    send(p.lx, r.lp, r.lr, partner)
    done(p.lx, r.lr)
    mean_f = r.lp[...] + r.lr[...]
    r.logits_o[...] = mean_f.astype(BF)

    ids = (lax.broadcasted_iota(jnp.int32, (B, VD), 1) + t * VD).astype(F32)
    found = jnp.sum(jnp.where(ids == wanted, mean_f, 0.0), axis=1, keepdims=True)
    peak = jnp.max(mean_f, axis=1, keepdims=True)
    total = jnp.sum(jnp.exp(mean_f - peak), axis=1, keepdims=True)
    lane = lax.broadcasted_iota(jnp.int32, (B, B), 1)
    stat = jnp.where(lane == 0, peak, jnp.where(lane == 1, total, jnp.where(lane == 2, found, 0.0)))
    r.sz[z] = stat.T[:8]

    def combine(ref, count):
        peaks = [ref[k, 0:1, :] for k in range(count)]
        top_ = peaks[0]
        for k in range(1, count):
            top_ = jnp.maximum(top_, peaks[k])
        tot = ref[0, 1:2, :] * jnp.exp(peaks[0] - top_)
        hit = ref[0, 2:3, :]
        for k in range(1, count):
            tot = tot + ref[k, 1:2, :] * jnp.exp(peaks[k] - top_)
            hit = hit + ref[k, 2:3, :]
        return top_, tot, hit

    z_send(p.s16, lambda zz: r.sz.at[z], r.sz.at[z])
    done(p.s16, r.sz.at[0:7])
    a, b_, h = combine(r.sz, NZ)
    r.sx[n] = jnp.concatenate([a, b_, h, jnp.zeros((5, 128), F32)], axis=0)
    xy_send(p.s17, lambda m: r.sx.at[n], r.sx.at[n])
    done(p.s17, r.sx.at[0:15])
    a, b_, h = combine(r.sx, NP)
    r.lp_o[...] = h - (a + jnp.log(b_))

    for sem, ref in drains:
        wait_bytes(sem, ref)


def hand_on(logits, logprob, logits_o, logprob_o):
    logits_o[...] = logits[...]
    logprob_o[...] = logprob[...]


def body(
    stream_in, kv_cache, lengths, targets, norm_gains, w_qkv, w_out, w_gate_up, w_down, lm_head,
    fast_in, fast_hidden, fast_out,
):
    freq = np.float32(500000.0) ** (-np.arange(64, dtype=np.float32) * 2.0 / 128)
    freq = jnp.asarray(np.concatenate([freq, freq])[None, :], F32)
    args = dict(
        stream=stream_in, kv=kv_cache, lengths=lengths, targets=targets.reshape(1, B),
        gains=norm_gains, wqkv=w_qkv.T, wout=w_out,
        wgu=w_gate_up.swapaxes(1, 2), wdown=w_down, lmh=lm_head,
        fin=fast_in, fhid=fast_hidden.swapaxes(0, 1), fout=fast_out, freq=freq,
    )
    got = pl.pallas_call(
        functools.partial(kernel, list(args)),
        out_shape=[VM(k.shape, k.dtype) for k in OUTS.values()],
        in_specs=[
            pl.BlockSpec(memory_space=pltpu.SMEM if v is lengths else pl.ANY)
            for v in args.values()
        ],
        out_specs=[pl.BlockSpec(memory_space=VM)] * len(OUTS),
        scratch_shapes=[
            *SCRATCH.values(),
            *LS.values(),
            *(DMA((count,)) for n in PHASES.values() for count in (1, n)),
        ],
        compiler_params=pltpu.CompilerParams(
            collective_id=0, has_side_effects=True, vmem_limit_bytes=60 * 1024 * 1024
        ),
        name="step",
    )(*args.values())
    got = [pltpu.with_memory_space_constraint(k, VM) for k in got]
    got = pl.pallas_call(
        hand_on,
        out_shape=list(OUTS.values()),
        in_specs=[pl.BlockSpec(memory_space=VM)] * 2,
        name="result",
    )(*got)
    return (got[0], got[1].reshape(B))


MEMBER_TP = ("member", "tp_0", "tp_1", "tp_2")
TP = ("tp_0", "tp_1", "tp_2")
IN_SPECS = (
    P(MEMBER_TP, None), P(MEMBER_TP, None, None), P(), P(), P(), P(None, TP), P(TP, None),
    P(None, None, TP), P(TP, None), P(None, TP), P("member", None, None), P("member", None, TP),
    P("member", None),
)


def solution(mesh):
    split = Mesh(
        mesh.devices.reshape(mesh.shape["member"], NX, NZ, NY), MEMBER_TP
    )
    return jax.shard_map(
        body, mesh=split, in_specs=IN_SPECS, out_specs=(P(None, TP), P()), check_vma=False
    )
```
